256 devices in a mesh: gx: 4 (over x), gy: 8 (over z_hi, core), gz: 8 (over z_lo, y).
Axes of the slice: x: 4, y: 4, z: 8 (z_hi: 4, z_lo: 2; z = z_hi * 2 + z_lo), core: 2. Of those that a mesh axis runs over, the one named last changes fastest.
Arguments:
- velocity: float32 [3, 20971520], P(None, ('gx', 'gy', 'gz')), may hold values from -6 to 6
- particle_place: int32 [20971520], P(('gx', 'gy', 'gz')), may hold values from 0 to 8191
- grid_shift: int32 [3], replicated, may hold values from 1 to 3
- rotation_axis: int32 [256, 128, 128], P('gy', 'gx', 'gz'), may hold values from 0 to 1023
Outputs:
- new_velocity: float32 [3, 20971520], P(None, ('gx', 'gy', 'gz'))
- modes: float32 [2, 3, 128, 256, 128], P(None, None, ('gy', 'gz'), 'gx')
- spectrum: float32 [64], replicated
The draws below stay inside these ranges and needn't reach their ends.
Inputs may be any that keep to these rules, and one draw needn't show every extreme that they name: `particle_place`: A device's particle slots come in tiles of 640 slots; tile j holds particles of the device's local cells j * 128 to j * 128 + 127, and a value is (cell within the tile) * 4**3 + (sub-cell code).
All inputs are finite; a program needn't handle non-finite values.
Results may differ from the reference program's by a relative error of at most 0.0005.
Values sent between devices are 32-bit elements; how exact they have to be, the bound alone decides.
No kernel may reach another device: no remote copies, remote signals or barrier semaphores. Data moves between devices by JAX's collectives and lax.ppermute only.
A program may use at most 128 MiB of HBM per device.

```python
import math
import jax
import jax.numpy as jnp
from jax import lax

CX = 32
CY = 32
CZ = 16
PPC = 5
TILE = 128
SUB = 4
NAXES = 1024
NX = 128
NY = 256
NZ = 128
NSHELL = 64
PARTS_SIZE = 20971520
N_GY = 8
N_GZ = 8


def plant(array, own_key, smallest, top_value):
    extent = array.shape
    index_at = [jax.random.randint(jax.random.fold_in(own_key, axis), (), 0, extent[axis]) for axis in range(len(extent))]
    array = array.at[tuple(index_at)].set(smallest)
    longest = extent.index(max(extent))
    index_at[longest] = (index_at[longest] + 1) % extent[longest]
    return array.at[tuple(index_at)].set(top_value)


def levels(stream_key, dims, shards, low, largest):
    factor_of = 1.0
    for position, parts in shards:
        steps = jax.random.uniform(jax.random.fold_in(jax.random.fold_in(stream_key, 6), position), (parts,), jnp.float32, low / len(shards), largest / len(shards))
        factor_of = factor_of * jnp.repeat(jnp.exp(steps), dims[position] // parts).reshape((-1,) + (1,) * (len(dims) - 1 - position))
    return factor_of


def scatter_about(rng, dims, scale, most, split=(), held_as=jnp.bfloat16):
    level = levels(rng, dims, split, -0.22, 0.18) if split else 1.0
    array = jax.random.normal(rng, dims, jnp.float32) * scale * level
    return jnp.minimum(jnp.maximum(array, -most), most).astype(held_as)


def setup_inputs(seed: int = 0) -> dict:
    key_of = jax.random.split(jax.random.key(seed), 5)
    return {
        "velocity": scatter_about(key_of[0], (3, PARTS_SIZE), 1.0, 6.0, ((1, 256),), jnp.float32),
        "particle_place": plant(jax.random.randint(key_of[1], (PARTS_SIZE,), 0, TILE * SUB**3), jax.random.fold_in(key_of[1], 1), 0, (TILE * SUB**3) - 1).astype(jnp.int32),
        "grid_shift": jax.random.randint(key_of[2], (3,), 1, SUB).astype(jnp.int32),
        "rotation_axis": plant(jax.random.randint(key_of[3], (NY, NX, NZ), 0, NAXES), jax.random.fold_in(key_of[3], 1), 0, NAXES - 1).astype(jnp.int32),
    }


ROT_COS = math.cos(130.0 * math.pi / 180.0)
ROT_SIN = math.sin(130.0 * math.pi / 180.0)

def axis_vectors(axis_index):
    level = 1.0 - (2.0 * axis_index.astype(jnp.float32) + 1.0) / NAXES
    radius = jnp.sqrt(1.0 - level * level)
    turn = (axis_index * 1597 % 2584).astype(jnp.float32) * (2.0 * math.pi / 2584.0)
    return jnp.stack([radius * jnp.cos(turn), radius * jnp.sin(turn), level])

def collide(particle_speed, cell_mean, normal):
    offset = particle_speed - cell_mean
    across = jnp.cross(normal, offset, axis=0)
    along = lax.optimization_barrier(jnp.sum(normal * offset, axis=0))
    return cell_mean + ROT_COS * offset + ROT_SIN * across + (1.0 - ROT_COS) * along * normal

def signed_wave(length):
    wave = jnp.arange(length, dtype=jnp.int32)
    return jnp.where(wave >= length // 2, wave - length, wave)

def reference(velocity, particle_place, grid_shift, rotation_axis):
    per_device = PPC * CX * CY * CZ
    per_tile = PPC * TILE
    particle_total = velocity.shape[1]
    slot_id = jnp.arange(particle_total, dtype=jnp.int32)
    device = slot_id // per_device
    within = slot_id % per_device
    local_cell = within // per_tile * TILE + particle_place // SUB ** 3
    sub_cell = particle_place % SUB ** 3
    along_x = device // (N_GY * N_GZ)
    along_y = device // N_GZ % N_GY
    along_z = device % N_GZ
    cell_z = along_z * CZ + local_cell % CZ
    cell_x = along_x * CX + local_cell // CZ % CX
    cell_y = along_y * CY + local_cell // (CZ * CX)
    step_x = (sub_cell // (SUB * SUB) + grid_shift[0] >= SUB).astype(jnp.int32)
    step_y = (sub_cell // SUB % SUB + grid_shift[1] >= SUB).astype(jnp.int32)
    step_z = (sub_cell % SUB + grid_shift[2] >= SUB).astype(jnp.int32)
    shifted = ((cell_y + step_y) % NY * NX + (cell_x + step_x) % NX) * NZ + (cell_z + step_z) % NZ
    plain_cell = (cell_y * NX + cell_x) * NZ + cell_z
    cell_total = NX * NY * NZ
    ones = jnp.ones((particle_total,), jnp.float32)
    momentum = jax.ops.segment_sum(velocity.T, shifted, num_segments=cell_total)
    shifted_count = jax.ops.segment_sum(ones, shifted, num_segments=cell_total)
    cell_mean = momentum / jnp.maximum(shifted_count, 1.0)[:, None]
    normal = axis_vectors(rotation_axis.reshape(-1))
    new_speed = collide(velocity, cell_mean[shifted].T, normal[:, shifted])
    plain_sum = jax.ops.segment_sum(new_speed.T, plain_cell, num_segments=cell_total)
    plain_count = jax.ops.segment_sum(ones, plain_cell, num_segments=cell_total)
    cell_velocity = (plain_sum / jnp.maximum(plain_count, 1.0)[:, None]).T.reshape(3, NY, NX, NZ)
    transformed = jnp.fft.fftn(cell_velocity, axes=(1, 2, 3))
    transformed = jnp.transpose(transformed, (0, 3, 1, 2)) / math.sqrt(NX * NY * NZ)
    modes = jnp.stack([jnp.real(transformed), jnp.imag(transformed)]).astype(jnp.float32)
    energy = lax.optimization_barrier(jnp.sum(modes * modes, axis=(0, 1)))
    wave_z = signed_wave(NZ)
    wave_y = signed_wave(NY)
    wave_x = signed_wave(NX)
    square = wave_z[:, None, None] ** 2 + wave_y[None, :, None] ** 2 + wave_x[None, None, :] ** 2
    shell_index = jnp.floor(jnp.sqrt(square.astype(jnp.float32))).astype(jnp.int32)
    shell_index = jnp.minimum(shell_index, NSHELL).reshape(-1)
    shell_sums = jax.ops.segment_sum(energy.reshape(-1), shell_index, num_segments=NSHELL + 1)
    shell_counts = jax.ops.segment_sum(jnp.ones_like(energy.reshape(-1)), shell_index, num_segments=NSHELL + 1)
    spectrum = shell_sums[:NSHELL] / shell_counts[:NSHELL]
    return (new_speed, modes, spectrum)
```

```python
import math

import jax
import jax.numpy as jnp
import numpy as np
from jax import lax
from jax.experimental import pallas as pl
from jax.experimental.pallas import tpu as pltpu
from jax.sharding import Mesh
from jax.sharding import PartitionSpec as P

PPC = 5
TILE = 128
SUB = 4
NAXES = 1024
NSHELL = 64
NX, NY, NZ = 128, 256, 128
GX_GY_GZ = ("gx", "gy_0", "gy_1", "gz_0", "gz_1")
GY = ("gy_0", "gy_1")
GZ = ("gz_0", "gz_1")
GY_GZ = ("gy_0", "gy_1", "gz_0", "gz_1")
ROT_COS = math.cos(130.0 * math.pi / 180.0)
ROT_SIN = math.sin(130.0 * math.pi / 180.0)
F32 = jnp.float32
BF16 = jnp.bfloat16
TILES = 128
ROWS = 160
SROW = 36
LROW = 68
BLOCKS = 4
GROUPS = TILES // 8 // BLOCKS


def axis_vectors(axis_index):
    level = 1.0 - (2.0 * axis_index.astype(F32) + 1.0) / NAXES
    radius = jnp.sqrt(1.0 - level * level)
    whole_turns = (axis_index * 1597).astype(F32) * (1.0 / 2584.0)
    turn = (axis_index * 1597 - 2584 * jnp.floor(whole_turns).astype(jnp.int32)).astype(F32)
    turn = turn * (2.0 * math.pi / 2584.0)
    return radius * jnp.cos(turn), radius * jnp.sin(turn), level


def iota(shape, dim):
    return lax.broadcasted_iota(jnp.int32, shape, dim)


def lroll(x, amount):
    amount %= 128
    return pltpu.roll(x, amount, 1) if amount else x


def sroll(x, amount):
    return pltpu.roll(x, amount % x.shape[0], 0)


def split(x):
    high = x.astype(BF16)
    return high, (x - high.astype(F32)).astype(BF16)


def dot(a, b):
    return jnp.dot(a, b, preferred_element_type=F32)


def octants(place, shift_ref):
    bit_x = (((place >> 4) & 3) + shift_ref[0] >= SUB).astype(jnp.int32)
    bit_y = (((place >> 2) & 3) + shift_ref[1] >= SUB).astype(jnp.int32)
    bit_z = ((place & 3) + shift_ref[2] >= SUB).astype(jnp.int32)
    return bit_x * 4 + bit_y * 2 + bit_z


def tile_row(rows, t):
    return jnp.concatenate([rows[PPC * t + r : PPC * t + r + 1, :] for r in range(PPC)], axis=1)


def onehot_of(member, t, cells):
    return jnp.concatenate(
        [
            (cells == member[PPC * t + r : PPC * t + r + 1, :]).astype(F32).astype(BF16)
            for r in range(PPC)
        ],
        axis=1,
    )


def scatter_body(shift_ref, v_ref, p_ref, axis_ref, s_ref, m_ref, n_ref, xlo_ref, xhi_ref, ylo_ref,
                 yhi_ref, zlo_ref, zhi_ref, turn_ref, edge_ref, zed_ref):
    step = pl.program_id(0)
    cells = iota((TILE, TILE), 0)
    upper = iota((8, TILE), 0) < 4

    def group(g, carry):
        place = p_ref[pl.ds(pl.multiple_of(g * 40, 8), 40), :]
        member = place >> 6
        octant = octants(place, shift_ref)
        speed = v_ref[:, pl.ds(pl.multiple_of(g * 5120, 128), 5120)]
        high = speed.astype(BF16).astype(F32)
        low = speed - high
        one = jnp.ones((1, 640), F32)
        zero = jnp.zeros((1, 640), F32)
        for t in range(8):
            here = slice(t * 640, (t + 1) * 640)
            onehot = onehot_of(member, t, cells)
            code = jnp.broadcast_to(tile_row(octant, t), (8, 640))
            values = jnp.concatenate([high[:, here], one, low[:, here], zero], axis=0)
            weighted = jnp.concatenate(
                [jnp.where(code == o, values, 0.0) for o in range(8)], axis=0
            ).astype(BF16)
            sums = lax.dot_general(
                weighted, onehot, (((1,), (1,)), ((), ())), preferred_element_type=F32
            )
            for pair in range(4):
                even = sums[16 * pair : 16 * pair + 8]
                odd = sums[16 * pair + 8 : 16 * pair + 16]
                both = jnp.where(upper, even + sroll(even, 4), odd + sroll(odd, 4))
                turn_ref[SROW * t + 8 * pair : SROW * t + 8 * pair + 8, :] = both
        first = pl.multiple_of((step * GROUPS + g) * 8, 8)
        for r in range(32):
            s_ref[r, pl.ds(first, 8), :] = turn_ref[pl.ds(r, 8, stride=SROW), :]
        return carry

    lax.fori_loop(0, GROUPS, group, 0)

    @pl.when(step == BLOCKS - 1)
    def _():
        for c, part in enumerate(axis_vectors(axis_ref[...])):
            n_ref[c] = part
        lane = iota((TILES, 128), 1)
        row = iota((TILES, 128), 0)
        z = lane & 15
        x_in = lane >> 4
        x_out = row & 3
        last = (x_in == 7) & (x_out == 3)

        def x_shift(plane):
            rolled = lroll(plane, 16)
            return jnp.where(
                x_in > 0, rolled, jnp.where(x_out > 0, sroll(rolled, 1), 0.0)
            )

        for q in range(5):
            for by in range(2):
                parts = []
                for bx in range(2):
                    base = bx * 4 + by * 2
                    if q < 4:
                        above = s_ref[(base + 1) * 4 + q]
                        parts.append(
                            s_ref[base * 4 + q] + jnp.where(z > 0, lroll(above, 1), 0.0)
                        )
                    else:
                        rim = jnp.zeros((TILES, 128), F32)
                        for k in range(4):
                            rim = jnp.where(z == k, lroll(s_ref[(base + 1) * 4 + k], k - 15), rim)
                        parts.append(rim)
                main = parts[0] + x_shift(parts[1])
                edge = jnp.where(last, parts[1], 0.0)
                dst = m_ref if q < 4 else zed_ref
                at = q if q < 4 else 0
                if by == 0:
                    dst[at, 0:TILES, :] = main
                    dst[at, TILES:ROWS, :] = jnp.zeros((ROWS - TILES, 128), F32)
                    edge_ref[q, 0:TILES, :] = edge
                    edge_ref[q, TILES:ROWS, :] = jnp.zeros((ROWS - TILES, 128), F32)
                else:
                    dst[at, 4:132, :] = dst[at, 4:132, :] + main
                    edge_ref[q, 4:132, :] = edge_ref[q, 4:132, :] + edge
        lane40 = iota((40, 128), 1)
        low_face = jnp.zeros((40, 128), F32)
        high_face = jnp.zeros((40, 128), F32)
        for q in range(4):
            inside = (lane40 >> 4) == q
            low_face = jnp.where(inside, lroll(m_ref[q, pl.ds(0, 40, stride=4), :], 16 * q), low_face)
            high_face = jnp.where(
                inside, lroll(edge_ref[q, pl.ds(3, 40, stride=4), :], 16 * q - 112), high_face
            )
        inside = (lane40 >> 2) == 16
        low_face = jnp.where(inside, lroll(zed_ref[0, pl.ds(0, 40, stride=4), :], 64), low_face)
        high_face = jnp.where(inside, lroll(edge_ref[4, pl.ds(3, 40, stride=4), :], 64 - 112), high_face)
        for c in range(3):
            inside = ((lane40 >> 4) == 5 + c) & (iota((40, 128), 0) < 32)
            face = jnp.concatenate(
                [n_ref[c, pl.ds(0, 32, stride=4), :], jnp.zeros((8, 128), F32)], axis=0
            )
            low_face = jnp.where(inside, lroll(face, 80 + 16 * c), low_face)
        xlo_ref[...] = low_face
        xhi_ref[...] = high_face
        ylo_ref[...] = jnp.zeros((40, 128), F32)
        yhi_ref[...] = jnp.zeros((40, 128), F32)
        for q in range(5):
            src = m_ref if q < 4 else zed_ref
            at = q if q < 4 else 0
            ylo_ref[4 * q : 4 * q + 4, :] = src[at, 0:4, :]
            yhi_ref[4 * q : 4 * q + 4, :] = src[at, 128:132, :]
        for c in range(3):
            ylo_ref[20 + 4 * c : 24 + 4 * c, :] = n_ref[c, 0:4, :]
        big = iota((ROWS, 128), 1)
        slot = big & 15
        low_z = jnp.zeros((ROWS, 128), F32)
        for q in range(4):
            low_z = jnp.where(slot == q, lroll(m_ref[q], q), low_z)
        for c in range(3):
            face = jnp.concatenate([n_ref[c], jnp.zeros((ROWS - TILES, 128), F32)], axis=0)
            low_z = jnp.where(slot == 4 + c, lroll(face, 4 + c), low_z)
        zlo_ref[...] = low_z
        zhi_ref[...] = zed_ref[0]


def fold_x_body(xlo_ref, xhi_ref, from_low, from_high, ylo_ref, yhi_ref,
                xlo_out, xhi_out, ylo_out, yhi_out):
    low = xlo_ref[...] + from_low[...]
    high = xhi_ref[...] + from_high[...]
    xlo_out[...] = low
    xhi_out[...] = high
    lane = iota((1, 128), 1)
    for src, dst, y in ((ylo_ref, ylo_out, 0), (yhi_ref, yhi_out, 32)):
        dst[...] = src[...]
        for q in range(4):
            dst[4 * q : 4 * q + 1, :] = jnp.where(
                lane < 16, lroll(low[y : y + 1], -16 * q), src[4 * q : 4 * q + 1, :]
            )
        dst[16:17, :] = jnp.where(lane < 4, lroll(low[y : y + 1], -64), src[16:17, :])
        dst[32:33, :] = high[y : y + 1]


def fold_y_body(ylo_ref, yhi_ref, from_low, from_high, xlo_ref, xhi_ref, zlo_ref, zhi_ref,
                ylo_out, yhi_out, zlo_out, zhi_out):
    low = ylo_ref[...] + from_low[...]
    high = yhi_ref[...] + from_high[...]
    ylo_out[...] = low
    yhi_out[...] = high
    zlo_out[...] = zlo_ref[...]
    zhi_out[...] = zhi_ref[...]
    x_low = xlo_ref[...]
    x_high = xhi_ref[...]
    lane = iota((40, 128), 1)
    lo0 = zlo_out[pl.ds(0, 40, stride=4), :]
    hi0 = zhi_out[pl.ds(0, 40, stride=4), :]
    lo3 = zlo_out[pl.ds(3, 40, stride=4), :]
    hi3 = zhi_out[pl.ds(3, 40, stride=4), :]
    for q in range(4):
        lo0 = jnp.where(lane == q, lroll(x_low, q - 16 * q), lo0)
        lo3 = jnp.where(lane == 120 + q, lroll(x_high, 120 + q - 16 * q), lo3)
    for c in range(3):
        lo3 = jnp.where(lane == 124 + c, lroll(x_high, 124 + c - 80 - 16 * c), lo3)
    hi0 = jnp.where(lane < 4, lroll(x_low, -64), hi0)
    hi3 = jnp.where((lane >= 120) & (lane < 124), lroll(x_high, 120 - 64), hi3)
    zlo_out[pl.ds(0, 40, stride=4), :] = lo0
    zhi_out[pl.ds(0, 40, stride=4), :] = hi0
    zlo_out[pl.ds(3, 40, stride=4), :] = lo3
    zhi_out[pl.ds(3, 40, stride=4), :] = hi3
    lane4 = iota((4, 128), 1)
    slot = lane4 & 15
    corner = (iota((4, 128), 0) == 3) & (lane4 >= 120)
    for face, first in ((low, 0), (high, 128)):
        lo = jnp.zeros((4, 128), F32)
        for q in range(4):
            lo = jnp.where(slot == q, lroll(face[4 * q : 4 * q + 4], q), lo)
        for c in range(3):
            lo = jnp.where(slot == 4 + c, lroll(face[20 + 4 * c : 24 + 4 * c], 4 + c), lo)
        end = face[32:33]
        tail = jnp.zeros((1, 128), F32)
        lane1 = iota((1, 128), 1)
        for q in range(4):
            tail = jnp.where(lane1 == 120 + q, lroll(end, 120 + q - 16 * q), tail)
        for c in range(3):
            tail = jnp.where(lane1 == 124 + c, lroll(end, 124 + c - 80 - 16 * c), tail)
        zlo_out[first : first + 4, :] = jnp.where(corner, tail, lo)
        hi = jnp.where(slot < 4, face[16:20], 0.0)
        zhi_out[first : first + 4, :] = jnp.where(
            corner, jnp.where(lane1 < 124, lroll(end, 120 - 64), 0.0), hi
        )


VROWS = 136


def cell_body(s_ref, m_ref, n_ref, xlo_ref, xhi_ref, ylo_ref, yhi_ref, zlo_ref, zhi_ref,
              from_low, from_high, view_ref, send_ref, ext_ref, end_ref, vel_ref):
    z_low = zlo_ref[0:VROWS, :] + from_low[0:VROWS, :]
    z_high = zhi_ref[0:VROWS, :] + from_high[0:VROWS, :]
    x_low = xlo_ref[...]
    x_high = xhi_ref[...]
    y_low = ylo_ref[...]
    y_high = yhi_ref[...]
    lane40 = iota((40, 128), 1)
    lane = iota((VROWS, 128), 1)
    row = iota((VROWS, 128), 0)
    z = lane & 15
    x_in = lane >> 4
    x_out = row & 3
    for k in range(7):
        if k < 4:
            ext_ref[k] = m_ref[k]
            held = ext_ref[k, pl.ds(0, 40, stride=4), :]
            ext_ref[k, pl.ds(0, 40, stride=4), :] = jnp.where(
                lane40 < 16, lroll(x_low, -16 * k), held
            )
            ext_ref[k, 0:4, :] = y_low[4 * k : 4 * k + 4]
            ext_ref[k, 128:132, :] = y_high[4 * k : 4 * k + 4]
            amount = 112 - 16 * k
        else:
            c = k - 4
            ext_ref[k, 0:TILES, :] = n_ref[c]
            ext_ref[k, 128:132, :] = y_high[20 + 4 * c : 24 + 4 * c]
            amount = 32 - 16 * c
        end_ref[k, pl.ds(3, 40, stride=4), :] = lroll(x_high, amount)
        end_ref[k, 131:132, :] = lroll(y_high[32:33], amount)
        if k < 4:
            end_ref[k, 3:4, :] = lroll(y_low[32:33], amount)

    def pair(k):
        main = ext_ref[k, 0:VROWS, :]
        end = end_ref[k, 0:VROWS, :]
        if k < 4:
            main = jnp.where(z == 0, lroll(z_low, -k), main)
            end = jnp.where(z == 0, lroll(z_low, -8 - k), end)
        main1 = jnp.where(z < 15, lroll(main, -1), lroll(z_high, 15 - k))
        end1 = jnp.where(z < 15, lroll(end, -1), lroll(z_high, 7 - k))
        return (main, main1), (end, end1)

    count_main, count_end = pair(3)
    inv_main = [1.0 / jnp.maximum(a, 1.0) for a in count_main]
    inv_end = [1.0 / jnp.maximum(a, 1.0) for a in count_end]
    for slot, k in enumerate((0, 1, 2, 4, 5, 6)):
        mains, ends = pair(k)
        for bz in range(2):
            main, end = mains[bz], ends[bz]
            if k < 3:
                main = main * inv_main[bz]
                end = end * inv_end[bz]
            rolled = lroll(main, -16)
            ahead = jnp.where(x_in < 7, rolled, jnp.where(x_out == 3, end, sroll(rolled, -1)))
            view_ref[bz * 6 + slot] = main
            view_ref[(2 + bz) * 6 + slot] = ahead

    def group(g, carry):
        first = pl.multiple_of(g * 8, 8)
        acc = [jnp.zeros((8, 128), F32) for _ in range(3)]
        total = jnp.zeros((8, 128), F32)
        for bx in range(2):
            for bz in range(2):
                wide = [view_ref[(bx * 2 + bz) * 6 + k, pl.ds(first, 16), :] for k in range(6)]
                for by in range(2):
                    o = bx * 4 + by * 2 + bz
                    ux, uy, uz, nx, ny, nz = [w[4 * by : 4 * by + 8] for w in wide]
                    sx, sy, sz, num = [s_ref[o * 4 + q, pl.ds(first, 8), :] for q in range(4)]
                    mx, my, mz = num * ux, num * uy, num * uz
                    wx, wy, wz = sx - mx, sy - my, sz - mz
                    along = (1.0 - ROT_COS) * (nx * wx + ny * wy + nz * wz)
                    acc[0] += mx + ROT_COS * wx + ROT_SIN * (ny * wz - nz * wy) + along * nx
                    acc[1] += my + ROT_COS * wy + ROT_SIN * (nz * wx - nx * wz) + along * ny
                    acc[2] += mz + ROT_COS * wz + ROT_SIN * (nx * wy - ny * wx) + along * nz
                    total += num
        inverse = 1.0 / jnp.maximum(total, 1.0)
        for c in range(3):
            vel_ref[c, pl.ds(first, 8), :] = acc[c] * inverse
        return carry

    lax.fori_loop(0, TILES // 8, group, 0)
    lane = iota((TILES, 128), 1)
    row = iota((TILES, 128), 0)
    for c in range(3):
        plane = vel_ref[c]
        for bit in range(4):
            size = 1 << bit
            row_bit = (row >> bit) & 1
            lane_bit = (lane >> bit) & 1
            down = sroll(lroll(plane, size), -size)
            up = sroll(lroll(plane, -size), size)
            plane = jnp.where(row_bit == lane_bit, plane, jnp.where(row_bit == 0, down, up))
        for part in range(8):
            send_ref[part, 16 * c : 16 * c + 16, :] = plane[16 * part : 16 * part + 16]


def collide_body(shift_ref, v_ref, p_ref, view_ref, out_ref, turn_ref):
    step = pl.program_id(0)
    cells = iota((TILE, TILE), 0)

    @pl.when(step == 0)
    def _():
        turn_ref[...] = jnp.zeros(turn_ref.shape, F32)

    def group(g, carry):
        place = p_ref[pl.ds(pl.multiple_of(g * 40, 8), 40), :]
        member = place >> 6
        octant = octants(place, shift_ref)
        first = pl.multiple_of((step * GROUPS + g) * 8, 8)
        for bx in range(2):
            for bz in range(2):
                for k in range(6):
                    wide = view_ref[(bx * 2 + bz) * 6 + k, pl.ds(first, 16), :]
                    for by in range(2):
                        o = bx * 4 + by * 2 + bz
                        turn_ref[pl.ds(8 * o + k, 8, stride=LROW), :] = wide[4 * by : 4 * by + 8]
        for t in range(8):
            high, low = split(turn_ref[LROW * t : LROW * t + 64, :])
            onehot = onehot_of(member, t, cells)
            picked = dot(
                jnp.concatenate([high, low], axis=1), jnp.concatenate([onehot, onehot], axis=0)
            )
            code = jnp.broadcast_to(tile_row(octant, t), (8, 640))
            chosen = picked[0:8]
            for o in range(1, 8):
                chosen = jnp.where(code == o, picked[8 * o : 8 * o + 8], chosen)
            speed = v_ref[:, pl.ds(pl.multiple_of(g * 5120 + t * 640, 128), 640)]
            ux, uy, uz, nx, ny, nz = [chosen[k : k + 1] for k in range(6)]
            wx, wy, wz = speed[0:1] - ux, speed[1:2] - uy, speed[2:3] - uz
            along = (1.0 - ROT_COS) * (nx * wx + ny * wy + nz * wz)
            new = [
                ux + ROT_COS * wx + ROT_SIN * (ny * wz - nz * wy) + along * nx,
                uy + ROT_COS * wy + ROT_SIN * (nz * wx - nx * wz) + along * ny,
                uz + ROT_COS * wz + ROT_SIN * (nx * wy - ny * wx) + along * nz,
            ]
            out_ref[:, pl.ds(pl.multiple_of(g * 5120 + t * 640, 128), 640)] = jnp.concatenate(
                new, axis=0
            )
        return carry

    lax.fori_loop(0, GROUPS, group, 0)


def table_parts(table):
    table = np.asarray(table, np.float32)
    high = table.astype(BF16)
    low = (table - high.astype(np.float32)).astype(BF16)
    return high, low


def z_tables():
    kz_high = np.arange(64)[:, None]
    pos = np.arange(NZ)[None, :]
    rows = []
    for q in range(4):
        phase = (2 * kz_high + q // 2) * pos % NZ * (2.0 * np.pi / NZ)
        rows.append(-np.sin(phase) if q % 2 else np.cos(phase))
    return table_parts(np.concatenate(rows, axis=0))


def y_tables():
    phase = np.arange(NY)[:, None] * np.arange(NY)[None, :] % NY * (2.0 * np.pi / NY)
    return table_parts(np.concatenate([np.cos(phase), np.sin(phase)], axis=0))


def x_tables():
    k = np.arange(512)
    lane = k % 128
    x = k // 128 * 32 + (lane & 3) * 8 + lane // 16
    kz = (lane >> 3) & 1
    part = (lane >> 2) & 1
    n = np.arange(512)
    part_out, kz_out, kx = n // 256, n // 128 % 2, n % 128
    phase = x[:, None] * kx[None, :] % NX * (2.0 * np.pi / NX)
    same = kz[:, None] == kz_out[None, :]
    c, s = np.cos(phase), np.sin(phase)
    real = np.where(part[:, None] == 0, c, s)
    imag = np.where(part[:, None] == 0, -s, c)
    table = np.where(part_out[None, :] == 0, real, imag) * same / math.sqrt(NX * NY * NZ)
    return table_parts(table)


def shell_counts():
    def wave(n):
        k = np.arange(n)
        return np.where(k >= n // 2, k - n, k)

    square = wave(NZ)[:, None, None] ** 2 + wave(NY)[None, :, None] ** 2 + wave(NX)[None, None, :] ** 2
    edges = np.arange(NSHELL + 1) ** 2
    below = np.searchsorted(np.sort(square.reshape(-1)), edges, side="left")
    return np.diff(below).astype(np.float32)


def z_body(in_ref, fh_ref, fl_ref, out_ref):
    lane = iota((64, 128), 1)
    fh, fl = fh_ref[...], fl_ref[...]
    for c in range(3):
        data = in_ref[:, 16 * c : 16 * c + 16, :].reshape(128, 128)
        high, low = split(data)
        res = dot(fh, high) + dot(fh, low) + dot(fl, high)
        g = [res[64 * q : 64 * q + 64] for q in range(4)]
        for bit, size in ((2, 8), (1, 4)):
            clear = (lane & size) == 0
            new = list(g)
            for q in range(4):
                if not q & bit:
                    a, b = g[q], g[q | bit]
                    new[q] = jnp.where(clear, a, lroll(b, size))
                    new[q | bit] = jnp.where(clear, lroll(a, -size), b)
            g = new
        for r in range(4):
            out_ref[pl.ds(4 * c + r, 64, stride=12), :] = g[r]


def y_body(in_ref, fh_ref, fl_ref, out_ref):
    both = in_ref[...].reshape(32, 24, 128)
    v0, v1, v2 = both[:, 0:8], both[:, 8:16], both[:, 16:24]
    upper = iota((32, 8, 128), 1) < 4
    d0 = jnp.where(upper, v0, v1)
    d1 = pltpu.roll(jnp.where(upper, v2, v0), 4, 1)
    d2 = jnp.where(upper, v1, v2)
    data = jnp.concatenate([d.reshape(256, 128) for d in (d0, d1, d2)], axis=1)
    high, low = split(data)
    fh, fl = fh_ref[...], fl_ref[...]
    res = dot(fh, high) + dot(fh, low) + dot(fl, high)
    is_real = (iota((256, 128), 1) & 4) == 0
    for c in range(3):
        even = res[0:256, 128 * c : 128 * c + 128]
        odd = res[256:512, 128 * c : 128 * c + 128]
        out = even + jnp.where(is_real, lroll(odd, -4), -lroll(odd, 4))
        for d in range(4):
            out_ref[d, 64 * c : 64 * c + 64, :] = out[64 * d : 64 * d + 64]


def x_body(first_ref, in_ref, fh_ref, fl_ref, out_ref, shell_ref, sums_ref):
    data = jnp.concatenate([in_ref[s] for s in range(4)], axis=1)
    high, low = split(data)
    fh, fl = fh_ref[...], fl_ref[...]
    res = dot(high, fh) + dot(low, fh) + dot(high, fl)
    ky = first_ref[1] + iota((64, 128), 0)
    ky = jnp.where(ky >= NY // 2, ky - NY, ky)
    kx = iota((64, 128), 1)
    kx = jnp.where(kx >= NX // 2, kx - NX, kx)
    plane = ky * ky + kx * kx
    energy, square = [], []
    for kz in range(2):
        total = jnp.zeros((64, 128), F32)
        for part in range(2):
            for c in range(3):
                block = res[64 * c : 64 * c + 64, 256 * part + 128 * kz : 256 * part + 128 * kz + 128]
                out_ref[part, c, kz] = block
                total += block * block
        wave = first_ref[0] + kz
        wave = jnp.where(wave >= NZ // 2, wave - NZ, wave)
        energy.append(total)
        square.append(plane + wave * wave)
    energy = jnp.concatenate(energy, axis=0)
    square = jnp.concatenate(square, axis=0)
    for s in range(NSHELL):
        kept = jnp.where(square < (s + 1) * (s + 1), energy, 0.0)
        sums_ref[s : s + 1, :] = jnp.sum(kept, axis=0, keepdims=True)
    cumulative = sums_ref[...]
    before = jnp.where(iota((NSHELL, 128), 0) == 0, 0.0, sroll(cumulative, 1))
    own = jnp.concatenate([cumulative - before, jnp.zeros((64, 128), F32)], axis=0)
    shell_ref[...] = jnp.sum(own.T, axis=0, keepdims=True)


def struct(*shape):
    return jax.ShapeDtypeStruct(shape, F32)


SMEM = pl.BlockSpec(memory_space=pltpu.SMEM)


def ring(x, axis):
    count = lax.axis_size(axis)
    forward = [(i, (i + 1) % count) for i in range(count)]
    backward = [(target, source) for source, target in forward]
    low, high = x
    return lax.ppermute(high, axis, forward), lax.ppermute(low, axis, backward)


def gathered_sum(x, axes):
    count = lax.axis_size(axes)
    copies = jnp.broadcast_to(x[None], (count, *x.shape))
    return jnp.sum(lax.all_to_all(copies, axes, split_axis=0, concat_axis=0, tiled=True), axis=0)


def params(mib):
    return pltpu.CompilerParams(vmem_limit_bytes=mib * 1024 * 1024)


def whole(*shape):
    return pl.BlockSpec(shape, lambda i: (0,) * len(shape))


def per_device(velocity, particle_place, grid_shift, rotation_axis):
    place = particle_place.reshape(640, 128)
    axis_index = rotation_axis.reshape(TILES, 128)
    span = TILES * TILE * PPC // BLOCKS
    speed_spec = pl.BlockSpec((3, span), lambda i: (0, i))
    place_spec = pl.BlockSpec((640 // BLOCKS, 128), lambda i: (i, 0))
    out_shapes = [(32, TILES, 128), (4, ROWS, 128), (3, TILES, 128)]
    out_shapes += [(40, 128)] * 4 + [(ROWS, 128)] * 2
    sums, main, normal, x_lo, x_hi, y_lo, y_hi, z_lo, z_hi = pl.pallas_call(
        scatter_body,
        name="scatter",
        grid=(BLOCKS,),
        in_specs=[SMEM, speed_spec, place_spec, whole(TILES, 128)],
        out_specs=[whole(*s) for s in out_shapes],
        out_shape=[struct(*s) for s in out_shapes],
        scratch_shapes=[
            pltpu.VMEM((8 * SROW, 128), F32),
            pltpu.VMEM((5, ROWS, 128), F32),
            pltpu.VMEM((1, ROWS, 128), F32),
        ],
        compiler_params=params(12),
    )(grid_shift, velocity, place, axis_index)
    below, above = ring((x_lo, x_hi), "gx")
    x_lo, x_hi, y_lo, y_hi = pl.pallas_call(
        fold_x_body, name="fold_x", out_shape=[struct(40, 128)] * 4, compiler_params=params(2)
    )(x_lo, x_hi, below, above, y_lo, y_hi)
    below, above = ring((y_lo, y_hi), GY)
    y_lo, y_hi, z_lo, z_hi = pl.pallas_call(
        fold_y_body, name="fold_y", out_shape=[struct(40, 128)] * 2 + [struct(ROWS, 128)] * 2,
        compiler_params=params(3),
    )(y_lo, y_hi, below, above, x_lo, x_hi, z_lo, z_hi)
    below, above = ring((z_lo, z_hi), GZ)
    views, sent = pl.pallas_call(
        cell_body,
        name="cells",
        out_shape=[struct(24, VROWS, 128), struct(8, 48, 128)],
        scratch_shapes=[
            pltpu.VMEM((7, ROWS, 128), F32),
            pltpu.VMEM((7, ROWS, 128), F32),
            pltpu.VMEM((3, TILES, 128), F32),
        ],
        compiler_params=params(12),
    )(sums, main, normal, x_lo, x_hi, y_lo, y_hi, z_lo, z_hi, below, above)
    arrived = lax.all_to_all(sent, GZ, split_axis=0, concat_axis=0, tiled=True)
    lines = pl.pallas_call(z_body, name="z_lines", out_shape=struct(768, 128), compiler_params=params(12))(
        arrived, *z_tables()
    )
    new_velocity = pl.pallas_call(
        collide_body,
        name="collide",
        grid=(BLOCKS,),
        in_specs=[SMEM, speed_spec, place_spec, whole(24, VROWS, 128)],
        out_specs=speed_spec,
        out_shape=struct(*velocity.shape),
        scratch_shapes=[pltpu.VMEM((8 * LROW, 128), F32)],
        compiler_params=params(12),
        cost_estimate=pl.CostEstimate(flops=6_000_000_000, bytes_accessed=4_000_000, transcendentals=0),
    )(grid_shift, velocity, place, views)
    pencil = lax.all_to_all(lines.reshape(64, 12, 128), GY_GZ, split_axis=0, concat_axis=0, tiled=True)
    pencil, new_velocity = lax.optimization_barrier((pencil, new_velocity))
    rows = pl.pallas_call(y_body, name="y_lines", out_shape=struct(4, 192, 128), compiler_params=params(12))(
        pencil.reshape(768, 128), *y_tables()
    )
    columns = lax.all_to_all(rows, "gx", split_axis=0, concat_axis=0, tiled=True)
    first = jnp.stack([lax.axis_index(GY_GZ) * 2, lax.axis_index("gx") * 64]).astype(jnp.int32)
    modes, shells = pl.pallas_call(
        x_body,
        name="x_lines",
        in_specs=[SMEM] + [pl.BlockSpec(memory_space=pltpu.VMEM)] * 3,
        out_shape=[struct(2, 3, 2, 64, 128), struct(1, 128)],
        scratch_shapes=[pltpu.VMEM((NSHELL, 128), F32)],
        compiler_params=params(12),
    )(first, columns, *x_tables())
    total = gathered_sum(gathered_sum(shells, GY_GZ), "gx")
    spectrum = total[0, :NSHELL] / shell_counts()
    return new_velocity, modes, spectrum


def solution(mesh):
    torus = Mesh(
        mesh.devices.reshape(mesh.shape["gx"], 4, 2, 2, 4), ("gx", "gy_0", "gy_1", "gz_0", "gz_1")
    )
    in_specs = (P(None, GX_GY_GZ), P(GX_GY_GZ), P(), P(GY, "gx", GZ))
    out_specs = (P(None, GX_GY_GZ), P(None, None, GY_GZ, "gx", None), P())
    return jax.shard_map(
        per_device, mesh=torus, in_specs=in_specs, out_specs=out_specs, check_vma=False
    )
```

```python
import math

import jax
import jax.numpy as jnp
import numpy as np
from jax import lax
from jax.experimental import pallas as pl
from jax.experimental.pallas import tpu as pltpu
from jax.sharding import Mesh
from jax.sharding import PartitionSpec as P

PPC = 5
TILE = 128
SUB = 4
NAXES = 1024
NSHELL = 64
NX, NY, NZ = 128, 256, 128
GX_GY_GZ = ("gx", "gy_0", "gy_1", "gz_0", "gz_1")
GY = ("gy_0", "gy_1")
GZ = ("gz_0", "gz_1")
GY_GZ = ("gy_0", "gy_1", "gz_0", "gz_1")
ROT_COS = math.cos(130.0 * math.pi / 180.0)
ROT_SIN = math.sin(130.0 * math.pi / 180.0)
F32 = jnp.float32
BF16 = jnp.bfloat16
TILES = 128
ROWS = 160
SROW = 36
LROW = 68
BLOCKS = 1
GROUPS = TILES // 8 // BLOCKS
STEPS = 8
EARLY = 4
PARTS = TILES // 8 // STEPS


def axis_vectors(axis_index):
    level = 1.0 - (2.0 * axis_index.astype(F32) + 1.0) / NAXES
    radius = jnp.sqrt(1.0 - level * level)
    whole_turns = (axis_index * 1597).astype(F32) * (1.0 / 2584.0)
    turn = (axis_index * 1597 - 2584 * jnp.floor(whole_turns).astype(jnp.int32)).astype(F32)
    turn = turn * (2.0 * math.pi / 2584.0)
    return radius * jnp.cos(turn), radius * jnp.sin(turn), level


def iota(shape, dim):
    return lax.broadcasted_iota(jnp.int32, shape, dim)


def lroll(x, amount):
    amount %= 128
    return pltpu.roll(x, amount, 1) if amount else x


def sroll(x, amount):
    return pltpu.roll(x, amount % x.shape[0], 0)


def split(x):
    high = x.astype(BF16)
    return high, (x - high.astype(F32)).astype(BF16)


def dot(a, b):
    return jnp.dot(a, b, preferred_element_type=F32)


def octants(place, shift_ref):
    bit_x = (((place >> 4) & 3) + shift_ref[0] >= SUB).astype(jnp.int32)
    bit_y = (((place >> 2) & 3) + shift_ref[1] >= SUB).astype(jnp.int32)
    bit_z = ((place & 3) + shift_ref[2] >= SUB).astype(jnp.int32)
    return bit_x * 4 + bit_y * 2 + bit_z


def tile_row(rows, t):
    return jnp.concatenate([rows[PPC * t + r : PPC * t + r + 1, :] for r in range(PPC)], axis=1)


def onehot_of(member, t, cells):
    return jnp.concatenate(
        [
            jnp.where(
                cells
                == jnp.broadcast_to(
                    member[PPC * t + r : PPC * t + r + 1, :], cells.shape
                ).astype(BF16),
                jnp.ones(cells.shape, BF16),
                jnp.zeros(cells.shape, BF16),
            )
            for r in range(PPC)
        ],
        axis=1,
    )


def scatter_body(shift_ref, v_ref, p_ref, axis_ref, s_ref, m_ref, n_ref, xlo_ref, xhi_ref, ylo_ref,
                 yhi_ref, zlo_ref, zhi_ref, turn_ref, edge_ref, zed_ref):
    step = pl.program_id(0)
    cells = iota((TILE, TILE), 0).astype(F32).astype(BF16)
    upper = iota((8, TILE), 0) < 4

    def group(g, carry):
        place = p_ref[pl.ds(pl.multiple_of(g * 40, 8), 40), :]
        member = (place >> 6).astype(F32)
        octant = octants(place, shift_ref)
        speed = v_ref[:, pl.ds(pl.multiple_of(g * 5120, 128), 5120)]
        high = speed.astype(BF16).astype(F32)
        low = speed - high
        one = jnp.ones((1, 640), F32)
        zero = jnp.zeros((1, 640), F32)
        for t in range(8):
            here = slice(t * 640, (t + 1) * 640)
            onehot = onehot_of(member, t, cells)
            code = jnp.broadcast_to(tile_row(octant, t), (8, 640))
            values = jnp.concatenate([high[:, here], one, low[:, here], zero], axis=0)
            weighted = jnp.concatenate(
                [jnp.where(code == o, values, 0.0) for o in range(8)], axis=0
            ).astype(BF16)
            sums = lax.dot_general(
                onehot, weighted, (((1,), (1,)), ((), ())), preferred_element_type=F32
            ).T
            for pair in range(4):
                even = sums[16 * pair : 16 * pair + 8]
                odd = sums[16 * pair + 8 : 16 * pair + 16]
                both = jnp.where(upper, even + sroll(even, 4), odd + sroll(odd, 4))
                turn_ref[SROW * t + 8 * pair : SROW * t + 8 * pair + 8, :] = both
        first = pl.multiple_of((step * GROUPS + g) * 8, 8)
        for r in range(32):
            s_ref[r, pl.ds(first, 8), :] = turn_ref[pl.ds(r, 8, stride=SROW), :]
        return carry

    lax.fori_loop(0, GROUPS, group, 0)

    @pl.when(step == BLOCKS - 1)
    def _():
        for c, part in enumerate(axis_vectors(axis_ref[...])):
            n_ref[c] = part
        lane = iota((TILES, 128), 1)
        row = iota((TILES, 128), 0)
        z = lane & 15
        x_in = lane >> 4
        x_out = row & 3
        last = (x_in == 7) & (x_out == 3)

        def x_shift(plane):
            rolled = lroll(plane, 16)
            return jnp.where(
                x_in > 0, rolled, jnp.where(x_out > 0, sroll(rolled, 1), 0.0)
            )

        for q in range(5):
            for by in range(2):
                parts = []
                for bx in range(2):
                    base = bx * 4 + by * 2
                    if q < 4:
                        above = s_ref[(base + 1) * 4 + q]
                        parts.append(
                            s_ref[base * 4 + q] + jnp.where(z > 0, lroll(above, 1), 0.0)
                        )
                    else:
                        rim = jnp.zeros((TILES, 128), F32)
                        for k in range(4):
                            rim = jnp.where(z == k, lroll(s_ref[(base + 1) * 4 + k], k - 15), rim)
                        parts.append(rim)
                main = parts[0] + x_shift(parts[1])
                edge = jnp.where(last, parts[1], 0.0)
                dst = m_ref if q < 4 else zed_ref
                at = q if q < 4 else 0
                if by == 0:
                    dst[at, 0:TILES, :] = main
                    dst[at, TILES:ROWS, :] = jnp.zeros((ROWS - TILES, 128), F32)
                    edge_ref[q, 0:TILES, :] = edge
                    edge_ref[q, TILES:ROWS, :] = jnp.zeros((ROWS - TILES, 128), F32)
                else:
                    dst[at, 4:132, :] = dst[at, 4:132, :] + main
                    edge_ref[q, 4:132, :] = edge_ref[q, 4:132, :] + edge
        lane40 = iota((40, 128), 1)
        low_face = jnp.zeros((40, 128), F32)
        high_face = jnp.zeros((40, 128), F32)
        for q in range(4):
            inside = (lane40 >> 4) == q
            low_face = jnp.where(inside, lroll(m_ref[q, pl.ds(0, 40, stride=4), :], 16 * q), low_face)
            high_face = jnp.where(
                inside, lroll(edge_ref[q, pl.ds(3, 40, stride=4), :], 16 * q - 112), high_face
            )
        inside = (lane40 >> 2) == 16
        low_face = jnp.where(inside, lroll(zed_ref[0, pl.ds(0, 40, stride=4), :], 64), low_face)
        high_face = jnp.where(inside, lroll(edge_ref[4, pl.ds(3, 40, stride=4), :], 64 - 112), high_face)
        for c in range(3):
            inside = ((lane40 >> 4) == 5 + c) & (iota((40, 128), 0) < 32)
            face = jnp.concatenate(
                [n_ref[c, pl.ds(0, 32, stride=4), :], jnp.zeros((8, 128), F32)], axis=0
            )
            low_face = jnp.where(inside, lroll(face, 80 + 16 * c), low_face)
        xlo_ref[...] = low_face
        xhi_ref[...] = high_face
        ylo_ref[...] = jnp.zeros((40, 128), F32)
        yhi_ref[...] = jnp.zeros((40, 128), F32)
        for q in range(5):
            src = m_ref if q < 4 else zed_ref
            at = q if q < 4 else 0
            ylo_ref[4 * q : 4 * q + 4, :] = src[at, 0:4, :]
            yhi_ref[4 * q : 4 * q + 4, :] = src[at, 128:132, :]
        for c in range(3):
            ylo_ref[20 + 4 * c : 24 + 4 * c, :] = n_ref[c, 0:4, :]
        big = iota((ROWS, 128), 1)
        slot = big & 15
        low_z = jnp.zeros((ROWS, 128), F32)
        for q in range(4):
            low_z = jnp.where(slot == q, lroll(m_ref[q], q), low_z)
        for c in range(3):
            face = jnp.concatenate([n_ref[c], jnp.zeros((ROWS - TILES, 128), F32)], axis=0)
            low_z = jnp.where(slot == 4 + c, lroll(face, 4 + c), low_z)
        zlo_ref[...] = low_z
        zhi_ref[...] = zed_ref[0]


def fold_x_body(xlo_ref, xhi_ref, from_low, from_high, ylo_ref, yhi_ref,
                xlo_out, xhi_out, ylo_out, yhi_out):
    low = xlo_ref[...] + from_low[...]
    high = xhi_ref[...] + from_high[...]
    xlo_out[...] = low
    xhi_out[...] = high
    lane = iota((1, 128), 1)
    for src, dst, y in ((ylo_ref, ylo_out, 0), (yhi_ref, yhi_out, 32)):
        dst[...] = src[...]
        for q in range(4):
            dst[4 * q : 4 * q + 1, :] = jnp.where(
                lane < 16, lroll(low[y : y + 1], -16 * q), src[4 * q : 4 * q + 1, :]
            )
        dst[16:17, :] = jnp.where(lane < 4, lroll(low[y : y + 1], -64), src[16:17, :])
        dst[32:33, :] = high[y : y + 1]


def fold_y_body(ylo_ref, yhi_ref, from_low, from_high, xlo_ref, xhi_ref, zlo_ref, zhi_ref,
                ylo_out, yhi_out, zlo_out, zhi_out):
    low = ylo_ref[...] + from_low[...]
    high = yhi_ref[...] + from_high[...]
    ylo_out[...] = low
    yhi_out[...] = high
    zlo_out[...] = zlo_ref[...]
    zhi_out[...] = zhi_ref[...]
    x_low = xlo_ref[...]
    x_high = xhi_ref[...]
    lane = iota((40, 128), 1)
    lo0 = zlo_out[pl.ds(0, 40, stride=4), :]
    hi0 = zhi_out[pl.ds(0, 40, stride=4), :]
    lo3 = zlo_out[pl.ds(3, 40, stride=4), :]
    hi3 = zhi_out[pl.ds(3, 40, stride=4), :]
    for q in range(4):
        lo0 = jnp.where(lane == q, lroll(x_low, q - 16 * q), lo0)
        lo3 = jnp.where(lane == 120 + q, lroll(x_high, 120 + q - 16 * q), lo3)
    for c in range(3):
        lo3 = jnp.where(lane == 124 + c, lroll(x_high, 124 + c - 80 - 16 * c), lo3)
    hi0 = jnp.where(lane < 4, lroll(x_low, -64), hi0)
    hi3 = jnp.where((lane >= 120) & (lane < 124), lroll(x_high, 120 - 64), hi3)
    zlo_out[pl.ds(0, 40, stride=4), :] = lo0
    zhi_out[pl.ds(0, 40, stride=4), :] = hi0
    zlo_out[pl.ds(3, 40, stride=4), :] = lo3
    zhi_out[pl.ds(3, 40, stride=4), :] = hi3
    lane4 = iota((4, 128), 1)
    slot = lane4 & 15
    corner = (iota((4, 128), 0) == 3) & (lane4 >= 120)
    for face, first in ((low, 0), (high, 128)):
        lo = jnp.zeros((4, 128), F32)
        for q in range(4):
            lo = jnp.where(slot == q, lroll(face[4 * q : 4 * q + 4], q), lo)
        for c in range(3):
            lo = jnp.where(slot == 4 + c, lroll(face[20 + 4 * c : 24 + 4 * c], 4 + c), lo)
        end = face[32:33]
        tail = jnp.zeros((1, 128), F32)
        lane1 = iota((1, 128), 1)
        for q in range(4):
            tail = jnp.where(lane1 == 120 + q, lroll(end, 120 + q - 16 * q), tail)
        for c in range(3):
            tail = jnp.where(lane1 == 124 + c, lroll(end, 124 + c - 80 - 16 * c), tail)
        zlo_out[first : first + 4, :] = jnp.where(corner, tail, lo)
        hi = jnp.where(slot < 4, face[16:20], 0.0)
        zhi_out[first : first + 4, :] = jnp.where(
            corner, jnp.where(lane1 < 124, lroll(end, 120 - 64), 0.0), hi
        )


VROWS = 136


def cell_body(s_ref, m_ref, n_ref, xlo_ref, xhi_ref, ylo_ref, yhi_ref, zlo_ref, zhi_ref,
              from_low, from_high, view_ref, send_ref, ext_ref, end_ref, vel_ref):
    z_low = zlo_ref[0:VROWS, :] + from_low[0:VROWS, :]
    z_high = zhi_ref[0:VROWS, :] + from_high[0:VROWS, :]
    x_low = xlo_ref[...]
    x_high = xhi_ref[...]
    y_low = ylo_ref[...]
    y_high = yhi_ref[...]
    lane40 = iota((40, 128), 1)
    lane = iota((VROWS, 128), 1)
    row = iota((VROWS, 128), 0)
    z = lane & 15
    x_in = lane >> 4
    x_out = row & 3
    for k in range(7):
        if k < 4:
            ext_ref[k] = m_ref[k]
            held = ext_ref[k, pl.ds(0, 40, stride=4), :]
            ext_ref[k, pl.ds(0, 40, stride=4), :] = jnp.where(
                lane40 < 16, lroll(x_low, -16 * k), held
            )
            ext_ref[k, 0:4, :] = y_low[4 * k : 4 * k + 4]
            ext_ref[k, 128:132, :] = y_high[4 * k : 4 * k + 4]
            amount = 112 - 16 * k
        else:
            c = k - 4
            ext_ref[k, 0:TILES, :] = n_ref[c]
            ext_ref[k, 128:132, :] = y_high[20 + 4 * c : 24 + 4 * c]
            amount = 32 - 16 * c
        end_ref[k, pl.ds(3, 40, stride=4), :] = lroll(x_high, amount)
        end_ref[k, 131:132, :] = lroll(y_high[32:33], amount)
        if k < 4:
            end_ref[k, 3:4, :] = lroll(y_low[32:33], amount)

    def pair(k):
        main = ext_ref[k, 0:VROWS, :]
        end = end_ref[k, 0:VROWS, :]
        if k < 4:
            main = jnp.where(z == 0, lroll(z_low, -k), main)
            end = jnp.where(z == 0, lroll(z_low, -8 - k), end)
        main1 = jnp.where(z < 15, lroll(main, -1), lroll(z_high, 15 - k))
        end1 = jnp.where(z < 15, lroll(end, -1), lroll(z_high, 7 - k))
        return (main, main1), (end, end1)

    count_main, count_end = pair(3)
    inv_main = [1.0 / jnp.maximum(a, 1.0) for a in count_main]
    inv_end = [1.0 / jnp.maximum(a, 1.0) for a in count_end]
    for slot, k in enumerate((0, 1, 2, 4, 5, 6)):
        mains, ends = pair(k)
        for bz in range(2):
            main, end = mains[bz], ends[bz]
            if k < 3:
                main = main * inv_main[bz]
                end = end * inv_end[bz]
            rolled = lroll(main, -16)
            ahead = jnp.where(x_in < 7, rolled, jnp.where(x_out == 3, end, sroll(rolled, -1)))
            view_ref[bz * 6 + slot] = main
            view_ref[(2 + bz) * 6 + slot] = ahead

    def group(g, carry):
        first = pl.multiple_of(g * 8, 8)
        acc = [jnp.zeros((8, 128), F32) for _ in range(3)]
        total = jnp.zeros((8, 128), F32)
        for bx in range(2):
            for bz in range(2):
                wide = [view_ref[(bx * 2 + bz) * 6 + k, pl.ds(first, 16), :] for k in range(6)]
                for by in range(2):
                    o = bx * 4 + by * 2 + bz
                    ux, uy, uz, nx, ny, nz = [w[4 * by : 4 * by + 8] for w in wide]
                    sx, sy, sz, num = [s_ref[o * 4 + q, pl.ds(first, 8), :] for q in range(4)]
                    mx, my, mz = num * ux, num * uy, num * uz
                    wx, wy, wz = sx - mx, sy - my, sz - mz
                    along = (1.0 - ROT_COS) * (nx * wx + ny * wy + nz * wz)
                    acc[0] += mx + ROT_COS * wx + ROT_SIN * (ny * wz - nz * wy) + along * nx
                    acc[1] += my + ROT_COS * wy + ROT_SIN * (nz * wx - nx * wz) + along * ny
                    acc[2] += mz + ROT_COS * wz + ROT_SIN * (nx * wy - ny * wx) + along * nz
                    total += num
        inverse = 1.0 / jnp.maximum(total, 1.0)
        for c in range(3):
            vel_ref[c, pl.ds(first, 8), :] = acc[c] * inverse
        return carry

    lax.fori_loop(0, TILES // 8, group, 0)
    lane = iota((TILES, 128), 1)
    row = iota((TILES, 128), 0)
    for c in range(3):
        plane = vel_ref[c]
        for bit in range(4):
            size = 1 << bit
            row_bit = (row >> bit) & 1
            lane_bit = (lane >> bit) & 1
            down = sroll(lroll(plane, size), -size)
            up = sroll(lroll(plane, -size), size)
            plane = jnp.where(row_bit == lane_bit, plane, jnp.where(row_bit == 0, down, up))
        for part in range(8):
            send_ref[part, 32 * c : 32 * c + 32, :] = plane[32 * (part % 4) : 32 * (part % 4) + 32]


def collide_body(start, shift_ref, v_ref, p_ref, view_ref, *refs):
    out_ref, turn_ref = refs[-2:]
    step = pl.program_id(0) + start
    cells = iota((TILE, TILE), 0).astype(F32).astype(BF16)

    @pl.when(step == start)
    def _():
        turn_ref[...] = jnp.zeros(turn_ref.shape, F32)

    def group(g, carry):
        place = p_ref[pl.ds(pl.multiple_of(g * 40, 8), 40), :]
        member = (place >> 6).astype(F32)
        octant = octants(place, shift_ref)
        first = pl.multiple_of((step * PARTS + g) * 8, 8)
        for bx in range(2):
            for bz in range(2):
                for k in range(6):
                    wide = view_ref[(bx * 2 + bz) * 6 + k, pl.ds(first, 16), :]
                    for by in range(2):
                        o = bx * 4 + by * 2 + bz
                        turn_ref[pl.ds(8 * o + k, 8, stride=LROW), :] = wide[4 * by : 4 * by + 8]
        for t in range(8):
            high, low = split(turn_ref[LROW * t : LROW * t + 64, :])
            onehot = onehot_of(member, t, cells)
            picked = dot(
                jnp.concatenate([high, low], axis=1), jnp.concatenate([onehot, onehot], axis=0)
            )
            code = jnp.broadcast_to(tile_row(octant, t), (8, 640))
            chosen = picked[0:8]
            for o in range(1, 8):
                chosen = jnp.where(code == o, picked[8 * o : 8 * o + 8], chosen)
            speed = v_ref[:, pl.ds(pl.multiple_of(g * 5120 + t * 640, 128), 640)]
            ux, uy, uz, nx, ny, nz = [chosen[k : k + 1] for k in range(6)]
            wx, wy, wz = speed[0:1] - ux, speed[1:2] - uy, speed[2:3] - uz
            along = (1.0 - ROT_COS) * (nx * wx + ny * wy + nz * wz)
            new = [
                ux + ROT_COS * wx + ROT_SIN * (ny * wz - nz * wy) + along * nx,
                uy + ROT_COS * wy + ROT_SIN * (nz * wx - nx * wz) + along * ny,
                uz + ROT_COS * wz + ROT_SIN * (nx * wy - ny * wx) + along * nz,
            ]
            out_ref[:, pl.ds(pl.multiple_of(g * 5120 + t * 640, 128), 640)] = jnp.concatenate(
                new, axis=0
            )
        return carry

    lax.fori_loop(0, PARTS, group, 0)


def table_parts(table):
    table = np.asarray(table, np.float32)
    high = table.astype(BF16)
    low = (table - high.astype(np.float32)).astype(BF16)
    return high, low


def z_tables():
    pos = np.arange(NZ)[None, :]
    line = np.arange(32)[:, None]
    halves = []
    for half in range(2):
        owner = line // 4 * 8 + half * 4 + line % 4
        for q in range(4):
            phase = (2 * owner + q // 2) * pos % NZ * (2.0 * np.pi / NZ)
            halves.append(-np.sin(phase) if q % 2 else np.cos(phase))
    return table_parts(np.concatenate(halves, axis=0).reshape(2, 128, NZ))


def y_tables():
    phase = np.arange(NY)[:, None] * np.arange(NY)[None, :] % NY * (2.0 * np.pi / NY)
    return table_parts(np.concatenate([np.cos(phase), np.sin(phase)], axis=0))


def x_tables():
    k = np.arange(512)
    lane = k % 128
    x = k // 128 * 32 + (lane & 3) * 8 + lane // 16
    kz = (lane >> 3) & 1
    part = (lane >> 2) & 1
    n = np.arange(512)
    part_out, kz_out, kx = n // 256, n // 128 % 2, n % 128
    phase = x[:, None] * kx[None, :] % NX * (2.0 * np.pi / NX)
    same = kz[:, None] == kz_out[None, :]
    c, s = np.cos(phase), np.sin(phase)
    real = np.where(part[:, None] == 0, c, s)
    imag = np.where(part[:, None] == 0, -s, c)
    table = np.where(part_out[None, :] == 0, real, imag) * same / math.sqrt(NX * NY * NZ)
    return table_parts(table)


def shell_counts():
    def wave(n):
        k = np.arange(n)
        return np.where(k >= n // 2, k - n, k)

    square = wave(NZ)[:, None, None] ** 2 + wave(NY)[None, :, None] ** 2 + wave(NX)[None, None, :] ** 2
    edges = np.arange(NSHELL + 1) ** 2
    below = np.searchsorted(np.sort(square.reshape(-1)), edges, side="left")
    return np.diff(below).astype(np.float32)


def z_body(first_ref, in_ref, fh_ref, fl_ref, out_ref):
    lane = iota((32, 128), 1)
    fh, fl = fh_ref[first_ref[2]], fl_ref[first_ref[2]]
    for c in range(3):
        data = jnp.concatenate(
            [
                in_ref[:, 32 * c + 16 * r : 32 * c + 16 * r + 16, :].reshape(128, 128)
                for r in range(2)
            ],
            axis=1,
        )
        high, low = split(data)
        res = dot(fh, high) + dot(fh, low) + dot(fl, high)
        for r in range(2):
            g = [res[32 * q : 32 * q + 32, 128 * r : 128 * r + 128] for q in range(4)]
            for bit, size in ((2, 8), (1, 4)):
                clear = (lane & size) == 0
                new = list(g)
                for q in range(4):
                    if not q & bit:
                        a, b = g[q], g[q | bit]
                        new[q] = jnp.where(clear, a, lroll(b, size))
                        new[q | bit] = jnp.where(clear, lroll(a, -size), b)
                g = new
            for k in range(4):
                out_ref[pl.ds(8 * c + 4 * r + k, 32, stride=24), :] = g[k]


def y_body(in_ref, fh_ref, fl_ref, out_ref):
    both = in_ref[...].reshape(32, 24, 128)
    data = jnp.concatenate(
        [both[:, 8 * c : 8 * c + 8].reshape(256, 128) for c in range(3)], axis=1
    )
    high, low = split(data)
    fh, fl = fh_ref[...], fl_ref[...]
    res = dot(fh, high) + dot(fh, low) + dot(fl, high)
    is_real = (iota((256, 128), 1) & 4) == 0
    for c in range(3):
        even = res[0:256, 128 * c : 128 * c + 128]
        odd = res[256:512, 128 * c : 128 * c + 128]
        out = even + jnp.where(is_real, lroll(odd, -4), -lroll(odd, 4))
        for d in range(4):
            out_ref[d, 64 * c : 64 * c + 64, :] = out[64 * d : 64 * d + 64]
            out_ref[d, 192 + 64 * c : 256 + 64 * c, :] = out[0:64]


def x_body(first_ref, in_ref, fh_ref, fl_ref, out_ref, shell_ref, sums_ref):
    data = jnp.concatenate([in_ref[s] for s in range(4)], axis=1)
    high, low = split(data)
    fh, fl = fh_ref[...], fl_ref[...]
    res = dot(high, fh) + dot(low, fh) + dot(high, fl)
    ky = iota((64, 128), 0)
    kx = iota((64, 128), 1)
    kx = jnp.where(kx >= NX // 2, kx - NX, kx)
    plane = ky * ky + kx * kx
    weight = jnp.where(ky == 0, 1.0, 2.0)
    energy, square = [], []
    for kz in range(2):
        total = jnp.zeros((64, 128), F32)
        for part in range(2):
            for c in range(3):
                here = slice(256 * part + 128 * kz, 256 * part + 128 * kz + 128)
                out_ref[part, c, kz] = res[64 * c : 64 * c + 64, here]
                block = res[192 + 64 * c : 256 + 64 * c, here]
                total += block * block
        wave = first_ref[0] + kz
        wave = jnp.where(wave >= NZ // 2, wave - NZ, wave)
        energy.append(total * weight)
        square.append(plane + wave * wave)
    energy = jnp.concatenate(energy, axis=0)
    square = jnp.concatenate(square, axis=0)
    for s in range(NSHELL):
        kept = jnp.where(square < (s + 1) * (s + 1), energy, 0.0)
        sums_ref[s : s + 1, :] = jnp.sum(kept, axis=0, keepdims=True)
    cumulative = sums_ref[...]
    before = jnp.where(iota((NSHELL, 128), 0) == 0, 0.0, sroll(cumulative, 1))
    own = jnp.concatenate([cumulative - before, jnp.zeros((64, 128), F32)], axis=0)
    shell_ref[...] = jnp.sum(own.T, axis=0, keepdims=True)


def struct(*shape):
    return jax.ShapeDtypeStruct(shape, F32)


SMEM = pl.BlockSpec(memory_space=pltpu.SMEM)


def ring(x, axis):
    count = lax.axis_size(axis)
    forward = [(i, (i + 1) % count) for i in range(count)]
    backward = [(target, source) for source, target in forward]
    low, high = x
    return lax.ppermute(high, axis, forward), lax.ppermute(low, axis, backward)


def gathered_sum(x, axes):
    count = lax.axis_size(axes)
    copies = jnp.broadcast_to(x[None], (count, *x.shape))
    return jnp.sum(lax.all_to_all(copies, axes, split_axis=0, concat_axis=0, tiled=True), axis=0)


def params(mib):
    return pltpu.CompilerParams(vmem_limit_bytes=mib * 1024 * 1024)


def whole(*shape):
    return pl.BlockSpec(shape, lambda i: (0,) * len(shape))


def collide(start, stop, grid_shift, velocity, place, views, earlier):
    span = TILES * TILE * PPC // STEPS
    speed_spec = pl.BlockSpec((3, span), lambda i: (0, i + start))
    place_spec = pl.BlockSpec((640 // STEPS, 128), lambda i: (i + start, 0))
    more = [] if earlier is None else [earlier]
    return pl.pallas_call(
        lambda *refs: collide_body(start, *refs),
        name="collide",
        grid=(stop - start,),
        in_specs=[SMEM, speed_spec, place_spec, whole(24, VROWS, 128)]
        + [pl.BlockSpec(memory_space=pl.ANY)] * len(more),
        out_specs=speed_spec,
        out_shape=struct(*velocity.shape),
        scratch_shapes=[pltpu.VMEM((8 * LROW, 128), F32)],
        input_output_aliases={4: 0} if more else {},
        compiler_params=params(12),
        cost_estimate=pl.CostEstimate(
            flops=800_000_000 * (stop - start), bytes_accessed=4_000_000, transcendentals=0
        ),
    )(grid_shift, velocity, place, views, *more)


def per_device(velocity, particle_place, grid_shift, rotation_axis):
    place = particle_place.reshape(640, 128)
    axis_index = rotation_axis.reshape(TILES, 128)
    span = TILES * TILE * PPC // BLOCKS
    speed_spec = pl.BlockSpec((3, span), lambda i: (0, i))
    place_spec = pl.BlockSpec((640 // BLOCKS, 128), lambda i: (i, 0))
    out_shapes = [(32, TILES, 128), (4, ROWS, 128), (3, TILES, 128)]
    out_shapes += [(40, 128)] * 4 + [(ROWS, 128)] * 2
    sums, main, normal, x_lo, x_hi, y_lo, y_hi, z_lo, z_hi = pl.pallas_call(
        scatter_body,
        name="scatter",
        grid=(BLOCKS,),
        in_specs=[SMEM, speed_spec, place_spec, whole(TILES, 128)],
        out_specs=[whole(*s) for s in out_shapes],
        out_shape=[struct(*s) for s in out_shapes],
        scratch_shapes=[
            pltpu.VMEM((8 * SROW, 128), F32),
            pltpu.VMEM((5, ROWS, 128), F32),
            pltpu.VMEM((1, ROWS, 128), F32),
        ],
        compiler_params=params(12),
    )(grid_shift, velocity, place, axis_index)
    below, above = ring((x_lo, x_hi), "gx")
    x_lo, x_hi, y_lo, y_hi = pl.pallas_call(
        fold_x_body, name="fold_x", out_shape=[struct(40, 128)] * 4, compiler_params=params(2)
    )(x_lo, x_hi, below, above, y_lo, y_hi)
    below, above = ring((y_lo, y_hi), GY)
    y_lo, y_hi, z_lo, z_hi = pl.pallas_call(
        fold_y_body, name="fold_y", out_shape=[struct(40, 128)] * 2 + [struct(ROWS, 128)] * 2,
        compiler_params=params(3),
    )(y_lo, y_hi, below, above, x_lo, x_hi, z_lo, z_hi)
    below, above = ring((z_lo, z_hi), GZ)
    views, sent = pl.pallas_call(
        cell_body,
        name="cells",
        out_shape=[struct(24, VROWS, 128), struct(8, 96, 128)],
        scratch_shapes=[
            pltpu.VMEM((7, ROWS, 128), F32),
            pltpu.VMEM((7, ROWS, 128), F32),
            pltpu.VMEM((3, TILES, 128), F32),
        ],
        compiler_params=params(12),
    )(sums, main, normal, x_lo, x_hi, y_lo, y_hi, z_lo, z_hi, below, above)
    first = jnp.stack(
        [lax.axis_index(GY_GZ) * 2, lax.axis_index("gx") * 64, lax.axis_index("gz_0")]
    ).astype(jnp.int32)
    arrived = lax.all_to_all(sent, GZ, split_axis=0, concat_axis=0, tiled=True)
    updated = collide(0, EARLY, grid_shift, velocity, place, views, None)
    arrived, updated = lax.optimization_barrier((arrived, updated))
    vmem = pl.BlockSpec(memory_space=pltpu.VMEM)
    lines = pl.pallas_call(
        z_body,
        name="z_lines",
        in_specs=[SMEM, vmem, vmem, vmem],
        out_shape=struct(768, 128),
        compiler_params=params(6),
    )(first, arrived, *z_tables())
    pencil = lax.all_to_all(
        lines.reshape(32, 24, 128), ("gy_0", "gy_1", "gz_1"), split_axis=0, concat_axis=0, tiled=True
    )
    new_velocity = collide(EARLY, STEPS, grid_shift, velocity, place, views, updated)
    pencil, new_velocity = lax.optimization_barrier((pencil, new_velocity))
    rows = pl.pallas_call(y_body, name="y_lines", out_shape=struct(4, 384, 128), compiler_params=params(12))(
        pencil.reshape(768, 128), *y_tables()
    )
    columns = lax.all_to_all(rows, "gx", split_axis=0, concat_axis=0, tiled=True)
    modes, shells = pl.pallas_call(
        x_body,
        name="x_lines",
        in_specs=[SMEM, vmem, vmem, vmem],
        out_shape=[struct(2, 3, 2, 64, 128), struct(1, 128)],
        scratch_shapes=[pltpu.VMEM((NSHELL, 128), F32)],
        compiler_params=params(12),
    )(first, columns, *x_tables())
    total = gathered_sum(shells, GY_GZ)
    spectrum = total[0, :NSHELL] / shell_counts()
    return new_velocity, modes, spectrum


def solution(mesh):
    torus = Mesh(
        mesh.devices.reshape(mesh.shape["gx"], 4, 2, 2, 4), ("gx", "gy_0", "gy_1", "gz_0", "gz_1")
    )
    in_specs = (P(None, GX_GY_GZ), P(GX_GY_GZ), P(), P(GY, "gx", GZ))
    out_specs = (P(None, GX_GY_GZ), P(None, None, GY_GZ, "gx", None), P())
    return jax.shard_map(
        per_device, mesh=torus, in_specs=in_specs, out_specs=out_specs, check_vma=False
    )
```

```python
import math

import jax
import jax.numpy as jnp
import numpy as np
from jax import lax
from jax.experimental import pallas as pl
from jax.experimental.pallas import tpu as pltpu
from jax.sharding import Mesh
from jax.sharding import PartitionSpec as P

PPC = 5
TILE = 128
SUB = 4
NAXES = 1024
NSHELL = 64
NX, NY, NZ = 128, 256, 128
GX_GY_GZ = ("gx", "gy_0", "gy_1", "gz_0", "gz_1")
GY = ("gy_0", "gy_1")
GZ = ("gz_0", "gz_1")
GY_GZ = ("gy_0", "gy_1", "gz_0", "gz_1")
ROT_COS = math.cos(130.0 * math.pi / 180.0)
ROT_SIN = math.sin(130.0 * math.pi / 180.0)
F32 = jnp.float32
BF16 = jnp.bfloat16
TILES = 128
ROWS = 160
SROW = 36
LROW = 68
BLOCKS = 1
GROUPS = TILES // 8 // BLOCKS
STEPS = 8
EARLY = 6
PARTS = TILES // 8 // STEPS


def axis_vectors(axis_index):
    level = 1.0 - (2.0 * axis_index.astype(F32) + 1.0) / NAXES
    radius = jnp.sqrt(1.0 - level * level)
    whole_turns = (axis_index * 1597).astype(F32) * (1.0 / 2584.0)
    turn = (axis_index * 1597 - 2584 * jnp.floor(whole_turns).astype(jnp.int32)).astype(F32)
    turn = turn * (2.0 * math.pi / 2584.0)
    return radius * jnp.cos(turn), radius * jnp.sin(turn), level


def iota(shape, dim):
    return lax.broadcasted_iota(jnp.int32, shape, dim)


def lroll(x, amount):
    amount %= 128
    return pltpu.roll(x, amount, 1) if amount else x


def sroll(x, amount):
    return pltpu.roll(x, amount % x.shape[0], 0)


def split(x):
    high = x.astype(BF16)
    return high, (x - high.astype(F32)).astype(BF16)


def dot(a, b):
    return jnp.dot(a, b, preferred_element_type=F32)


def octants(place, shift_ref):
    bit_x = (((place >> 4) & 3) + shift_ref[0] >= SUB).astype(jnp.int32)
    bit_y = (((place >> 2) & 3) + shift_ref[1] >= SUB).astype(jnp.int32)
    bit_z = ((place & 3) + shift_ref[2] >= SUB).astype(jnp.int32)
    return bit_x * 4 + bit_y * 2 + bit_z


def tile_row(rows, t):
    return jnp.concatenate([rows[PPC * t + r : PPC * t + r + 1, :] for r in range(PPC)], axis=1)


def onehot_of(member, t, cells):
    return jnp.concatenate(
        [
            jnp.where(
                cells
                == jnp.broadcast_to(
                    member[PPC * t + r : PPC * t + r + 1, :], cells.shape
                ).astype(BF16),
                jnp.ones(cells.shape, BF16),
                jnp.zeros(cells.shape, BF16),
            )
            for r in range(PPC)
        ],
        axis=1,
    )


def scatter_body(shift_ref, v_ref, p_ref, axis_ref, s_ref, n_ref, xlo_ref, xhi_ref, turn_ref):
    step = pl.program_id(0)
    cells = iota((TILE, TILE), 0).astype(F32).astype(BF16)
    upper = iota((8, TILE), 0) < 4

    def group(g, carry):
        place = p_ref[pl.ds(pl.multiple_of(g * 40, 8), 40), :]
        member = (place >> 6).astype(F32)
        octant = octants(place, shift_ref)
        speed = v_ref[:, pl.ds(pl.multiple_of(g * 5120, 128), 5120)]
        high = speed.astype(BF16).astype(F32)
        low = speed - high
        one = jnp.ones((1, 640), F32)
        zero = jnp.zeros((1, 640), F32)
        for t in range(8):
            here = slice(t * 640, (t + 1) * 640)
            onehot = onehot_of(member, t, cells)
            code = jnp.broadcast_to(tile_row(octant, t), (8, 640))
            values = jnp.concatenate([high[:, here], one, low[:, here], zero], axis=0)
            weighted = jnp.concatenate(
                [jnp.where(code == o, values, 0.0) for o in range(8)], axis=0
            ).astype(BF16)
            sums = lax.dot_general(
                onehot, weighted, (((1,), (1,)), ((), ())), preferred_element_type=F32
            ).T
            for pair in range(4):
                even = sums[16 * pair : 16 * pair + 8]
                odd = sums[16 * pair + 8 : 16 * pair + 16]
                both = jnp.where(upper, even + sroll(even, 4), odd + sroll(odd, 4))
                turn_ref[SROW * t + 8 * pair : SROW * t + 8 * pair + 8, :] = both
        first = pl.multiple_of((step * GROUPS + g) * 8, 8)
        for r in range(32):
            s_ref[r, pl.ds(first, 8), :] = turn_ref[pl.ds(r, 8, stride=SROW), :]
        return carry

    lax.fori_loop(0, GROUPS, group, 0)

    @pl.when(step == BLOCKS - 1)
    def _():
        for c, part in enumerate(axis_vectors(axis_ref[...])):
            n_ref[c] = part
        z = iota((32, 128), 1) & 15
        lane = iota((40, 128), 1)
        pad = jnp.zeros((8, 128), F32)
        low_face = jnp.zeros((40, 128), F32)
        high_face = jnp.zeros((40, 128), F32)
        for q in range(5):
            faces = []
            for bx in range(2):
                parts = []
                for by in range(2):
                    base = bx * 4 + by * 2
                    rows = pl.ds(3 * bx, 32, stride=4)
                    if q < 4:
                        above = s_ref[(base + 1) * 4 + q, rows, :]
                        part = s_ref[base * 4 + q, rows, :] + jnp.where(z > 0, lroll(above, 1), 0.0)
                    else:
                        part = jnp.zeros((32, 128), F32)
                        for k in range(4):
                            above = s_ref[(base + 1) * 4 + k, rows, :]
                            part = jnp.where(z == k, lroll(above, k - 15), part)
                    parts.append(jnp.concatenate([part, pad], axis=0))
                faces.append(parts[0] + sroll(parts[1], 1))
            inside = (lane >> 4) == q if q < 4 else (lane >> 2) == 16
            low_face = jnp.where(inside, lroll(faces[0], 16 * q), low_face)
            high_face = jnp.where(inside, lroll(faces[1], 16 * q - 112), high_face)
        for c in range(3):
            inside = ((lane >> 4) == 5 + c) & (iota((40, 128), 0) < 32)
            face = jnp.concatenate([n_ref[c, pl.ds(0, 32, stride=4), :], pad], axis=0)
            low_face = jnp.where(inside, lroll(face, 80 + 16 * c), low_face)
        xlo_ref[...] = low_face
        xhi_ref[...] = high_face


def plane_body(s_ref, n_ref, m_ref, ylo_ref, yhi_ref, zlo_ref, zhi_ref, edge_ref, zed_ref):
    lane = iota((TILES, 128), 1)
    row = iota((TILES, 128), 0)
    z = lane & 15
    x_in = lane >> 4
    x_out = row & 3
    last = (x_in == 7) & (x_out == 3)

    def x_shift(plane):
        rolled = lroll(plane, 16)
        return jnp.where(
            x_in > 0, rolled, jnp.where(x_out > 0, sroll(rolled, 1), 0.0)
        )

    for q in range(5):
        for by in range(2):
            parts = []
            for bx in range(2):
                base = bx * 4 + by * 2
                if q < 4:
                    above = s_ref[(base + 1) * 4 + q]
                    parts.append(
                        s_ref[base * 4 + q] + jnp.where(z > 0, lroll(above, 1), 0.0)
                    )
                else:
                    rim = jnp.zeros((TILES, 128), F32)
                    for k in range(4):
                        rim = jnp.where(z == k, lroll(s_ref[(base + 1) * 4 + k], k - 15), rim)
                    parts.append(rim)
            main = parts[0] + x_shift(parts[1])
            edge = jnp.where(last, parts[1], 0.0)
            dst = m_ref if q < 4 else zed_ref
            at = q if q < 4 else 0
            if by == 0:
                dst[at, 0:TILES, :] = main
                dst[at, TILES:ROWS, :] = jnp.zeros((ROWS - TILES, 128), F32)
                edge_ref[q, 0:TILES, :] = edge
                edge_ref[q, TILES:ROWS, :] = jnp.zeros((ROWS - TILES, 128), F32)
            else:
                dst[at, 4:132, :] = dst[at, 4:132, :] + main
                edge_ref[q, 4:132, :] = edge_ref[q, 4:132, :] + edge
    ylo_ref[...] = jnp.zeros((40, 128), F32)
    yhi_ref[...] = jnp.zeros((40, 128), F32)
    for q in range(5):
        src = m_ref if q < 4 else zed_ref
        at = q if q < 4 else 0
        ylo_ref[4 * q : 4 * q + 4, :] = src[at, 0:4, :]
        yhi_ref[4 * q : 4 * q + 4, :] = src[at, 128:132, :]
    for c in range(3):
        ylo_ref[20 + 4 * c : 24 + 4 * c, :] = n_ref[c, 0:4, :]
    big = iota((ROWS, 128), 1)
    slot = big & 15
    low_z = jnp.zeros((ROWS, 128), F32)
    for q in range(4):
        low_z = jnp.where(slot == q, lroll(m_ref[q], q), low_z)
    for c in range(3):
        face = jnp.concatenate([n_ref[c], jnp.zeros((ROWS - TILES, 128), F32)], axis=0)
        low_z = jnp.where(slot == 4 + c, lroll(face, 4 + c), low_z)
    zlo_ref[...] = low_z
    zhi_ref[...] = zed_ref[0]


def fold_x_body(xlo_ref, xhi_ref, from_low, from_high, ylo_ref, yhi_ref,
                xlo_out, xhi_out, ylo_out, yhi_out):
    low = xlo_ref[...] + from_low[...]
    high = xhi_ref[...] + from_high[...]
    xlo_out[...] = low
    xhi_out[...] = high
    lane = iota((1, 128), 1)
    for src, dst, y in ((ylo_ref, ylo_out, 0), (yhi_ref, yhi_out, 32)):
        dst[...] = src[...]
        for q in range(4):
            dst[4 * q : 4 * q + 1, :] = jnp.where(
                lane < 16, lroll(low[y : y + 1], -16 * q), src[4 * q : 4 * q + 1, :]
            )
        dst[16:17, :] = jnp.where(lane < 4, lroll(low[y : y + 1], -64), src[16:17, :])
        dst[32:33, :] = high[y : y + 1]


def fold_y_body(ylo_ref, yhi_ref, from_low, from_high, xlo_ref, xhi_ref, zlo_ref, zhi_ref,
                ylo_out, yhi_out, zlo_out, zhi_out):
    low = ylo_ref[...] + from_low[...]
    high = yhi_ref[...] + from_high[...]
    ylo_out[...] = low
    yhi_out[...] = high
    zlo_out[...] = zlo_ref[...]
    zhi_out[...] = zhi_ref[...]
    x_low = xlo_ref[...]
    x_high = xhi_ref[...]
    lane = iota((40, 128), 1)
    lo0 = zlo_out[pl.ds(0, 40, stride=4), :]
    hi0 = zhi_out[pl.ds(0, 40, stride=4), :]
    lo3 = zlo_out[pl.ds(3, 40, stride=4), :]
    hi3 = zhi_out[pl.ds(3, 40, stride=4), :]
    for q in range(4):
        lo0 = jnp.where(lane == q, lroll(x_low, q - 16 * q), lo0)
        lo3 = jnp.where(lane == 120 + q, lroll(x_high, 120 + q - 16 * q), lo3)
    for c in range(3):
        lo3 = jnp.where(lane == 124 + c, lroll(x_high, 124 + c - 80 - 16 * c), lo3)
    hi0 = jnp.where(lane < 4, lroll(x_low, -64), hi0)
    hi3 = jnp.where((lane >= 120) & (lane < 124), lroll(x_high, 120 - 64), hi3)
    zlo_out[pl.ds(0, 40, stride=4), :] = lo0
    zhi_out[pl.ds(0, 40, stride=4), :] = hi0
    zlo_out[pl.ds(3, 40, stride=4), :] = lo3
    zhi_out[pl.ds(3, 40, stride=4), :] = hi3
    lane4 = iota((4, 128), 1)
    slot = lane4 & 15
    corner = (iota((4, 128), 0) == 3) & (lane4 >= 120)
    for face, first in ((low, 0), (high, 128)):
        lo = jnp.zeros((4, 128), F32)
        for q in range(4):
            lo = jnp.where(slot == q, lroll(face[4 * q : 4 * q + 4], q), lo)
        for c in range(3):
            lo = jnp.where(slot == 4 + c, lroll(face[20 + 4 * c : 24 + 4 * c], 4 + c), lo)
        end = face[32:33]
        tail = jnp.zeros((1, 128), F32)
        lane1 = iota((1, 128), 1)
        for q in range(4):
            tail = jnp.where(lane1 == 120 + q, lroll(end, 120 + q - 16 * q), tail)
        for c in range(3):
            tail = jnp.where(lane1 == 124 + c, lroll(end, 124 + c - 80 - 16 * c), tail)
        zlo_out[first : first + 4, :] = jnp.where(corner, tail, lo)
        hi = jnp.where(slot < 4, face[16:20], 0.0)
        zhi_out[first : first + 4, :] = jnp.where(
            corner, jnp.where(lane1 < 124, lroll(end, 120 - 64), 0.0), hi
        )


VROWS = 136


def cell_body(s_ref, m_ref, n_ref, xlo_ref, xhi_ref, ylo_ref, yhi_ref, zlo_ref, zhi_ref,
              from_low, from_high, view_ref, send_ref, ext_ref, end_ref, vel_ref):
    z_low = zlo_ref[0:VROWS, :] + from_low[0:VROWS, :]
    z_high = zhi_ref[0:VROWS, :] + from_high[0:VROWS, :]
    x_low = xlo_ref[...]
    x_high = xhi_ref[...]
    y_low = ylo_ref[...]
    y_high = yhi_ref[...]
    lane40 = iota((40, 128), 1)
    lane = iota((VROWS, 128), 1)
    row = iota((VROWS, 128), 0)
    z = lane & 15
    x_in = lane >> 4
    x_out = row & 3
    for k in range(7):
        if k < 4:
            ext_ref[k] = m_ref[k]
            held = ext_ref[k, pl.ds(0, 40, stride=4), :]
            ext_ref[k, pl.ds(0, 40, stride=4), :] = jnp.where(
                lane40 < 16, lroll(x_low, -16 * k), held
            )
            ext_ref[k, 0:4, :] = y_low[4 * k : 4 * k + 4]
            ext_ref[k, 128:132, :] = y_high[4 * k : 4 * k + 4]
            amount = 112 - 16 * k
        else:
            c = k - 4
            ext_ref[k, 0:TILES, :] = n_ref[c]
            ext_ref[k, 128:132, :] = y_high[20 + 4 * c : 24 + 4 * c]
            amount = 32 - 16 * c
        end_ref[k, pl.ds(3, 40, stride=4), :] = lroll(x_high, amount)
        end_ref[k, 131:132, :] = lroll(y_high[32:33], amount)
        if k < 4:
            end_ref[k, 3:4, :] = lroll(y_low[32:33], amount)

    def pair(k):
        main = ext_ref[k, 0:VROWS, :]
        end = end_ref[k, 0:VROWS, :]
        if k < 4:
            main = jnp.where(z == 0, lroll(z_low, -k), main)
            end = jnp.where(z == 0, lroll(z_low, -8 - k), end)
        main1 = jnp.where(z < 15, lroll(main, -1), lroll(z_high, 15 - k))
        end1 = jnp.where(z < 15, lroll(end, -1), lroll(z_high, 7 - k))
        return (main, main1), (end, end1)

    count_main, count_end = pair(3)
    inv_main = [1.0 / jnp.maximum(a, 1.0) for a in count_main]
    inv_end = [1.0 / jnp.maximum(a, 1.0) for a in count_end]
    for slot, k in enumerate((0, 1, 2, 4, 5, 6)):
        mains, ends = pair(k)
        for bz in range(2):
            main, end = mains[bz], ends[bz]
            if k < 3:
                main = main * inv_main[bz]
                end = end * inv_end[bz]
            rolled = lroll(main, -16)
            ahead = jnp.where(x_in < 7, rolled, jnp.where(x_out == 3, end, sroll(rolled, -1)))
            view_ref[bz * 6 + slot] = main
            view_ref[(2 + bz) * 6 + slot] = ahead

    def group(g, carry):
        first = pl.multiple_of(g * 8, 8)
        acc = [jnp.zeros((8, 128), F32) for _ in range(3)]
        total = jnp.zeros((8, 128), F32)
        for bx in range(2):
            for bz in range(2):
                wide = [view_ref[(bx * 2 + bz) * 6 + k, pl.ds(first, 16), :] for k in range(6)]
                for by in range(2):
                    o = bx * 4 + by * 2 + bz
                    ux, uy, uz, nx, ny, nz = [w[4 * by : 4 * by + 8] for w in wide]
                    sx, sy, sz, num = [s_ref[o * 4 + q, pl.ds(first, 8), :] for q in range(4)]
                    mx, my, mz = num * ux, num * uy, num * uz
                    wx, wy, wz = sx - mx, sy - my, sz - mz
                    along = (1.0 - ROT_COS) * (nx * wx + ny * wy + nz * wz)
                    acc[0] += mx + ROT_COS * wx + ROT_SIN * (ny * wz - nz * wy) + along * nx
                    acc[1] += my + ROT_COS * wy + ROT_SIN * (nz * wx - nx * wz) + along * ny
                    acc[2] += mz + ROT_COS * wz + ROT_SIN * (nx * wy - ny * wx) + along * nz
                    total += num
        inverse = 1.0 / jnp.maximum(total, 1.0)
        for c in range(3):
            vel_ref[c, pl.ds(first, 8), :] = acc[c] * inverse
        return carry

    lax.fori_loop(0, TILES // 8, group, 0)
    lane = iota((TILES, 128), 1)
    row = iota((TILES, 128), 0)
    for c in range(3):
        plane = vel_ref[c]
        for bit in range(4):
            size = 1 << bit
            row_bit = (row >> bit) & 1
            lane_bit = (lane >> bit) & 1
            down = sroll(lroll(plane, size), -size)
            up = sroll(lroll(plane, -size), size)
            plane = jnp.where(row_bit == lane_bit, plane, jnp.where(row_bit == 0, down, up))
        for part in range(8):
            send_ref[part, 64 * c : 64 * c + 64, :] = plane[64 * (part // 4) : 64 * (part // 4) + 64]


def collide_body(start, shift_ref, v_ref, p_ref, view_ref, *refs):
    out_ref, turn_ref = refs[-2:]
    step = pl.program_id(0) + start
    cells = iota((TILE, TILE), 0).astype(F32).astype(BF16)

    @pl.when(step == start)
    def _():
        turn_ref[...] = jnp.zeros(turn_ref.shape, F32)

    def group(g, carry):
        place = p_ref[pl.ds(pl.multiple_of(g * 40, 8), 40), :]
        member = (place >> 6).astype(F32)
        octant = octants(place, shift_ref)
        first = pl.multiple_of((step * PARTS + g) * 8, 8)
        for bx in range(2):
            for bz in range(2):
                for k in range(6):
                    wide = view_ref[(bx * 2 + bz) * 6 + k, pl.ds(first, 16), :]
                    for by in range(2):
                        o = bx * 4 + by * 2 + bz
                        turn_ref[pl.ds(8 * o + k, 8, stride=LROW), :] = wide[4 * by : 4 * by + 8]
        for t in range(8):
            high, low = split(turn_ref[LROW * t : LROW * t + 64, :])
            onehot = onehot_of(member, t, cells)
            picked = dot(
                jnp.concatenate([high, low], axis=1), jnp.concatenate([onehot, onehot], axis=0)
            )
            code = jnp.broadcast_to(tile_row(octant, t), (8, 640))
            chosen = picked[0:8]
            for o in range(1, 8):
                chosen = jnp.where(code == o, picked[8 * o : 8 * o + 8], chosen)
            speed = v_ref[:, pl.ds(pl.multiple_of(g * 5120 + t * 640, 128), 640)]
            ux, uy, uz, nx, ny, nz = [chosen[k : k + 1] for k in range(6)]
            wx, wy, wz = speed[0:1] - ux, speed[1:2] - uy, speed[2:3] - uz
            along = (1.0 - ROT_COS) * (nx * wx + ny * wy + nz * wz)
            new = [
                ux + ROT_COS * wx + ROT_SIN * (ny * wz - nz * wy) + along * nx,
                uy + ROT_COS * wy + ROT_SIN * (nz * wx - nx * wz) + along * ny,
                uz + ROT_COS * wz + ROT_SIN * (nx * wy - ny * wx) + along * nz,
            ]
            out_ref[:, pl.ds(pl.multiple_of(g * 5120 + t * 640, 128), 640)] = jnp.concatenate(
                new, axis=0
            )
        return carry

    lax.fori_loop(0, PARTS, group, 0)


def table_parts(table):
    table = np.asarray(table, np.float32)
    high = table.astype(BF16)
    low = (table - high.astype(np.float32)).astype(BF16)
    return high, low


def z_tables():
    pos = np.arange(NZ)[None, :]
    line = np.arange(16)[:, None]
    quarters = []
    for quarter in range(4):
        owner = line // 2 * 8 + line % 2 * 4 + quarter
        for q in range(4):
            phase = (2 * owner + q // 2) * pos % NZ * (2.0 * np.pi / NZ)
            quarters.append(-np.sin(phase) if q % 2 else np.cos(phase))
    return table_parts(np.concatenate(quarters, axis=0).reshape(4, 64, NZ))


def y_tables():
    phase = np.arange(NY)[:, None] * np.arange(NY)[None, :] % NY * (2.0 * np.pi / NY)
    return table_parts(np.concatenate([np.cos(phase), np.sin(phase)], axis=0))


def x_tables():
    k = np.arange(512)
    lane = k % 128
    x = k // 128 * 32 + (lane & 3) * 8 + lane // 16
    kz = (lane >> 3) & 1
    part = (lane >> 2) & 1
    n = np.arange(512)
    part_out, kz_out, kx = n // 256, n // 128 % 2, n % 128
    phase = x[:, None] * kx[None, :] % NX * (2.0 * np.pi / NX)
    same = kz[:, None] == kz_out[None, :]
    c, s = np.cos(phase), np.sin(phase)
    real = np.where(part[:, None] == 0, c, s)
    imag = np.where(part[:, None] == 0, -s, c)
    table = np.where(part_out[None, :] == 0, real, imag) * same / math.sqrt(NX * NY * NZ)
    return table_parts(table)


def shell_counts():
    def wave(n):
        k = np.arange(n)
        return np.where(k >= n // 2, k - n, k)

    square = wave(NZ)[:, None, None] ** 2 + wave(NY)[None, :, None] ** 2 + wave(NX)[None, None, :] ** 2
    edges = np.arange(NSHELL + 1) ** 2
    below = np.searchsorted(np.sort(square.reshape(-1)), edges, side="left")
    return np.diff(below).astype(np.float32)


def z_body(first_ref, in_ref, fh_ref, fl_ref, out_ref):
    lane = iota((16, 128), 1)
    fh, fl = fh_ref[first_ref[2]], fl_ref[first_ref[2]]
    for c in range(3):
        data = jnp.concatenate(
            [
                in_ref[:, 64 * c + 16 * r : 64 * c + 16 * r + 16, :].reshape(128, 128)
                for r in range(4)
            ],
            axis=1,
        )
        high, low = split(data)
        res = dot(fh, high) + dot(fh, low) + dot(fl, high)
        for r in range(4):
            g = [res[16 * q : 16 * q + 16, 128 * r : 128 * r + 128] for q in range(4)]
            for bit, size in ((2, 8), (1, 4)):
                clear = (lane & size) == 0
                new = list(g)
                for q in range(4):
                    if not q & bit:
                        a, b = g[q], g[q | bit]
                        new[q] = jnp.where(clear, a, lroll(b, size))
                        new[q | bit] = jnp.where(clear, lroll(a, -size), b)
                g = new
            for k in range(4):
                out_ref[pl.ds(16 * c + 4 * r + k, 16, stride=48), :] = g[k]


def y_body(in_ref, fh_ref, fl_ref, out_ref):
    both = in_ref[...].reshape(16, 48, 128)
    data = jnp.concatenate(
        [both[:, 16 * c : 16 * c + 16].reshape(256, 128) for c in range(3)], axis=1
    )
    high, low = split(data)
    fh, fl = fh_ref[...], fl_ref[...]
    res = dot(fh, high) + dot(fh, low) + dot(fl, high)
    is_real = (iota((256, 128), 1) & 4) == 0
    for c in range(3):
        even = res[0:256, 128 * c : 128 * c + 128]
        odd = res[256:512, 128 * c : 128 * c + 128]
        out = even + jnp.where(is_real, lroll(odd, -4), -lroll(odd, 4))
        for d in range(4):
            out_ref[d, 64 * c : 64 * c + 64, :] = out[64 * d : 64 * d + 64]
            out_ref[d, 192 + 64 * c : 256 + 64 * c, :] = out[0:64]


def x_body(first_ref, in_ref, fh_ref, fl_ref, out_ref, shell_ref, sums_ref):
    data = jnp.concatenate([in_ref[s] for s in range(4)], axis=1)
    high, low = split(data)
    fh, fl = fh_ref[...], fl_ref[...]
    res = dot(high, fh) + dot(low, fh) + dot(high, fl)
    ky = iota((64, 128), 0)
    kx = iota((64, 128), 1)
    kx = jnp.where(kx >= NX // 2, kx - NX, kx)
    plane = ky * ky + kx * kx
    weight = jnp.where(ky == 0, 1.0, 2.0)
    energy, square = [], []
    for kz in range(2):
        total = jnp.zeros((64, 128), F32)
        for part in range(2):
            for c in range(3):
                here = slice(256 * part + 128 * kz, 256 * part + 128 * kz + 128)
                out_ref[part, c, kz] = res[64 * c : 64 * c + 64, here]
                block = res[192 + 64 * c : 256 + 64 * c, here]
                total += block * block
        wave = first_ref[0] + kz
        wave = jnp.where(wave >= NZ // 2, wave - NZ, wave)
        energy.append(total * weight)
        square.append(plane + wave * wave)
    energy = jnp.concatenate(energy, axis=0)
    square = jnp.concatenate(square, axis=0)
    for s in range(NSHELL):
        kept = jnp.where(square < (s + 1) * (s + 1), energy, 0.0)
        sums_ref[s : s + 1, :] = jnp.sum(kept, axis=0, keepdims=True)
    cumulative = sums_ref[...]
    before = jnp.where(iota((NSHELL, 128), 0) == 0, 0.0, sroll(cumulative, 1))
    own = jnp.concatenate([cumulative - before, jnp.zeros((64, 128), F32)], axis=0)
    shell_ref[...] = jnp.sum(own.T, axis=0, keepdims=True)


def struct(*shape):
    return jax.ShapeDtypeStruct(shape, F32)


SMEM = pl.BlockSpec(memory_space=pltpu.SMEM)


def ring(x, axis):
    count = lax.axis_size(axis)
    forward = [(i, (i + 1) % count) for i in range(count)]
    backward = [(target, source) for source, target in forward]
    low, high = x
    return lax.ppermute(high, axis, forward), lax.ppermute(low, axis, backward)


def gathered_sum(x, axes):
    count = lax.axis_size(axes)
    copies = jnp.broadcast_to(x[None], (count, *x.shape))
    return jnp.sum(lax.all_to_all(copies, axes, split_axis=0, concat_axis=0, tiled=True), axis=0)


def params(mib):
    return pltpu.CompilerParams(vmem_limit_bytes=mib * 1024 * 1024)


def whole(*shape):
    return pl.BlockSpec(shape, lambda i: (0,) * len(shape))


def collide(start, stop, grid_shift, velocity, place, views, earlier):
    span = TILES * TILE * PPC // STEPS
    speed_spec = pl.BlockSpec((3, span), lambda i: (0, i + start))
    place_spec = pl.BlockSpec((640 // STEPS, 128), lambda i: (i + start, 0))
    more = [] if earlier is None else [earlier]
    return pl.pallas_call(
        lambda *refs: collide_body(start, *refs),
        name="collide",
        grid=(stop - start,),
        in_specs=[SMEM, speed_spec, place_spec, whole(24, VROWS, 128)]
        + [pl.BlockSpec(memory_space=pl.ANY)] * len(more),
        out_specs=speed_spec,
        out_shape=struct(*velocity.shape),
        scratch_shapes=[pltpu.VMEM((8 * LROW, 128), F32)],
        input_output_aliases={4: 0} if more else {},
        compiler_params=params(12),
        cost_estimate=pl.CostEstimate(
            flops=800_000_000 * (stop - start), bytes_accessed=4_000_000, transcendentals=0
        ),
    )(grid_shift, velocity, place, views, *more)


def per_device(velocity, particle_place, grid_shift, rotation_axis):
    place = particle_place.reshape(640, 128)
    axis_index = rotation_axis.reshape(TILES, 128)
    span = TILES * TILE * PPC // BLOCKS
    speed_spec = pl.BlockSpec((3, span), lambda i: (0, i))
    place_spec = pl.BlockSpec((640 // BLOCKS, 128), lambda i: (i, 0))
    out_shapes = [(32, TILES, 128), (3, TILES, 128), (40, 128), (40, 128)]
    sums, normal, x_lo, x_hi = pl.pallas_call(
        scatter_body,
        name="scatter",
        grid=(BLOCKS,),
        in_specs=[SMEM, speed_spec, place_spec, whole(TILES, 128)],
        out_specs=[whole(*s) for s in out_shapes],
        out_shape=[struct(*s) for s in out_shapes],
        scratch_shapes=[pltpu.VMEM((8 * SROW, 128), F32)],
        compiler_params=params(12),
    )(grid_shift, velocity, place, axis_index)
    main, y_lo, y_hi, z_lo, z_hi = pl.pallas_call(
        plane_body,
        name="planes",
        out_shape=[struct(4, ROWS, 128)] + [struct(40, 128)] * 2 + [struct(ROWS, 128)] * 2,
        scratch_shapes=[pltpu.VMEM((5, ROWS, 128), F32), pltpu.VMEM((1, ROWS, 128), F32)],
        compiler_params=params(12),
        cost_estimate=pl.CostEstimate(flops=1_000_000_000, bytes_accessed=3_000_000, transcendentals=0),
    )(sums, normal)
    below, above = ring((x_lo, x_hi), "gx")
    x_lo, x_hi, y_lo, y_hi = pl.pallas_call(
        fold_x_body, name="fold_x", out_shape=[struct(40, 128)] * 4, compiler_params=params(2)
    )(x_lo, x_hi, below, above, y_lo, y_hi)
    below, above = ring((y_lo, y_hi), GY)
    y_lo, y_hi, z_lo, z_hi = pl.pallas_call(
        fold_y_body, name="fold_y", out_shape=[struct(40, 128)] * 2 + [struct(ROWS, 128)] * 2,
        compiler_params=params(3),
    )(y_lo, y_hi, below, above, x_lo, x_hi, z_lo, z_hi)
    below, above = ring((z_lo, z_hi), GZ)
    views, sent = pl.pallas_call(
        cell_body,
        name="cells",
        out_shape=[struct(24, VROWS, 128), struct(8, 192, 128)],
        scratch_shapes=[
            pltpu.VMEM((7, ROWS, 128), F32),
            pltpu.VMEM((7, ROWS, 128), F32),
            pltpu.VMEM((3, TILES, 128), F32),
        ],
        compiler_params=params(12),
    )(sums, main, normal, x_lo, x_hi, y_lo, y_hi, z_lo, z_hi, below, above)
    first = jnp.stack(
        [lax.axis_index(GY_GZ) * 2, lax.axis_index("gx") * 64, lax.axis_index("gz_1")]
    ).astype(jnp.int32)
    arrived = lax.all_to_all(sent, GZ, split_axis=0, concat_axis=0, tiled=True)
    updated = collide(0, EARLY, grid_shift, velocity, place, views, None)
    arrived, updated = lax.optimization_barrier((arrived, updated))
    vmem = pl.BlockSpec(memory_space=pltpu.VMEM)
    lines = pl.pallas_call(
        z_body,
        name="z_lines",
        in_specs=[SMEM, vmem, vmem, vmem],
        out_shape=struct(768, 128),
        compiler_params=params(6),
    )(first, arrived, *z_tables())
    pencil = lax.all_to_all(
        lines.reshape(16, 48, 128), ("gy_0", "gy_1", "gz_0"), split_axis=0, concat_axis=0, tiled=True
    )
    new_velocity = collide(EARLY, STEPS, grid_shift, velocity, place, views, updated)
    pencil, new_velocity = lax.optimization_barrier((pencil, new_velocity))
    rows = pl.pallas_call(y_body, name="y_lines", out_shape=struct(4, 384, 128), compiler_params=params(12))(
        pencil.reshape(768, 128), *y_tables()
    )
    columns = lax.all_to_all(rows, "gx", split_axis=0, concat_axis=0, tiled=True)
    modes, shells = pl.pallas_call(
        x_body,
        name="x_lines",
        in_specs=[SMEM, vmem, vmem, vmem],
        out_shape=[struct(2, 3, 2, 64, 128), struct(1, 128)],
        scratch_shapes=[pltpu.VMEM((NSHELL, 128), F32)],
        compiler_params=params(12),
    )(first, columns, *x_tables())
    total = gathered_sum(shells, GY_GZ)
    spectrum = total[0, :NSHELL] / shell_counts()
    return new_velocity, modes, spectrum


def solution(mesh):
    torus = Mesh(
        mesh.devices.reshape(mesh.shape["gx"], 4, 2, 2, 4), ("gx", "gy_0", "gy_1", "gz_0", "gz_1")
    )
    in_specs = (P(None, GX_GY_GZ), P(GX_GY_GZ), P(), P(GY, "gx", GZ))
    out_specs = (P(None, GX_GY_GZ), P(None, None, GY_GZ, "gx", None), P())
    return jax.shard_map(
        per_device, mesh=torus, in_specs=in_specs, out_specs=out_specs, check_vma=False
    )
```

```python
import math

import jax
import jax.numpy as jnp
import numpy as np
from jax import lax
from jax.experimental import pallas as pl
from jax.experimental.pallas import tpu as pltpu
from jax.sharding import Mesh
from jax.sharding import PartitionSpec as P

PPC = 5
TILE = 128
SUB = 4
NAXES = 1024
NSHELL = 64
NX, NY, NZ = 128, 256, 128
GX_GY_GZ = ("gx", "gy_0", "gy_1", "gz_0", "gz_1")
GY = ("gy_0", "gy_1")
GZ = ("gz_0", "gz_1")
GY_GZ = ("gy_0", "gy_1", "gz_0", "gz_1")
ROT_COS = math.cos(130.0 * math.pi / 180.0)
ROT_SIN = math.sin(130.0 * math.pi / 180.0)
F32 = jnp.float32
BF16 = jnp.bfloat16
TILES = 128
ROWS = 160
SROW = 36
LROW = 68
BLOCKS = 1
GROUPS = TILES // 8 // BLOCKS
STEPS = 8
EARLY = 6
PARTS = TILES // 8 // STEPS


def axis_vectors(axis_index):
    level = 1.0 - (2.0 * axis_index.astype(F32) + 1.0) / NAXES
    radius = jnp.sqrt(1.0 - level * level)
    whole_turns = (axis_index * 1597).astype(F32) * (1.0 / 2584.0)
    turn = (axis_index * 1597 - 2584 * jnp.floor(whole_turns).astype(jnp.int32)).astype(F32)
    turn = turn * (2.0 * math.pi / 2584.0)
    return radius * jnp.cos(turn), radius * jnp.sin(turn), level


def iota(shape, dim):
    return lax.broadcasted_iota(jnp.int32, shape, dim)


def lroll(x, amount):
    amount %= 128
    return pltpu.roll(x, amount, 1) if amount else x


def sroll(x, amount):
    return pltpu.roll(x, amount % x.shape[0], 0)


def split(x):
    high = x.astype(BF16)
    return high, (x - high.astype(F32)).astype(BF16)


def dot(a, b):
    return jnp.dot(a, b, preferred_element_type=F32)


def octants(place, shift_ref):
    bit_x = (((place >> 4) & 3) + shift_ref[0] >= SUB).astype(jnp.int32)
    bit_y = (((place >> 2) & 3) + shift_ref[1] >= SUB).astype(jnp.int32)
    bit_z = ((place & 3) + shift_ref[2] >= SUB).astype(jnp.int32)
    return bit_x * 4 + bit_y * 2 + bit_z


def tile_row(rows, t):
    return jnp.concatenate([rows[PPC * t + r : PPC * t + r + 1, :] for r in range(PPC)], axis=1)


def onehot_of(member, t, cells):
    return jnp.concatenate(
        [
            jnp.where(
                cells
                == jnp.broadcast_to(
                    member[PPC * t + r : PPC * t + r + 1, :], cells.shape
                ).astype(BF16),
                jnp.ones(cells.shape, BF16),
                jnp.zeros(cells.shape, BF16),
            )
            for r in range(PPC)
        ],
        axis=1,
    )


def scatter_body(shift_ref, v_ref, p_ref, axis_ref, s_ref, n_ref, xlo_ref, xhi_ref, turn_ref):
    step = pl.program_id(0)
    cells = iota((TILE, TILE), 0).astype(F32).astype(BF16)
    upper = iota((8, TILE), 0) < 4

    def group(g, carry):
        place = p_ref[pl.ds(pl.multiple_of(g * 40, 8), 40), :]
        member = (place >> 6).astype(F32)
        octant = octants(place, shift_ref)
        speed = v_ref[:, pl.ds(pl.multiple_of(g * 5120, 128), 5120)]
        high = speed.astype(BF16).astype(F32)
        low = speed - high
        one = jnp.ones((1, 640), F32)
        zero = jnp.zeros((1, 640), F32)
        for t in range(8):
            here = slice(t * 640, (t + 1) * 640)
            onehot = onehot_of(member, t, cells)
            code = jnp.broadcast_to(tile_row(octant, t), (8, 640))
            values = jnp.concatenate([high[:, here], one, low[:, here], zero], axis=0)
            weighted = jnp.concatenate(
                [jnp.where(code == o, values, 0.0) for o in range(8)], axis=0
            ).astype(BF16)
            sums = lax.dot_general(
                onehot, weighted, (((1,), (1,)), ((), ())), preferred_element_type=F32
            ).T
            for pair in range(4):
                even = sums[16 * pair : 16 * pair + 8]
                odd = sums[16 * pair + 8 : 16 * pair + 16]
                both = jnp.where(upper, even + sroll(even, 4), odd + sroll(odd, 4))
                turn_ref[SROW * t + 8 * pair : SROW * t + 8 * pair + 8, :] = both
        first = pl.multiple_of((step * GROUPS + g) * 8, 8)
        for r in range(32):
            s_ref[r, pl.ds(first, 8), :] = turn_ref[pl.ds(r, 8, stride=SROW), :]
        return carry

    lax.fori_loop(0, GROUPS, group, 0)

    @pl.when(step == BLOCKS - 1)
    def _():
        for c, part in enumerate(axis_vectors(axis_ref[...])):
            n_ref[c] = part
        z = iota((32, 128), 1) & 15
        lane = iota((40, 128), 1)
        pad = jnp.zeros((8, 128), F32)
        low_face = jnp.zeros((40, 128), F32)
        high_face = jnp.zeros((40, 128), F32)
        for q in range(5):
            faces = []
            for bx in range(2):
                parts = []
                for by in range(2):
                    base = bx * 4 + by * 2
                    rows = pl.ds(3 * bx, 32, stride=4)
                    if q < 4:
                        above = s_ref[(base + 1) * 4 + q, rows, :]
                        part = s_ref[base * 4 + q, rows, :] + jnp.where(z > 0, lroll(above, 1), 0.0)
                    else:
                        part = jnp.zeros((32, 128), F32)
                        for k in range(4):
                            above = s_ref[(base + 1) * 4 + k, rows, :]
                            part = jnp.where(z == k, lroll(above, k - 15), part)
                    parts.append(jnp.concatenate([part, pad], axis=0))
                faces.append(parts[0] + sroll(parts[1], 1))
            inside = (lane >> 4) == q if q < 4 else (lane >> 2) == 16
            low_face = jnp.where(inside, lroll(faces[0], 16 * q), low_face)
            high_face = jnp.where(inside, lroll(faces[1], 16 * q - 112), high_face)
        for c in range(3):
            inside = ((lane >> 4) == 5 + c) & (iota((40, 128), 0) < 32)
            face = jnp.concatenate([n_ref[c, pl.ds(0, 32, stride=4), :], pad], axis=0)
            low_face = jnp.where(inside, lroll(face, 80 + 16 * c), low_face)
        xlo_ref[...] = low_face
        xhi_ref[...] = high_face


def plane_body(s_ref, n_ref, m_ref, ylo_ref, yhi_ref, zlo_ref, zhi_ref, edge_ref, zed_ref):
    lane = iota((TILES, 128), 1)
    row = iota((TILES, 128), 0)
    z = lane & 15
    x_in = lane >> 4
    x_out = row & 3
    last = (x_in == 7) & (x_out == 3)

    def x_shift(plane):
        rolled = lroll(plane, 16)
        return jnp.where(
            x_in > 0, rolled, jnp.where(x_out > 0, sroll(rolled, 1), 0.0)
        )

    for q in range(5):
        for by in range(2):
            parts = []
            for bx in range(2):
                base = bx * 4 + by * 2
                if q < 4:
                    above = s_ref[(base + 1) * 4 + q]
                    parts.append(
                        s_ref[base * 4 + q] + jnp.where(z > 0, lroll(above, 1), 0.0)
                    )
                else:
                    rim = jnp.zeros((TILES, 128), F32)
                    for k in range(4):
                        rim = jnp.where(z == k, lroll(s_ref[(base + 1) * 4 + k], k - 15), rim)
                    parts.append(rim)
            main = parts[0] + x_shift(parts[1])
            edge = jnp.where(last, parts[1], 0.0)
            dst = m_ref if q < 4 else zed_ref
            at = q if q < 4 else 0
            if by == 0:
                dst[at, 0:TILES, :] = main
                dst[at, TILES:ROWS, :] = jnp.zeros((ROWS - TILES, 128), F32)
                edge_ref[q, 0:TILES, :] = edge
                edge_ref[q, TILES:ROWS, :] = jnp.zeros((ROWS - TILES, 128), F32)
            else:
                dst[at, 4:132, :] = dst[at, 4:132, :] + main
                edge_ref[q, 4:132, :] = edge_ref[q, 4:132, :] + edge
    ylo_ref[...] = jnp.zeros((40, 128), F32)
    yhi_ref[...] = jnp.zeros((40, 128), F32)
    for q in range(5):
        src = m_ref if q < 4 else zed_ref
        at = q if q < 4 else 0
        ylo_ref[4 * q : 4 * q + 4, :] = src[at, 0:4, :]
        yhi_ref[4 * q : 4 * q + 4, :] = src[at, 128:132, :]
    for c in range(3):
        ylo_ref[20 + 4 * c : 24 + 4 * c, :] = n_ref[c, 0:4, :]
    big = iota((ROWS, 128), 1)
    slot = big & 15
    low_z = jnp.zeros((ROWS, 128), F32)
    for q in range(4):
        low_z = jnp.where(slot == q, lroll(m_ref[q], q), low_z)
    for c in range(3):
        face = jnp.concatenate([n_ref[c], jnp.zeros((ROWS - TILES, 128), F32)], axis=0)
        low_z = jnp.where(slot == 4 + c, lroll(face, 4 + c), low_z)
    zlo_ref[...] = low_z
    zhi_ref[...] = zed_ref[0]


def fold_x_body(xlo_ref, xhi_ref, from_low, from_high, ylo_ref, yhi_ref,
                xlo_out, xhi_out, ylo_out, yhi_out):
    low = xlo_ref[...] + from_low[...]
    high = xhi_ref[...] + from_high[...]
    xlo_out[...] = low
    xhi_out[...] = high
    lane = iota((1, 128), 1)
    for src, dst, y in ((ylo_ref, ylo_out, 0), (yhi_ref, yhi_out, 32)):
        dst[...] = src[...]
        for q in range(4):
            dst[4 * q : 4 * q + 1, :] = jnp.where(
                lane < 16, lroll(low[y : y + 1], -16 * q), src[4 * q : 4 * q + 1, :]
            )
        dst[16:17, :] = jnp.where(lane < 4, lroll(low[y : y + 1], -64), src[16:17, :])
        dst[32:33, :] = high[y : y + 1]


def fold_y_body(ylo_ref, yhi_ref, from_low, from_high, xlo_ref, xhi_ref, zlo_ref, zhi_ref,
                ylo_out, yhi_out, zlo_out, zhi_out):
    low = ylo_ref[...] + from_low[...]
    high = yhi_ref[...] + from_high[...]
    ylo_out[...] = low
    yhi_out[...] = high
    zlo_out[...] = zlo_ref[...]
    zhi_out[...] = zhi_ref[...]
    x_low = xlo_ref[...]
    x_high = xhi_ref[...]
    lane = iota((40, 128), 1)
    lo0 = zlo_out[pl.ds(0, 40, stride=4), :]
    hi0 = zhi_out[pl.ds(0, 40, stride=4), :]
    lo3 = zlo_out[pl.ds(3, 40, stride=4), :]
    hi3 = zhi_out[pl.ds(3, 40, stride=4), :]
    for q in range(4):
        lo0 = jnp.where(lane == q, lroll(x_low, q - 16 * q), lo0)
        lo3 = jnp.where(lane == 120 + q, lroll(x_high, 120 + q - 16 * q), lo3)
    for c in range(3):
        lo3 = jnp.where(lane == 124 + c, lroll(x_high, 124 + c - 80 - 16 * c), lo3)
    hi0 = jnp.where(lane < 4, lroll(x_low, -64), hi0)
    hi3 = jnp.where((lane >= 120) & (lane < 124), lroll(x_high, 120 - 64), hi3)
    zlo_out[pl.ds(0, 40, stride=4), :] = lo0
    zhi_out[pl.ds(0, 40, stride=4), :] = hi0
    zlo_out[pl.ds(3, 40, stride=4), :] = lo3
    zhi_out[pl.ds(3, 40, stride=4), :] = hi3
    lane4 = iota((4, 128), 1)
    slot = lane4 & 15
    corner = (iota((4, 128), 0) == 3) & (lane4 >= 120)
    for face, first in ((low, 0), (high, 128)):
        lo = jnp.zeros((4, 128), F32)
        for q in range(4):
            lo = jnp.where(slot == q, lroll(face[4 * q : 4 * q + 4], q), lo)
        for c in range(3):
            lo = jnp.where(slot == 4 + c, lroll(face[20 + 4 * c : 24 + 4 * c], 4 + c), lo)
        end = face[32:33]
        tail = jnp.zeros((1, 128), F32)
        lane1 = iota((1, 128), 1)
        for q in range(4):
            tail = jnp.where(lane1 == 120 + q, lroll(end, 120 + q - 16 * q), tail)
        for c in range(3):
            tail = jnp.where(lane1 == 124 + c, lroll(end, 124 + c - 80 - 16 * c), tail)
        zlo_out[first : first + 4, :] = jnp.where(corner, tail, lo)
        hi = jnp.where(slot < 4, face[16:20], 0.0)
        zhi_out[first : first + 4, :] = jnp.where(
            corner, jnp.where(lane1 < 124, lroll(end, 120 - 64), 0.0), hi
        )


VROWS = 136


def cell_body(s_ref, m_ref, n_ref, xlo_ref, xhi_ref, ylo_ref, yhi_ref, zlo_ref, zhi_ref,
              from_low, from_high, view_ref, send_ref, ext_ref, end_ref, vel_ref):
    z_low = zlo_ref[0:VROWS, :] + from_low[0:VROWS, :]
    z_high = zhi_ref[0:VROWS, :] + from_high[0:VROWS, :]
    x_low = xlo_ref[...]
    x_high = xhi_ref[...]
    y_low = ylo_ref[...]
    y_high = yhi_ref[...]
    lane40 = iota((40, 128), 1)
    lane = iota((VROWS, 128), 1)
    row = iota((VROWS, 128), 0)
    z = lane & 15
    x_in = lane >> 4
    x_out = row & 3
    for k in range(7):
        if k < 4:
            ext_ref[k] = m_ref[k]
            held = ext_ref[k, pl.ds(0, 40, stride=4), :]
            ext_ref[k, pl.ds(0, 40, stride=4), :] = jnp.where(
                lane40 < 16, lroll(x_low, -16 * k), held
            )
            ext_ref[k, 0:4, :] = y_low[4 * k : 4 * k + 4]
            ext_ref[k, 128:132, :] = y_high[4 * k : 4 * k + 4]
            amount = 112 - 16 * k
        else:
            c = k - 4
            ext_ref[k, 0:TILES, :] = n_ref[c]
            ext_ref[k, 128:132, :] = y_high[20 + 4 * c : 24 + 4 * c]
            amount = 32 - 16 * c
        end_ref[k, pl.ds(3, 40, stride=4), :] = lroll(x_high, amount)
        end_ref[k, 131:132, :] = lroll(y_high[32:33], amount)
        if k < 4:
            end_ref[k, 3:4, :] = lroll(y_low[32:33], amount)

    def pair(k):
        main = ext_ref[k, 0:VROWS, :]
        end = end_ref[k, 0:VROWS, :]
        if k < 4:
            main = jnp.where(z == 0, lroll(z_low, -k), main)
            end = jnp.where(z == 0, lroll(z_low, -8 - k), end)
        main1 = jnp.where(z < 15, lroll(main, -1), lroll(z_high, 15 - k))
        end1 = jnp.where(z < 15, lroll(end, -1), lroll(z_high, 7 - k))
        return (main, main1), (end, end1)

    count_main, count_end = pair(3)
    inv_main = [1.0 / jnp.maximum(a, 1.0) for a in count_main]
    inv_end = [1.0 / jnp.maximum(a, 1.0) for a in count_end]
    for slot, k in enumerate((0, 1, 2, 4, 5, 6)):
        mains, ends = pair(k)
        for bz in range(2):
            main, end = mains[bz], ends[bz]
            if k < 3:
                main = main * inv_main[bz]
                end = end * inv_end[bz]
            rolled = lroll(main, -16)
            ahead = jnp.where(x_in < 7, rolled, jnp.where(x_out == 3, end, sroll(rolled, -1)))
            view_ref[bz * 6 + slot] = main
            view_ref[(2 + bz) * 6 + slot] = ahead

    def group(g, carry):
        first = pl.multiple_of(g * 8, 8)
        acc = [jnp.zeros((8, 128), F32) for _ in range(3)]
        total = jnp.zeros((8, 128), F32)
        for bx in range(2):
            for bz in range(2):
                wide = [view_ref[(bx * 2 + bz) * 6 + k, pl.ds(first, 16), :] for k in range(6)]
                for by in range(2):
                    o = bx * 4 + by * 2 + bz
                    ux, uy, uz, nx, ny, nz = [w[4 * by : 4 * by + 8] for w in wide]
                    sx, sy, sz, num = [s_ref[o * 4 + q, pl.ds(first, 8), :] for q in range(4)]
                    mx, my, mz = num * ux, num * uy, num * uz
                    wx, wy, wz = sx - mx, sy - my, sz - mz
                    along = (1.0 - ROT_COS) * (nx * wx + ny * wy + nz * wz)
                    acc[0] += mx + ROT_COS * wx + ROT_SIN * (ny * wz - nz * wy) + along * nx
                    acc[1] += my + ROT_COS * wy + ROT_SIN * (nz * wx - nx * wz) + along * ny
                    acc[2] += mz + ROT_COS * wz + ROT_SIN * (nx * wy - ny * wx) + along * nz
                    total += num
        inverse = 1.0 / jnp.maximum(total, 1.0)
        for c in range(3):
            vel_ref[c, pl.ds(first, 8), :] = acc[c] * inverse
        return carry

    lax.fori_loop(0, TILES // 8, group, 0)
    lane = iota((TILES, 128), 1)
    row = iota((TILES, 128), 0)
    for c in range(3):
        plane = vel_ref[c]
        for bit in range(4):
            size = 1 << bit
            row_bit = (row >> bit) & 1
            lane_bit = (lane >> bit) & 1
            down = sroll(lroll(plane, size), -size)
            up = sroll(lroll(plane, -size), size)
            plane = jnp.where(row_bit == lane_bit, plane, jnp.where(row_bit == 0, down, up))
        for part in range(8):
            send_ref[part, 64 * c : 64 * c + 64, :] = plane[64 * (part // 4) : 64 * (part // 4) + 64]


def collide_body(start, shift_ref, v_ref, p_ref, view_ref, *refs):
    out_ref, turn_ref = refs[-2:]
    step = pl.program_id(0) + start
    cells = iota((TILE, TILE), 0).astype(F32).astype(BF16)

    @pl.when(step == start)
    def _():
        turn_ref[...] = jnp.zeros(turn_ref.shape, F32)

    def group(g, carry):
        place = p_ref[pl.ds(pl.multiple_of(g * 40, 8), 40), :]
        member = (place >> 6).astype(F32)
        octant = octants(place, shift_ref)
        first = pl.multiple_of((step * PARTS + g) * 8, 8)
        for bx in range(2):
            for bz in range(2):
                for k in range(6):
                    wide = view_ref[(bx * 2 + bz) * 6 + k, pl.ds(first, 16), :]
                    for by in range(2):
                        o = bx * 4 + by * 2 + bz
                        turn_ref[pl.ds(8 * o + k, 8, stride=LROW), :] = wide[4 * by : 4 * by + 8]
        for t in range(8):
            high, low = split(turn_ref[LROW * t : LROW * t + 64, :])
            onehot = onehot_of(member, t, cells)
            picked = dot(
                jnp.concatenate([high, low], axis=1), jnp.concatenate([onehot, onehot], axis=0)
            )
            code = jnp.broadcast_to(tile_row(octant, t), (8, 640))
            chosen = picked[0:8]
            for o in range(1, 8):
                chosen = jnp.where(code == o, picked[8 * o : 8 * o + 8], chosen)
            speed = v_ref[:, pl.ds(pl.multiple_of(g * 5120 + t * 640, 128), 640)]
            ux, uy, uz, nx, ny, nz = [chosen[k : k + 1] for k in range(6)]
            wx, wy, wz = speed[0:1] - ux, speed[1:2] - uy, speed[2:3] - uz
            along = (1.0 - ROT_COS) * (nx * wx + ny * wy + nz * wz)
            new = [
                ux + ROT_COS * wx + ROT_SIN * (ny * wz - nz * wy) + along * nx,
                uy + ROT_COS * wy + ROT_SIN * (nz * wx - nx * wz) + along * ny,
                uz + ROT_COS * wz + ROT_SIN * (nx * wy - ny * wx) + along * nz,
            ]
            out_ref[:, pl.ds(pl.multiple_of(g * 5120 + t * 640, 128), 640)] = jnp.concatenate(
                new, axis=0
            )
        return carry

    lax.fori_loop(0, PARTS, group, 0)


def table_parts(table):
    table = np.asarray(table, np.float32)
    high = table.astype(BF16)
    low = (table - high.astype(np.float32)).astype(BF16)
    return high, low


def z_tables():
    pos = np.arange(NZ)[None, :]
    line = np.arange(16)[:, None]
    quarters = []
    for quarter in range(4):
        owner = line // 2 * 8 + line % 2 * 4 + quarter
        for q in range(4):
            phase = (2 * owner + q // 2) * pos % NZ * (2.0 * np.pi / NZ)
            quarters.append(-np.sin(phase) if q % 2 else np.cos(phase))
    return table_parts(np.concatenate(quarters, axis=0).reshape(4, 64, NZ))


def y_tables():
    phase = np.arange(NY)[:, None] * np.arange(NY)[None, :] % NY * (2.0 * np.pi / NY)
    return table_parts(np.concatenate([np.cos(phase), np.sin(phase)], axis=0))


def x_tables():
    k = np.arange(512)
    lane = k % 128
    x = k // 128 * 32 + (lane & 3) * 8 + lane // 16
    kz = (lane >> 3) & 1
    part = (lane >> 2) & 1
    n = np.arange(512)
    part_out, kz_out, kx = n // 256, n // 128 % 2, n % 128
    phase = x[:, None] * kx[None, :] % NX * (2.0 * np.pi / NX)
    same = kz[:, None] == kz_out[None, :]
    c, s = np.cos(phase), np.sin(phase)
    real = np.where(part[:, None] == 0, c, s)
    imag = np.where(part[:, None] == 0, -s, c)
    table = np.where(part_out[None, :] == 0, real, imag) * same / math.sqrt(NX * NY * NZ)
    return table_parts(table)


def shell_counts():
    def wave(n):
        k = np.arange(n)
        return np.where(k >= n // 2, k - n, k)

    square = wave(NZ)[:, None, None] ** 2 + wave(NY)[None, :, None] ** 2 + wave(NX)[None, None, :] ** 2
    edges = np.arange(NSHELL + 1) ** 2
    below = np.searchsorted(np.sort(square.reshape(-1)), edges, side="left")
    return np.diff(below).astype(np.float32)


def z_body(first_ref, in_ref, fh_ref, fl_ref, out_ref):
    lane = iota((16, 128), 1)
    fh, fl = fh_ref[first_ref[2]], fl_ref[first_ref[2]]
    for c in range(3):
        data = jnp.concatenate(
            [
                in_ref[:, 64 * c + 16 * r : 64 * c + 16 * r + 16, :].reshape(128, 128)
                for r in range(4)
            ],
            axis=1,
        )
        high, low = split(data)
        res = dot(fh, high) + dot(fh, low) + dot(fl, high)
        for r in range(4):
            g = [res[16 * q : 16 * q + 16, 128 * r : 128 * r + 128] for q in range(4)]
            for bit, size in ((2, 8), (1, 4)):
                clear = (lane & size) == 0
                new = list(g)
                for q in range(4):
                    if not q & bit:
                        a, b = g[q], g[q | bit]
                        new[q] = jnp.where(clear, a, lroll(b, size))
                        new[q | bit] = jnp.where(clear, lroll(a, -size), b)
                g = new
            for k in range(4):
                out_ref[pl.ds(16 * c + 4 * r + k, 16, stride=48), :] = g[k]


def y_body(in_ref, fh_ref, fl_ref, out_ref):
    both = in_ref[...].reshape(16, 48, 128)
    data = jnp.concatenate(
        [both[:, 16 * c : 16 * c + 16].reshape(256, 128) for c in range(3)], axis=1
    )
    high, low = split(data)
    fh, fl = fh_ref[...], fl_ref[...]
    res = dot(fh, high) + dot(fh, low) + dot(fl, high)
    is_real = (iota((256, 128), 1) & 4) == 0
    for c in range(3):
        even = res[0:256, 128 * c : 128 * c + 128]
        odd = res[256:512, 128 * c : 128 * c + 128]
        out = even + jnp.where(is_real, lroll(odd, -4), -lroll(odd, 4))
        for d in range(4):
            out_ref[d, 64 * c : 64 * c + 64, :] = out[64 * d : 64 * d + 64]
            out_ref[d, 192 + 8 * c : 200 + 8 * c, :] = out[0:8]
    for d in range(4):
        out_ref[d, 216:224, :] = jnp.zeros((8, 128), F32)


def x_body(first_ref, in_ref, fh_ref, fl_ref, out_ref, shell_ref, sums_ref):
    data = jnp.concatenate([in_ref[s] for s in range(4)], axis=1)
    high, low = split(data)
    fh, fl = fh_ref[...], fl_ref[...]
    res = dot(high, fh) + dot(low, fh) + dot(high, fl)
    kx = iota((64, 128), 1)
    kx = jnp.where(kx >= NX // 2, kx - NX, kx)
    ky = first_ref[1] + iota((64, 128), 0)
    ky = jnp.where(ky >= NY // 2, ky - NY, ky)
    plane = ky * ky + kx * kx
    weight = jnp.where(ky == 0, 1.0, 2.0)
    extra_row = (iota((8, 128), 0) == 0) & (first_ref[1] == 3 * NY // 4)
    extra_plane = kx[0:8] * kx[0:8]
    energy, square = [], []
    for kz in range(2):
        total = jnp.zeros((64, 128), F32)
        extra = jnp.zeros((8, 128), F32)
        for part in range(2):
            for c in range(3):
                here = slice(256 * part + 128 * kz, 256 * part + 128 * kz + 128)
                block = res[64 * c : 64 * c + 64, here]
                out_ref[part, c, kz] = block
                total += block * block
                block = res[192 + 8 * c : 200 + 8 * c, here]
                extra += block * block
        wave = first_ref[0] + kz
        wave = jnp.where(wave >= NZ // 2, wave - NZ, wave)
        energy += [total * weight, jnp.where(extra_row, extra, 0.0)]
        square += [plane + wave * wave, extra_plane + wave * wave]
    energy = jnp.concatenate(energy, axis=0)
    square = jnp.concatenate(square, axis=0)
    for s in range(NSHELL):
        kept = jnp.where(square < (s + 1) * (s + 1), energy, 0.0)
        sums_ref[s : s + 1, :] = jnp.sum(kept, axis=0, keepdims=True)
    cumulative = sums_ref[...]
    before = jnp.where(iota((NSHELL, 128), 0) == 0, 0.0, sroll(cumulative, 1))
    own = jnp.concatenate([cumulative - before, jnp.zeros((64, 128), F32)], axis=0)
    shell_ref[...] = jnp.sum(own.T, axis=0, keepdims=True)


def struct(*shape):
    return jax.ShapeDtypeStruct(shape, F32)


SMEM = pl.BlockSpec(memory_space=pltpu.SMEM)


def ring(x, axis):
    count = lax.axis_size(axis)
    forward = [(i, (i + 1) % count) for i in range(count)]
    backward = [(target, source) for source, target in forward]
    low, high = x
    return lax.ppermute(high, axis, forward), lax.ppermute(low, axis, backward)


def gathered_sum(x, axes):
    count = lax.axis_size(axes)
    copies = jnp.broadcast_to(x[None], (count, *x.shape))
    return jnp.sum(lax.all_to_all(copies, axes, split_axis=0, concat_axis=0, tiled=True), axis=0)


def params(mib):
    return pltpu.CompilerParams(vmem_limit_bytes=mib * 1024 * 1024)


def whole(*shape):
    return pl.BlockSpec(shape, lambda i: (0,) * len(shape))


def collide(start, stop, grid_shift, velocity, place, views, earlier):
    span = TILES * TILE * PPC // STEPS
    speed_spec = pl.BlockSpec((3, span), lambda i: (0, i + start))
    place_spec = pl.BlockSpec((640 // STEPS, 128), lambda i: (i + start, 0))
    more = [] if earlier is None else [earlier]
    return pl.pallas_call(
        lambda *refs: collide_body(start, *refs),
        name="collide",
        grid=(stop - start,),
        in_specs=[SMEM, speed_spec, place_spec, whole(24, VROWS, 128)]
        + [pl.BlockSpec(memory_space=pl.ANY)] * len(more),
        out_specs=speed_spec,
        out_shape=struct(*velocity.shape),
        scratch_shapes=[pltpu.VMEM((8 * LROW, 128), F32)],
        input_output_aliases={4: 0} if more else {},
        compiler_params=params(12),
        cost_estimate=pl.CostEstimate(
            flops=800_000_000 * (stop - start), bytes_accessed=4_000_000, transcendentals=0
        ),
    )(grid_shift, velocity, place, views, *more)


def per_device(velocity, particle_place, grid_shift, rotation_axis):
    place = particle_place.reshape(640, 128)
    axis_index = rotation_axis.reshape(TILES, 128)
    span = TILES * TILE * PPC // BLOCKS
    speed_spec = pl.BlockSpec((3, span), lambda i: (0, i))
    place_spec = pl.BlockSpec((640 // BLOCKS, 128), lambda i: (i, 0))
    out_shapes = [(32, TILES, 128), (3, TILES, 128), (40, 128), (40, 128)]
    sums, normal, x_lo, x_hi = pl.pallas_call(
        scatter_body,
        name="scatter",
        grid=(BLOCKS,),
        in_specs=[SMEM, speed_spec, place_spec, whole(TILES, 128)],
        out_specs=[whole(*s) for s in out_shapes],
        out_shape=[struct(*s) for s in out_shapes],
        scratch_shapes=[pltpu.VMEM((8 * SROW, 128), F32)],
        compiler_params=params(12),
    )(grid_shift, velocity, place, axis_index)
    main, y_lo, y_hi, z_lo, z_hi = pl.pallas_call(
        plane_body,
        name="planes",
        out_shape=[struct(4, ROWS, 128)] + [struct(40, 128)] * 2 + [struct(ROWS, 128)] * 2,
        scratch_shapes=[pltpu.VMEM((5, ROWS, 128), F32), pltpu.VMEM((1, ROWS, 128), F32)],
        compiler_params=params(12),
        cost_estimate=pl.CostEstimate(flops=1_000_000_000, bytes_accessed=3_000_000, transcendentals=0),
    )(sums, normal)
    below, above = ring((x_lo, x_hi), "gx")
    x_lo, x_hi, y_lo, y_hi = pl.pallas_call(
        fold_x_body, name="fold_x", out_shape=[struct(40, 128)] * 4, compiler_params=params(2)
    )(x_lo, x_hi, below, above, y_lo, y_hi)
    below, above = ring((y_lo, y_hi), GY)
    y_lo, y_hi, z_lo, z_hi = pl.pallas_call(
        fold_y_body, name="fold_y", out_shape=[struct(40, 128)] * 2 + [struct(ROWS, 128)] * 2,
        compiler_params=params(3),
    )(y_lo, y_hi, below, above, x_lo, x_hi, z_lo, z_hi)
    below, above = ring((z_lo, z_hi), GZ)
    views, sent = pl.pallas_call(
        cell_body,
        name="cells",
        out_shape=[struct(24, VROWS, 128), struct(8, 192, 128)],
        scratch_shapes=[
            pltpu.VMEM((7, ROWS, 128), F32),
            pltpu.VMEM((7, ROWS, 128), F32),
            pltpu.VMEM((3, TILES, 128), F32),
        ],
        compiler_params=params(12),
    )(sums, main, normal, x_lo, x_hi, y_lo, y_hi, z_lo, z_hi, below, above)
    first = jnp.stack(
        [lax.axis_index(GY_GZ) * 2, lax.axis_index("gx") * 64, lax.axis_index("gz_1")]
    ).astype(jnp.int32)
    arrived = lax.all_to_all(sent, GZ, split_axis=0, concat_axis=0, tiled=True)
    updated = collide(0, EARLY, grid_shift, velocity, place, views, None)
    arrived, updated = lax.optimization_barrier((arrived, updated))
    vmem = pl.BlockSpec(memory_space=pltpu.VMEM)
    lines = pl.pallas_call(
        z_body,
        name="z_lines",
        in_specs=[SMEM, vmem, vmem, vmem],
        out_shape=struct(768, 128),
        compiler_params=params(6),
    )(first, arrived, *z_tables())
    pencil = lax.all_to_all(
        lines.reshape(16, 48, 128), ("gy_0", "gy_1", "gz_0"), split_axis=0, concat_axis=0, tiled=True
    )
    new_velocity = collide(EARLY, STEPS, grid_shift, velocity, place, views, updated)
    pencil, new_velocity = lax.optimization_barrier((pencil, new_velocity))
    rows = pl.pallas_call(y_body, name="y_lines", out_shape=struct(4, 224, 128), compiler_params=params(12))(
        pencil.reshape(768, 128), *y_tables()
    )
    columns = lax.all_to_all(rows, "gx", split_axis=0, concat_axis=0, tiled=True)
    modes, shells = pl.pallas_call(
        x_body,
        name="x_lines",
        in_specs=[SMEM, vmem, vmem, vmem],
        out_shape=[struct(2, 3, 2, 64, 128), struct(1, 128)],
        scratch_shapes=[pltpu.VMEM((NSHELL, 128), F32)],
        compiler_params=params(12),
    )(first, columns, *x_tables())
    total = gathered_sum(shells, GY_GZ)
    passed = lax.ppermute(total, "gx", [(0, 1), (3, 2)])
    x_part = lax.axis_index("gx")
    total = jnp.where((x_part == 1) | (x_part == 2), passed, total)
    spectrum = total[0, :NSHELL] / shell_counts()
    return new_velocity, modes, spectrum


def solution(mesh):
    torus = Mesh(
        mesh.devices.reshape(mesh.shape["gx"], 4, 2, 2, 4), ("gx", "gy_0", "gy_1", "gz_0", "gz_1")
    )
    in_specs = (P(None, GX_GY_GZ), P(GX_GY_GZ), P(), P(GY, "gx", GZ))
    out_specs = (P(None, GX_GY_GZ), P(None, None, GY_GZ, "gx", None), P())
    return jax.shard_map(
        per_device, mesh=torus, in_specs=in_specs, out_specs=out_specs, check_vma=False
    )
```

```python
import math

import jax
import jax.numpy as jnp
import numpy as np
from jax import lax
from jax.experimental import pallas as pl
from jax.experimental.pallas import tpu as pltpu
from jax.sharding import Mesh
from jax.sharding import PartitionSpec as P

PPC = 5
TILE = 128
SUB = 4
NAXES = 1024
NSHELL = 64
NX, NY, NZ = 128, 256, 128
GX_GY_GZ = ("gx", "gy_0", "gy_1", "gz_0", "gz_1")
GY = ("gy_0", "gy_1")
GZ = ("gz_0", "gz_1")
GY_GZ = ("gy_0", "gy_1", "gz_0", "gz_1")
ROT_COS = math.cos(130.0 * math.pi / 180.0)
ROT_SIN = math.sin(130.0 * math.pi / 180.0)
F32 = jnp.float32
BF16 = jnp.bfloat16
TILES = 128
ROWS = 160
SROW = 36
LROW = 68
BLOCKS = 1
GROUPS = TILES // 8 // BLOCKS
STEPS = 8
EARLY = 6
PARTS = TILES // 8 // STEPS


def axis_vectors(axis_index):
    level = 1.0 - (2.0 * axis_index.astype(F32) + 1.0) / NAXES
    radius = jnp.sqrt(1.0 - level * level)
    whole_turns = (axis_index * 1597).astype(F32) * (1.0 / 2584.0)
    turn = (axis_index * 1597 - 2584 * jnp.floor(whole_turns).astype(jnp.int32)).astype(F32)
    turn = turn * (2.0 * math.pi / 2584.0)
    return radius * jnp.cos(turn), radius * jnp.sin(turn), level


def iota(shape, dim):
    return lax.broadcasted_iota(jnp.int32, shape, dim)


def lroll(x, amount):
    amount %= 128
    return pltpu.roll(x, amount, 1) if amount else x


def sroll(x, amount):
    return pltpu.roll(x, amount % x.shape[0], 0)


def split(x):
    high = x.astype(BF16)
    return high, (x - high.astype(F32)).astype(BF16)


def dot(a, b):
    return jnp.dot(a, b, preferred_element_type=F32)


def particle_codes(place, grid_shift):
    bit_x = (((place >> 4) & 3) + grid_shift[0] >= SUB).astype(jnp.int32)
    bit_y = (((place >> 2) & 3) + grid_shift[1] >= SUB).astype(jnp.int32)
    bit_z = ((place & 3) + grid_shift[2] >= SUB).astype(jnp.int32)
    return (place >> 6) * 8 + bit_x * 4 + bit_y * 2 + bit_z


def tile_row(rows, t):
    return jnp.concatenate([rows[PPC * t + r : PPC * t + r + 1, :] for r in range(PPC)], axis=1)


def onehot_of(member, t, cells):
    return jnp.concatenate(
        [
            jnp.where(
                cells
                == jnp.broadcast_to(
                    member[PPC * t + r : PPC * t + r + 1, :], cells.shape
                ).astype(BF16),
                jnp.ones(cells.shape, BF16),
                jnp.zeros(cells.shape, BF16),
            )
            for r in range(PPC)
        ],
        axis=1,
    )


def scatter_body(v_ref, p_ref, axis_ref, s_ref, n_ref, xlo_ref, xhi_ref, turn_ref):
    step = pl.program_id(0)
    cells = iota((TILE, TILE), 0).astype(F32).astype(BF16)
    upper = iota((8, TILE), 0) < 4

    def group(g, carry):
        codes = p_ref[pl.ds(pl.multiple_of(g * 40, 8), 40), :]
        member = (codes >> 3).astype(F32)
        octant = codes & 7
        speed = v_ref[:, pl.ds(pl.multiple_of(g * 5120, 128), 5120)]
        high = speed.astype(BF16).astype(F32)
        low = speed - high
        one = jnp.ones((1, 640), F32)
        zero = jnp.zeros((1, 640), F32)
        for t in range(8):
            here = slice(t * 640, (t + 1) * 640)
            onehot = onehot_of(member, t, cells)
            code = jnp.broadcast_to(tile_row(octant, t), (8, 640))
            values = jnp.concatenate([high[:, here], one, low[:, here], zero], axis=0)
            weighted = jnp.concatenate(
                [jnp.where(code == o, values, 0.0) for o in range(8)], axis=0
            ).astype(BF16)
            sums = lax.dot_general(
                onehot, weighted, (((1,), (1,)), ((), ())), preferred_element_type=F32
            ).T
            for pair in range(4):
                even = sums[16 * pair : 16 * pair + 8]
                odd = sums[16 * pair + 8 : 16 * pair + 16]
                both = jnp.where(upper, even + sroll(even, 4), odd + sroll(odd, 4))
                turn_ref[SROW * t + 8 * pair : SROW * t + 8 * pair + 8, :] = both
        first = pl.multiple_of((step * GROUPS + g) * 8, 8)
        for r in range(32):
            s_ref[r, pl.ds(first, 8), :] = turn_ref[pl.ds(r, 8, stride=SROW), :]
        return carry

    lax.fori_loop(0, GROUPS, group, 0)

    @pl.when(step == BLOCKS - 1)
    def _():
        for c, part in enumerate(axis_vectors(axis_ref[...])):
            n_ref[c] = part
        z = iota((32, 128), 1) & 15
        lane = iota((40, 128), 1)
        pad = jnp.zeros((8, 128), F32)
        low_face = jnp.zeros((40, 128), F32)
        high_face = jnp.zeros((40, 128), F32)
        for q in range(5):
            faces = []
            for bx in range(2):
                parts = []
                for by in range(2):
                    base = bx * 4 + by * 2
                    rows = pl.ds(3 * bx, 32, stride=4)
                    if q < 4:
                        above = s_ref[(base + 1) * 4 + q, rows, :]
                        part = s_ref[base * 4 + q, rows, :] + jnp.where(z > 0, lroll(above, 1), 0.0)
                    else:
                        part = jnp.zeros((32, 128), F32)
                        for k in range(4):
                            above = s_ref[(base + 1) * 4 + k, rows, :]
                            part = jnp.where(z == k, lroll(above, k - 15), part)
                    parts.append(jnp.concatenate([part, pad], axis=0))
                faces.append(parts[0] + sroll(parts[1], 1))
            inside = (lane >> 4) == q if q < 4 else (lane >> 2) == 16
            low_face = jnp.where(inside, lroll(faces[0], 16 * q), low_face)
            high_face = jnp.where(inside, lroll(faces[1], 16 * q - 112), high_face)
        for c in range(3):
            inside = ((lane >> 4) == 5 + c) & (iota((40, 128), 0) < 32)
            face = jnp.concatenate([n_ref[c, pl.ds(0, 32, stride=4), :], pad], axis=0)
            low_face = jnp.where(inside, lroll(face, 80 + 16 * c), low_face)
        xlo_ref[...] = low_face
        xhi_ref[...] = high_face


def plane_body(s_ref, n_ref, m_ref, ylo_ref, yhi_ref, zlo_ref, zhi_ref, edge_ref, zed_ref):
    lane = iota((TILES, 128), 1)
    row = iota((TILES, 128), 0)
    z = lane & 15
    x_in = lane >> 4
    x_out = row & 3
    last = (x_in == 7) & (x_out == 3)

    def x_shift(plane):
        rolled = lroll(plane, 16)
        return jnp.where(
            x_in > 0, rolled, jnp.where(x_out > 0, sroll(rolled, 1), 0.0)
        )

    for q in range(5):
        for by in range(2):
            parts = []
            for bx in range(2):
                base = bx * 4 + by * 2
                if q < 4:
                    above = s_ref[(base + 1) * 4 + q]
                    parts.append(
                        s_ref[base * 4 + q] + jnp.where(z > 0, lroll(above, 1), 0.0)
                    )
                else:
                    rim = jnp.zeros((TILES, 128), F32)
                    for k in range(4):
                        rim = jnp.where(z == k, lroll(s_ref[(base + 1) * 4 + k], k - 15), rim)
                    parts.append(rim)
            main = parts[0] + x_shift(parts[1])
            edge = jnp.where(last, parts[1], 0.0)
            dst = m_ref if q < 4 else zed_ref
            at = q if q < 4 else 0
            if by == 0:
                dst[at, 0:TILES, :] = main
                dst[at, TILES:ROWS, :] = jnp.zeros((ROWS - TILES, 128), F32)
                edge_ref[q, 0:TILES, :] = edge
                edge_ref[q, TILES:ROWS, :] = jnp.zeros((ROWS - TILES, 128), F32)
            else:
                dst[at, 4:132, :] = dst[at, 4:132, :] + main
                edge_ref[q, 4:132, :] = edge_ref[q, 4:132, :] + edge
    ylo_ref[...] = jnp.zeros((40, 128), F32)
    yhi_ref[...] = jnp.zeros((40, 128), F32)
    for q in range(5):
        src = m_ref if q < 4 else zed_ref
        at = q if q < 4 else 0
        ylo_ref[4 * q : 4 * q + 4, :] = src[at, 0:4, :]
        yhi_ref[4 * q : 4 * q + 4, :] = src[at, 128:132, :]
    for c in range(3):
        ylo_ref[20 + 4 * c : 24 + 4 * c, :] = n_ref[c, 0:4, :]
    big = iota((ROWS, 128), 1)
    slot = big & 15
    low_z = jnp.zeros((ROWS, 128), F32)
    for q in range(4):
        low_z = jnp.where(slot == q, lroll(m_ref[q], q), low_z)
    for c in range(3):
        face = jnp.concatenate([n_ref[c], jnp.zeros((ROWS - TILES, 128), F32)], axis=0)
        low_z = jnp.where(slot == 4 + c, lroll(face, 4 + c), low_z)
    zlo_ref[...] = low_z
    zhi_ref[...] = zed_ref[0]


def fold_x_body(xlo_ref, xhi_ref, from_low, from_high, ylo_ref, yhi_ref,
                xlo_out, xhi_out, ylo_out, yhi_out):
    low = xlo_ref[...] + from_low[...]
    high = xhi_ref[...] + from_high[...]
    xlo_out[...] = low
    xhi_out[...] = high
    lane = iota((1, 128), 1)
    for src, dst, y in ((ylo_ref, ylo_out, 0), (yhi_ref, yhi_out, 32)):
        dst[...] = src[...]
        for q in range(4):
            dst[4 * q : 4 * q + 1, :] = jnp.where(
                lane < 16, lroll(low[y : y + 1], -16 * q), src[4 * q : 4 * q + 1, :]
            )
        dst[16:17, :] = jnp.where(lane < 4, lroll(low[y : y + 1], -64), src[16:17, :])
        dst[32:33, :] = high[y : y + 1]


def fold_y_body(ylo_ref, yhi_ref, from_low, from_high, xlo_ref, xhi_ref, zlo_ref, zhi_ref,
                ylo_out, yhi_out, zlo_out, zhi_out):
    low = ylo_ref[...] + from_low[...]
    high = yhi_ref[...] + from_high[...]
    ylo_out[...] = low
    yhi_out[...] = high
    zlo_out[...] = zlo_ref[...]
    zhi_out[...] = zhi_ref[...]
    x_low = xlo_ref[...]
    x_high = xhi_ref[...]
    lane = iota((40, 128), 1)
    lo0 = zlo_out[pl.ds(0, 40, stride=4), :]
    hi0 = zhi_out[pl.ds(0, 40, stride=4), :]
    lo3 = zlo_out[pl.ds(3, 40, stride=4), :]
    hi3 = zhi_out[pl.ds(3, 40, stride=4), :]
    for q in range(4):
        lo0 = jnp.where(lane == q, lroll(x_low, q - 16 * q), lo0)
        lo3 = jnp.where(lane == 120 + q, lroll(x_high, 120 + q - 16 * q), lo3)
    for c in range(3):
        lo3 = jnp.where(lane == 124 + c, lroll(x_high, 124 + c - 80 - 16 * c), lo3)
    hi0 = jnp.where(lane < 4, lroll(x_low, -64), hi0)
    hi3 = jnp.where((lane >= 120) & (lane < 124), lroll(x_high, 120 - 64), hi3)
    zlo_out[pl.ds(0, 40, stride=4), :] = lo0
    zhi_out[pl.ds(0, 40, stride=4), :] = hi0
    zlo_out[pl.ds(3, 40, stride=4), :] = lo3
    zhi_out[pl.ds(3, 40, stride=4), :] = hi3
    lane4 = iota((4, 128), 1)
    slot = lane4 & 15
    corner = (iota((4, 128), 0) == 3) & (lane4 >= 120)
    for face, first in ((low, 0), (high, 128)):
        lo = jnp.zeros((4, 128), F32)
        for q in range(4):
            lo = jnp.where(slot == q, lroll(face[4 * q : 4 * q + 4], q), lo)
        for c in range(3):
            lo = jnp.where(slot == 4 + c, lroll(face[20 + 4 * c : 24 + 4 * c], 4 + c), lo)
        end = face[32:33]
        tail = jnp.zeros((1, 128), F32)
        lane1 = iota((1, 128), 1)
        for q in range(4):
            tail = jnp.where(lane1 == 120 + q, lroll(end, 120 + q - 16 * q), tail)
        for c in range(3):
            tail = jnp.where(lane1 == 124 + c, lroll(end, 124 + c - 80 - 16 * c), tail)
        zlo_out[first : first + 4, :] = jnp.where(corner, tail, lo)
        hi = jnp.where(slot < 4, face[16:20], 0.0)
        zhi_out[first : first + 4, :] = jnp.where(
            corner, jnp.where(lane1 < 124, lroll(end, 120 - 64), 0.0), hi
        )


VROWS = 136


def cell_body(s_ref, m_ref, n_ref, xlo_ref, xhi_ref, ylo_ref, yhi_ref, zlo_ref, zhi_ref,
              from_low, from_high, view_ref, send_ref, ext_ref, end_ref, vel_ref):
    z_low = zlo_ref[0:VROWS, :] + from_low[0:VROWS, :]
    z_high = zhi_ref[0:VROWS, :] + from_high[0:VROWS, :]
    x_low = xlo_ref[...]
    x_high = xhi_ref[...]
    y_low = ylo_ref[...]
    y_high = yhi_ref[...]
    lane40 = iota((40, 128), 1)
    lane = iota((VROWS, 128), 1)
    row = iota((VROWS, 128), 0)
    z = lane & 15
    x_in = lane >> 4
    x_out = row & 3
    for k in range(7):
        if k < 4:
            ext_ref[k] = m_ref[k]
            held = ext_ref[k, pl.ds(0, 40, stride=4), :]
            ext_ref[k, pl.ds(0, 40, stride=4), :] = jnp.where(
                lane40 < 16, lroll(x_low, -16 * k), held
            )
            ext_ref[k, 0:4, :] = y_low[4 * k : 4 * k + 4]
            ext_ref[k, 128:132, :] = y_high[4 * k : 4 * k + 4]
            amount = 112 - 16 * k
        else:
            c = k - 4
            ext_ref[k, 0:TILES, :] = n_ref[c]
            ext_ref[k, 128:132, :] = y_high[20 + 4 * c : 24 + 4 * c]
            amount = 32 - 16 * c
        end_ref[k, pl.ds(3, 40, stride=4), :] = lroll(x_high, amount)
        end_ref[k, 131:132, :] = lroll(y_high[32:33], amount)
        if k < 4:
            end_ref[k, 3:4, :] = lroll(y_low[32:33], amount)

    def pair(k):
        main = ext_ref[k, 0:VROWS, :]
        end = end_ref[k, 0:VROWS, :]
        if k < 4:
            main = jnp.where(z == 0, lroll(z_low, -k), main)
            end = jnp.where(z == 0, lroll(z_low, -8 - k), end)
        main1 = jnp.where(z < 15, lroll(main, -1), lroll(z_high, 15 - k))
        end1 = jnp.where(z < 15, lroll(end, -1), lroll(z_high, 7 - k))
        return (main, main1), (end, end1)

    count_main, count_end = pair(3)
    inv_main = [1.0 / jnp.maximum(a, 1.0) for a in count_main]
    inv_end = [1.0 / jnp.maximum(a, 1.0) for a in count_end]
    for slot, k in enumerate((0, 1, 2, 4, 5, 6)):
        mains, ends = pair(k)
        for bz in range(2):
            main, end = mains[bz], ends[bz]
            if k < 3:
                main = main * inv_main[bz]
                end = end * inv_end[bz]
            rolled = lroll(main, -16)
            ahead = jnp.where(x_in < 7, rolled, jnp.where(x_out == 3, end, sroll(rolled, -1)))
            view_ref[bz * 6 + slot] = main
            view_ref[(2 + bz) * 6 + slot] = ahead

    def group(g, carry):
        first = pl.multiple_of(g * 8, 8)
        acc = [jnp.zeros((8, 128), F32) for _ in range(3)]
        total = jnp.zeros((8, 128), F32)
        for bx in range(2):
            for bz in range(2):
                wide = [view_ref[(bx * 2 + bz) * 6 + k, pl.ds(first, 16), :] for k in range(6)]
                for by in range(2):
                    o = bx * 4 + by * 2 + bz
                    ux, uy, uz, nx, ny, nz = [w[4 * by : 4 * by + 8] for w in wide]
                    sx, sy, sz, num = [s_ref[o * 4 + q, pl.ds(first, 8), :] for q in range(4)]
                    mx, my, mz = num * ux, num * uy, num * uz
                    wx, wy, wz = sx - mx, sy - my, sz - mz
                    along = (1.0 - ROT_COS) * (nx * wx + ny * wy + nz * wz)
                    acc[0] += mx + ROT_COS * wx + ROT_SIN * (ny * wz - nz * wy) + along * nx
                    acc[1] += my + ROT_COS * wy + ROT_SIN * (nz * wx - nx * wz) + along * ny
                    acc[2] += mz + ROT_COS * wz + ROT_SIN * (nx * wy - ny * wx) + along * nz
                    total += num
        inverse = 1.0 / jnp.maximum(total, 1.0)
        for c in range(3):
            vel_ref[c, pl.ds(first, 8), :] = acc[c] * inverse
        return carry

    lax.fori_loop(0, TILES // 8, group, 0)
    lane = iota((TILES, 128), 1)
    row = iota((TILES, 128), 0)
    for c in range(3):
        plane = vel_ref[c]
        for bit in range(4):
            size = 1 << bit
            row_bit = (row >> bit) & 1
            lane_bit = (lane >> bit) & 1
            down = sroll(lroll(plane, size), -size)
            up = sroll(lroll(plane, -size), size)
            plane = jnp.where(row_bit == lane_bit, plane, jnp.where(row_bit == 0, down, up))
        for part in range(8):
            send_ref[part, 64 * c : 64 * c + 64, :] = plane[64 * (part // 4) : 64 * (part // 4) + 64]


def collide_body(start, v_ref, p_ref, view_ref, *refs):
    out_ref, turn_ref = refs[-2:]
    step = pl.program_id(0) + start
    cells = iota((TILE, TILE), 0).astype(F32).astype(BF16)

    @pl.when(step == start)
    def _():
        turn_ref[...] = jnp.zeros(turn_ref.shape, F32)

    def group(g, carry):
        codes = p_ref[pl.ds(pl.multiple_of(g * 40, 8), 40), :]
        member = (codes >> 3).astype(F32)
        octant = codes & 7
        first = pl.multiple_of((step * PARTS + g) * 8, 8)
        for bx in range(2):
            for bz in range(2):
                for k in range(6):
                    wide = view_ref[(bx * 2 + bz) * 6 + k, pl.ds(first, 16), :]
                    for by in range(2):
                        o = bx * 4 + by * 2 + bz
                        turn_ref[pl.ds(8 * o + k, 8, stride=LROW), :] = wide[4 * by : 4 * by + 8]
        for t in range(8):
            high, low = split(turn_ref[LROW * t : LROW * t + 64, :])
            onehot = onehot_of(member, t, cells)
            picked = dot(
                jnp.concatenate([high, low], axis=1), jnp.concatenate([onehot, onehot], axis=0)
            )
            code = jnp.broadcast_to(tile_row(octant, t), (8, 640))
            chosen = picked[0:8]
            for o in range(1, 8):
                chosen = jnp.where(code == o, picked[8 * o : 8 * o + 8], chosen)
            speed = v_ref[:, pl.ds(pl.multiple_of(g * 5120 + t * 640, 128), 640)]
            ux, uy, uz, nx, ny, nz = [chosen[k : k + 1] for k in range(6)]
            wx, wy, wz = speed[0:1] - ux, speed[1:2] - uy, speed[2:3] - uz
            along = (1.0 - ROT_COS) * (nx * wx + ny * wy + nz * wz)
            new = [
                ux + ROT_COS * wx + ROT_SIN * (ny * wz - nz * wy) + along * nx,
                uy + ROT_COS * wy + ROT_SIN * (nz * wx - nx * wz) + along * ny,
                uz + ROT_COS * wz + ROT_SIN * (nx * wy - ny * wx) + along * nz,
            ]
            out_ref[:, pl.ds(pl.multiple_of(g * 5120 + t * 640, 128), 640)] = jnp.concatenate(
                new, axis=0
            )
        return carry

    lax.fori_loop(0, PARTS, group, 0)


def table_parts(table):
    table = np.asarray(table, np.float32)
    high = table.astype(BF16)
    low = (table - high.astype(np.float32)).astype(BF16)
    return high, low


def z_tables():
    pos = np.arange(NZ)[None, :]
    line = np.arange(16)[:, None]
    quarters = []
    for quarter in range(4):
        owner = line // 2 * 8 + line % 2 * 4 + quarter
        for q in range(4):
            phase = (2 * owner + q // 2) * pos % NZ * (2.0 * np.pi / NZ)
            quarters.append(-np.sin(phase) if q % 2 else np.cos(phase))
    return table_parts(np.concatenate(quarters, axis=0).reshape(4, 64, NZ))


def y_tables():
    phase = np.arange(NY)[:, None] * np.arange(NY)[None, :] % NY * (2.0 * np.pi / NY)
    return table_parts(np.concatenate([np.cos(phase), np.sin(phase)], axis=0))


def x_tables():
    k = np.arange(512)
    lane = k % 128
    x = k // 128 * 32 + (lane & 3) * 8 + lane // 16
    kz = (lane >> 3) & 1
    part = (lane >> 2) & 1
    n = np.arange(512)
    part_out, kz_out, kx = n // 256, n // 128 % 2, n % 128
    phase = x[:, None] * kx[None, :] % NX * (2.0 * np.pi / NX)
    same = kz[:, None] == kz_out[None, :]
    c, s = np.cos(phase), np.sin(phase)
    real = np.where(part[:, None] == 0, c, s)
    imag = np.where(part[:, None] == 0, -s, c)
    table = np.where(part_out[None, :] == 0, real, imag) * same / math.sqrt(NX * NY * NZ)
    return table_parts(table)


def shell_counts():
    def wave(n):
        k = np.arange(n)
        return np.where(k >= n // 2, k - n, k)

    square = wave(NZ)[:, None, None] ** 2 + wave(NY)[None, :, None] ** 2 + wave(NX)[None, None, :] ** 2
    edges = np.arange(NSHELL + 1) ** 2
    below = np.searchsorted(np.sort(square.reshape(-1)), edges, side="left")
    return np.diff(below).astype(np.float32)


def z_body(first_ref, in_ref, fh_ref, fl_ref, out_ref):
    lane = iota((16, 128), 1)
    fh, fl = fh_ref[first_ref[2]], fl_ref[first_ref[2]]
    for c in range(3):
        data = jnp.concatenate(
            [
                in_ref[:, 64 * c + 16 * r : 64 * c + 16 * r + 16, :].reshape(128, 128)
                for r in range(4)
            ],
            axis=1,
        )
        high, low = split(data)
        res = dot(fh, high) + dot(fh, low) + dot(fl, high)
        for r in range(4):
            g = [res[16 * q : 16 * q + 16, 128 * r : 128 * r + 128] for q in range(4)]
            for bit, size in ((2, 8), (1, 4)):
                clear = (lane & size) == 0
                new = list(g)
                for q in range(4):
                    if not q & bit:
                        a, b = g[q], g[q | bit]
                        new[q] = jnp.where(clear, a, lroll(b, size))
                        new[q | bit] = jnp.where(clear, lroll(a, -size), b)
                g = new
            for k in range(4):
                out_ref[pl.ds(16 * c + 4 * r + k, 16, stride=48), :] = g[k]


def y_body(in_ref, fh_ref, fl_ref, out_ref):
    both = in_ref[...].reshape(16, 48, 128)
    data = jnp.concatenate(
        [both[:, 16 * c : 16 * c + 16].reshape(256, 128) for c in range(3)], axis=1
    )
    high, low = split(data)
    fh, fl = fh_ref[...], fl_ref[...]
    res = dot(fh, high) + dot(fh, low) + dot(fl, high)
    is_real = (iota((256, 128), 1) & 4) == 0
    for c in range(3):
        even = res[0:256, 128 * c : 128 * c + 128]
        odd = res[256:512, 128 * c : 128 * c + 128]
        out = even + jnp.where(is_real, lroll(odd, -4), -lroll(odd, 4))
        for d in range(4):
            out_ref[d, 64 * c : 64 * c + 64, :] = out[64 * d : 64 * d + 64]
            out_ref[d, 192 + 64 * c : 256 + 64 * c, :] = out[0:64]


def x_body(first_ref, in_ref, fh_ref, fl_ref, modes_ref, shell_ref, sums_ref, out_ref, sem):
    data = jnp.concatenate([in_ref[s] for s in range(4)], axis=1)
    high, low = split(data)
    fh, fl = fh_ref[...], fl_ref[...]
    res = dot(high, fh) + dot(low, fh) + dot(high, fl)
    ky = iota((64, 128), 0)
    kx = iota((64, 128), 1)
    kx = jnp.where(kx >= NX // 2, kx - NX, kx)
    plane = ky * ky + kx * kx
    weight = jnp.where(ky == 0, 1.0, 2.0)
    energy, square = [], []
    for kz in range(2):
        total = jnp.zeros((64, 128), F32)
        for part in range(2):
            for c in range(3):
                here = slice(256 * part + 128 * kz, 256 * part + 128 * kz + 128)
                out_ref[part, c, kz] = res[64 * c : 64 * c + 64, here]
                block = res[192 + 64 * c : 256 + 64 * c, here]
                total += block * block
        wave = first_ref[0] + kz
        wave = jnp.where(wave >= NZ // 2, wave - NZ, wave)
        energy.append(total * weight)
        square.append(plane + wave * wave)
    modes_copy = pltpu.make_async_copy(out_ref, modes_ref, sem)
    modes_copy.start()
    energy = jnp.concatenate(energy, axis=0)
    square = jnp.concatenate(square, axis=0)
    for s in range(NSHELL):
        kept = jnp.where(square < (s + 1) * (s + 1), energy, 0.0)
        sums_ref[s : s + 1, :] = jnp.sum(kept, axis=0, keepdims=True)
    cumulative = sums_ref[...]
    before = jnp.where(iota((NSHELL, 128), 0) == 0, 0.0, sroll(cumulative, 1))
    own = jnp.concatenate([cumulative - before, jnp.zeros((64, 128), F32)], axis=0)
    shell_ref[...] = jnp.sum(own.T, axis=0, keepdims=True)
    modes_copy.wait()


def struct(*shape):
    return jax.ShapeDtypeStruct(shape, F32)


SMEM = pl.BlockSpec(memory_space=pltpu.SMEM)


def ring(x, axis):
    count = lax.axis_size(axis)
    forward = [(i, (i + 1) % count) for i in range(count)]
    backward = [(target, source) for source, target in forward]
    low, high = x
    return lax.ppermute(high, axis, forward), lax.ppermute(low, axis, backward)


def gathered_sum(x, axes):
    count = lax.axis_size(axes)
    copies = jnp.broadcast_to(x[None], (count, *x.shape))
    return jnp.sum(lax.all_to_all(copies, axes, split_axis=0, concat_axis=0, tiled=True), axis=0)


def params(mib):
    return pltpu.CompilerParams(vmem_limit_bytes=mib * 1024 * 1024)


def whole(*shape):
    return pl.BlockSpec(shape, lambda i: (0,) * len(shape))


def collide(start, stop, velocity, codes, views, earlier):
    span = TILES * TILE * PPC // STEPS
    speed_spec = pl.BlockSpec((3, span), lambda i: (0, i + start))
    place_spec = pl.BlockSpec((640 // STEPS, 128), lambda i: (i + start, 0))
    more = [] if earlier is None else [earlier]
    return pl.pallas_call(
        lambda *refs: collide_body(start, *refs),
        name="collide",
        grid=(stop - start,),
        in_specs=[speed_spec, place_spec, whole(24, VROWS, 128)]
        + [pl.BlockSpec(memory_space=pl.ANY)] * len(more),
        out_specs=speed_spec,
        out_shape=struct(*velocity.shape),
        scratch_shapes=[pltpu.VMEM((8 * LROW, 128), F32)],
        input_output_aliases={3: 0} if more else {},
        compiler_params=params(12),
        cost_estimate=pl.CostEstimate(
            flops=800_000_000 * (stop - start), bytes_accessed=4_000_000, transcendentals=0
        ),
    )(velocity, codes, views, *more)


def per_device(velocity, particle_place, grid_shift, rotation_axis):
    codes = particle_codes(particle_place, grid_shift).reshape(640, 128)
    axis_index = rotation_axis.reshape(TILES, 128)
    span = TILES * TILE * PPC // BLOCKS
    speed_spec = pl.BlockSpec((3, span), lambda i: (0, i))
    place_spec = pl.BlockSpec((640 // BLOCKS, 128), lambda i: (i, 0))
    out_shapes = [(32, TILES, 128), (3, TILES, 128), (40, 128), (40, 128)]
    sums, normal, x_lo, x_hi = pl.pallas_call(
        scatter_body,
        name="scatter",
        grid=(BLOCKS,),
        in_specs=[speed_spec, place_spec, whole(TILES, 128)],
        out_specs=[whole(*s) for s in out_shapes],
        out_shape=[struct(*s) for s in out_shapes],
        scratch_shapes=[pltpu.VMEM((8 * SROW, 128), F32)],
        compiler_params=params(12),
    )(velocity, codes, axis_index)
    main, y_lo, y_hi, z_lo, z_hi = pl.pallas_call(
        plane_body,
        name="planes",
        out_shape=[struct(4, ROWS, 128)] + [struct(40, 128)] * 2 + [struct(ROWS, 128)] * 2,
        scratch_shapes=[pltpu.VMEM((5, ROWS, 128), F32), pltpu.VMEM((1, ROWS, 128), F32)],
        compiler_params=params(12),
        cost_estimate=pl.CostEstimate(flops=1_000_000_000, bytes_accessed=3_000_000, transcendentals=0),
    )(sums, normal)
    below, above = ring((x_lo, x_hi), "gx")
    x_lo, x_hi, y_lo, y_hi = pl.pallas_call(
        fold_x_body, name="fold_x", out_shape=[struct(40, 128)] * 4, compiler_params=params(2)
    )(x_lo, x_hi, below, above, y_lo, y_hi)
    below, above = ring((y_lo, y_hi), GY)
    y_lo, y_hi, z_lo, z_hi = pl.pallas_call(
        fold_y_body, name="fold_y", out_shape=[struct(40, 128)] * 2 + [struct(ROWS, 128)] * 2,
        compiler_params=params(3),
    )(y_lo, y_hi, below, above, x_lo, x_hi, z_lo, z_hi)
    below, above = ring((z_lo, z_hi), GZ)
    views, sent = pl.pallas_call(
        cell_body,
        name="cells",
        out_shape=[struct(24, VROWS, 128), struct(8, 192, 128)],
        scratch_shapes=[
            pltpu.VMEM((7, ROWS, 128), F32),
            pltpu.VMEM((7, ROWS, 128), F32),
            pltpu.VMEM((3, TILES, 128), F32),
        ],
        compiler_params=params(12),
    )(sums, main, normal, x_lo, x_hi, y_lo, y_hi, z_lo, z_hi, below, above)
    first = jnp.stack(
        [lax.axis_index(GY_GZ) * 2, lax.axis_index("gx") * 64, lax.axis_index("gz_1")]
    ).astype(jnp.int32)
    arrived = lax.all_to_all(sent, GZ, split_axis=0, concat_axis=0, tiled=True)
    updated = collide(0, EARLY, velocity, codes, views, None)
    arrived, updated = lax.optimization_barrier((arrived, updated))
    vmem = pl.BlockSpec(memory_space=pltpu.VMEM)
    lines = pl.pallas_call(
        z_body,
        name="z_lines",
        in_specs=[SMEM, vmem, vmem, vmem],
        out_shape=struct(768, 128),
        compiler_params=params(6),
    )(first, arrived, *z_tables())
    pencil = lax.all_to_all(
        lines.reshape(16, 48, 128), ("gy_0", "gy_1", "gz_0"), split_axis=0, concat_axis=0, tiled=True
    )
    new_velocity = collide(EARLY, STEPS, velocity, codes, views, updated)
    pencil, new_velocity = lax.optimization_barrier((pencil, new_velocity))
    rows = pl.pallas_call(y_body, name="y_lines", out_shape=struct(4, 384, 128), compiler_params=params(12))(
        pencil.reshape(768, 128), *y_tables()
    )
    columns = lax.all_to_all(rows, "gx", split_axis=0, concat_axis=0, tiled=True)
    modes, shells = pl.pallas_call(
        x_body,
        name="x_lines",
        in_specs=[SMEM, vmem, vmem, vmem],
        out_shape=[struct(2, 3, 2, 64, 128), struct(1, 128)],
        out_specs=[pl.BlockSpec(memory_space=pl.ANY), vmem],
        scratch_shapes=[
            pltpu.VMEM((NSHELL, 128), F32),
            pltpu.VMEM((2, 3, 2, 64, 128), F32),
            pltpu.SemaphoreType.DMA,
        ],
        compiler_params=params(12),
    )(first, columns, *x_tables())
    total = gathered_sum(shells, GY_GZ)
    spectrum = total[0, :NSHELL] / shell_counts()
    return new_velocity, modes, spectrum


def solution(mesh):
    torus = Mesh(
        mesh.devices.reshape(mesh.shape["gx"], 4, 2, 2, 4), ("gx", "gy_0", "gy_1", "gz_0", "gz_1")
    )
    in_specs = (P(None, GX_GY_GZ), P(GX_GY_GZ), P(), P(GY, "gx", GZ))
    out_specs = (P(None, GX_GY_GZ), P(None, None, GY_GZ, "gx", None), P())
    return jax.shard_map(
        per_device, mesh=torus, in_specs=in_specs, out_specs=out_specs, check_vma=False
    )
```

```python
import math

import jax
import jax.numpy as jnp
import numpy as np
from jax import lax
from jax.experimental import pallas as pl
from jax.experimental.pallas import tpu as pltpu
from jax.sharding import Mesh
from jax.sharding import PartitionSpec as P

PPC = 5
TILE = 128
SUB = 4
NAXES = 1024
NSHELL = 64
NX, NY, NZ = 128, 256, 128
GX_GY_GZ = ("gx", "gy_0", "gy_1", "gz_0", "gz_1")
GY = ("gy_0", "gy_1")
GZ = ("gz_0", "gz_1")
GY_GZ = ("gy_0", "gy_1", "gz_0", "gz_1")
ROT_COS = math.cos(130.0 * math.pi / 180.0)
ROT_SIN = math.sin(130.0 * math.pi / 180.0)
F32 = jnp.float32
BF16 = jnp.bfloat16
TILES = 128
ROWS = 160
SROW = 36
LROW = 68
BLOCKS = 1
GROUPS = TILES // 8 // BLOCKS
STEPS = 8
EARLY = 5
PARTS = TILES // 8 // STEPS


def axis_vectors(axis_index):
    level = 1.0 - (2.0 * axis_index.astype(F32) + 1.0) / NAXES
    radius = jnp.sqrt(1.0 - level * level)
    whole_turns = (axis_index * 1597).astype(F32) * (1.0 / 2584.0)
    turn = (axis_index * 1597 - 2584 * jnp.floor(whole_turns).astype(jnp.int32)).astype(F32)
    turn = turn * (2.0 * math.pi / 2584.0)
    return radius * jnp.cos(turn), radius * jnp.sin(turn), level


def iota(shape, dim):
    return lax.broadcasted_iota(jnp.int32, shape, dim)


def lroll(x, amount):
    amount %= 128
    return pltpu.roll(x, amount, 1) if amount else x


def sroll(x, amount):
    return pltpu.roll(x, amount % x.shape[0], 0)


def split(x):
    high = x.astype(BF16)
    return high, (x - high.astype(F32)).astype(BF16)


def dot(a, b):
    return jnp.dot(a, b, preferred_element_type=F32)


def octants(place, shift_ref):
    bit_x = (((place >> 4) & 3) + shift_ref[0] >= SUB).astype(jnp.int32)
    bit_y = (((place >> 2) & 3) + shift_ref[1] >= SUB).astype(jnp.int32)
    bit_z = ((place & 3) + shift_ref[2] >= SUB).astype(jnp.int32)
    return bit_x * 4 + bit_y * 2 + bit_z


def tile_row(rows, t):
    return jnp.concatenate([rows[PPC * t + r : PPC * t + r + 1, :] for r in range(PPC)], axis=1)


def onehot_of(member, t, cells):
    return jnp.concatenate(
        [
            jnp.where(
                cells
                == jnp.broadcast_to(
                    member[PPC * t + r : PPC * t + r + 1, :], cells.shape
                ).astype(BF16),
                jnp.ones(cells.shape, BF16),
                jnp.zeros(cells.shape, BF16),
            )
            for r in range(PPC)
        ],
        axis=1,
    )


def scatter_body(shift_ref, v_ref, p_ref, axis_ref, s_ref, n_ref, xlo_ref, xhi_ref, turn_ref):
    step = pl.program_id(0)
    cells = iota((TILE, TILE), 0).astype(F32).astype(BF16)
    upper = iota((8, TILE), 0) < 4

    def group(g, carry):
        place = p_ref[pl.ds(pl.multiple_of(g * 40, 8), 40), :]
        member = (place >> 6).astype(F32)
        octant = octants(place, shift_ref)
        speed = v_ref[:, pl.ds(pl.multiple_of(g * 5120, 128), 5120)]
        high = speed.astype(BF16).astype(F32)
        low = speed - high
        one = jnp.ones((1, 640), F32)
        zero = jnp.zeros((1, 640), F32)
        for t in range(8):
            here = slice(t * 640, (t + 1) * 640)
            onehot = onehot_of(member, t, cells)
            code = jnp.broadcast_to(tile_row(octant, t), (8, 640))
            values = jnp.concatenate([high[:, here], one, low[:, here], zero], axis=0)
            weighted = jnp.concatenate(
                [jnp.where(code == o, values, 0.0) for o in range(8)], axis=0
            ).astype(BF16)
            sums = lax.dot_general(
                onehot, weighted, (((1,), (1,)), ((), ())), preferred_element_type=F32
            ).T
            for pair in range(4):
                even = sums[16 * pair : 16 * pair + 8]
                odd = sums[16 * pair + 8 : 16 * pair + 16]
                both = jnp.where(upper, even + sroll(even, 4), odd + sroll(odd, 4))
                turn_ref[SROW * t + 8 * pair : SROW * t + 8 * pair + 8, :] = both
        first = pl.multiple_of((step * GROUPS + g) * 8, 8)
        for c, axis in enumerate(axis_vectors(axis_ref[pl.ds(first, 8), :])):
            n_ref[c, pl.ds(first, 8), :] = axis
        for r in range(32):
            s_ref[r, pl.ds(first, 8), :] = turn_ref[pl.ds(r, 8, stride=SROW), :]
        return carry

    lax.fori_loop(0, GROUPS, group, 0)

    @pl.when(step == BLOCKS - 1)
    def _():
        z = iota((32, 128), 1) & 15
        lane = iota((40, 128), 1)
        pad = jnp.zeros((8, 128), F32)
        low_face = jnp.zeros((40, 128), F32)
        high_face = jnp.zeros((40, 128), F32)
        for q in range(5):
            faces = []
            for bx in range(2):
                parts = []
                for by in range(2):
                    base = bx * 4 + by * 2
                    rows = pl.ds(3 * bx, 32, stride=4)
                    if q < 4:
                        above = s_ref[(base + 1) * 4 + q, rows, :]
                        part = s_ref[base * 4 + q, rows, :] + jnp.where(z > 0, lroll(above, 1), 0.0)
                    else:
                        part = jnp.zeros((32, 128), F32)
                        for k in range(4):
                            above = s_ref[(base + 1) * 4 + k, rows, :]
                            part = jnp.where(z == k, lroll(above, k - 15), part)
                    parts.append(jnp.concatenate([part, pad], axis=0))
                faces.append(parts[0] + sroll(parts[1], 1))
            inside = (lane >> 4) == q if q < 4 else (lane >> 2) == 16
            low_face = jnp.where(inside, lroll(faces[0], 16 * q), low_face)
            high_face = jnp.where(inside, lroll(faces[1], 16 * q - 112), high_face)
        for c in range(3):
            inside = ((lane >> 4) == 5 + c) & (iota((40, 128), 0) < 32)
            face = jnp.concatenate([n_ref[c, pl.ds(0, 32, stride=4), :], pad], axis=0)
            low_face = jnp.where(inside, lroll(face, 80 + 16 * c), low_face)
        xlo_ref[...] = low_face
        xhi_ref[...] = high_face


def plane_body(s_ref, n_ref, m_ref, ylo_ref, yhi_ref, zlo_ref, zhi_ref, edge_ref, zed_ref):
    lane = iota((TILES, 128), 1)
    row = iota((TILES, 128), 0)
    z = lane & 15
    x_in = lane >> 4
    x_out = row & 3
    last = (x_in == 7) & (x_out == 3)

    def x_shift(plane):
        rolled = lroll(plane, 16)
        return jnp.where(
            x_in > 0, rolled, jnp.where(x_out > 0, sroll(rolled, 1), 0.0)
        )

    for q in range(5):
        for by in range(2):
            parts = []
            for bx in range(2):
                base = bx * 4 + by * 2
                if q < 4:
                    above = s_ref[(base + 1) * 4 + q]
                    parts.append(
                        s_ref[base * 4 + q] + jnp.where(z > 0, lroll(above, 1), 0.0)
                    )
                else:
                    rim = jnp.zeros((TILES, 128), F32)
                    for k in range(4):
                        rim = jnp.where(z == k, lroll(s_ref[(base + 1) * 4 + k], k - 15), rim)
                    parts.append(rim)
            main = parts[0] + x_shift(parts[1])
            edge = jnp.where(last, parts[1], 0.0)
            dst = m_ref if q < 4 else zed_ref
            at = q if q < 4 else 0
            if by == 0:
                dst[at, 0:TILES, :] = main
                dst[at, TILES:ROWS, :] = jnp.zeros((ROWS - TILES, 128), F32)
                edge_ref[q, 0:TILES, :] = edge
                edge_ref[q, TILES:ROWS, :] = jnp.zeros((ROWS - TILES, 128), F32)
            else:
                dst[at, 4:132, :] = dst[at, 4:132, :] + main
                edge_ref[q, 4:132, :] = edge_ref[q, 4:132, :] + edge
    ylo_ref[...] = jnp.zeros((40, 128), F32)
    yhi_ref[...] = jnp.zeros((40, 128), F32)
    for q in range(5):
        src = m_ref if q < 4 else zed_ref
        at = q if q < 4 else 0
        ylo_ref[4 * q : 4 * q + 4, :] = src[at, 0:4, :]
        yhi_ref[4 * q : 4 * q + 4, :] = src[at, 128:132, :]
    for c in range(3):
        ylo_ref[20 + 4 * c : 24 + 4 * c, :] = n_ref[c, 0:4, :]
    big = iota((ROWS, 128), 1)
    slot = big & 15
    low_z = jnp.zeros((ROWS, 128), F32)
    for q in range(4):
        low_z = jnp.where(slot == q, lroll(m_ref[q], q), low_z)
    for c in range(3):
        face = jnp.concatenate([n_ref[c], jnp.zeros((ROWS - TILES, 128), F32)], axis=0)
        low_z = jnp.where(slot == 4 + c, lroll(face, 4 + c), low_z)
    zlo_ref[...] = low_z
    zhi_ref[...] = zed_ref[0]


def fold_x_body(xlo_ref, xhi_ref, from_low, from_high, ylo_ref, yhi_ref,
                xlo_out, xhi_out, ylo_out, yhi_out):
    low = xlo_ref[...] + from_low[...]
    high = xhi_ref[...] + from_high[...]
    xlo_out[...] = low
    xhi_out[...] = high
    lane = iota((1, 128), 1)
    for src, dst, y in ((ylo_ref, ylo_out, 0), (yhi_ref, yhi_out, 32)):
        dst[...] = src[...]
        for q in range(4):
            dst[4 * q : 4 * q + 1, :] = jnp.where(
                lane < 16, lroll(low[y : y + 1], -16 * q), src[4 * q : 4 * q + 1, :]
            )
        dst[16:17, :] = jnp.where(lane < 4, lroll(low[y : y + 1], -64), src[16:17, :])
        dst[32:33, :] = high[y : y + 1]


def fold_y_body(ylo_ref, yhi_ref, from_low, from_high, xlo_ref, xhi_ref, zlo_ref, zhi_ref,
                ylo_out, yhi_out, zlo_out, zhi_out):
    low = ylo_ref[...] + from_low[...]
    high = yhi_ref[...] + from_high[...]
    ylo_out[...] = low
    yhi_out[...] = high
    zlo_out[...] = zlo_ref[...]
    zhi_out[...] = zhi_ref[...]
    x_low = xlo_ref[...]
    x_high = xhi_ref[...]
    lane = iota((40, 128), 1)
    lo0 = zlo_out[pl.ds(0, 40, stride=4), :]
    hi0 = zhi_out[pl.ds(0, 40, stride=4), :]
    lo3 = zlo_out[pl.ds(3, 40, stride=4), :]
    hi3 = zhi_out[pl.ds(3, 40, stride=4), :]
    for q in range(4):
        lo0 = jnp.where(lane == q, lroll(x_low, q - 16 * q), lo0)
        lo3 = jnp.where(lane == 120 + q, lroll(x_high, 120 + q - 16 * q), lo3)
    for c in range(3):
        lo3 = jnp.where(lane == 124 + c, lroll(x_high, 124 + c - 80 - 16 * c), lo3)
    hi0 = jnp.where(lane < 4, lroll(x_low, -64), hi0)
    hi3 = jnp.where((lane >= 120) & (lane < 124), lroll(x_high, 120 - 64), hi3)
    zlo_out[pl.ds(0, 40, stride=4), :] = lo0
    zhi_out[pl.ds(0, 40, stride=4), :] = hi0
    zlo_out[pl.ds(3, 40, stride=4), :] = lo3
    zhi_out[pl.ds(3, 40, stride=4), :] = hi3
    lane4 = iota((4, 128), 1)
    slot = lane4 & 15
    corner = (iota((4, 128), 0) == 3) & (lane4 >= 120)
    for face, first in ((low, 0), (high, 128)):
        lo = jnp.zeros((4, 128), F32)
        for q in range(4):
            lo = jnp.where(slot == q, lroll(face[4 * q : 4 * q + 4], q), lo)
        for c in range(3):
            lo = jnp.where(slot == 4 + c, lroll(face[20 + 4 * c : 24 + 4 * c], 4 + c), lo)
        end = face[32:33]
        tail = jnp.zeros((1, 128), F32)
        lane1 = iota((1, 128), 1)
        for q in range(4):
            tail = jnp.where(lane1 == 120 + q, lroll(end, 120 + q - 16 * q), tail)
        for c in range(3):
            tail = jnp.where(lane1 == 124 + c, lroll(end, 124 + c - 80 - 16 * c), tail)
        zlo_out[first : first + 4, :] = jnp.where(corner, tail, lo)
        hi = jnp.where(slot < 4, face[16:20], 0.0)
        zhi_out[first : first + 4, :] = jnp.where(
            corner, jnp.where(lane1 < 124, lroll(end, 120 - 64), 0.0), hi
        )


VROWS = 136


def view_body(m_ref, n_ref, xlo_ref, xhi_ref, ylo_ref, yhi_ref, zlo_ref, zhi_ref,
              from_low, from_high, view_ref, ext_ref, end_ref):
    z_low = zlo_ref[0:VROWS, :] + from_low[0:VROWS, :]
    z_high = zhi_ref[0:VROWS, :] + from_high[0:VROWS, :]
    x_low = xlo_ref[...]
    x_high = xhi_ref[...]
    y_low = ylo_ref[...]
    y_high = yhi_ref[...]
    lane40 = iota((40, 128), 1)
    lane = iota((VROWS, 128), 1)
    row = iota((VROWS, 128), 0)
    z = lane & 15
    x_in = lane >> 4
    x_out = row & 3
    for k in range(7):
        if k < 4:
            ext_ref[k] = m_ref[k]
            held = ext_ref[k, pl.ds(0, 40, stride=4), :]
            ext_ref[k, pl.ds(0, 40, stride=4), :] = jnp.where(
                lane40 < 16, lroll(x_low, -16 * k), held
            )
            ext_ref[k, 0:4, :] = y_low[4 * k : 4 * k + 4]
            ext_ref[k, 128:132, :] = y_high[4 * k : 4 * k + 4]
            amount = 112 - 16 * k
        else:
            c = k - 4
            ext_ref[k, 0:TILES, :] = n_ref[c]
            ext_ref[k, 128:132, :] = y_high[20 + 4 * c : 24 + 4 * c]
            amount = 32 - 16 * c
        end_ref[k, pl.ds(3, 40, stride=4), :] = lroll(x_high, amount)
        end_ref[k, 131:132, :] = lroll(y_high[32:33], amount)
        if k < 4:
            end_ref[k, 3:4, :] = lroll(y_low[32:33], amount)

    def pair(k):
        main = ext_ref[k, 0:VROWS, :]
        end = end_ref[k, 0:VROWS, :]
        if k < 4:
            main = jnp.where(z == 0, lroll(z_low, -k), main)
            end = jnp.where(z == 0, lroll(z_low, -8 - k), end)
        main1 = jnp.where(z < 15, lroll(main, -1), lroll(z_high, 15 - k))
        end1 = jnp.where(z < 15, lroll(end, -1), lroll(z_high, 7 - k))
        return (main, main1), (end, end1)

    count_main, count_end = pair(3)
    inv_main = [1.0 / jnp.maximum(a, 1.0) for a in count_main]
    inv_end = [1.0 / jnp.maximum(a, 1.0) for a in count_end]
    for slot, k in enumerate((0, 1, 2, 4, 5, 6)):
        mains, ends = pair(k)
        for bz in range(2):
            main, end = mains[bz], ends[bz]
            if k < 3:
                main = main * inv_main[bz]
                end = end * inv_end[bz]
            rolled = lroll(main, -16)
            ahead = jnp.where(x_in < 7, rolled, jnp.where(x_out == 3, end, sroll(rolled, -1)))
            view_ref[bz * 6 + slot] = main
            view_ref[(2 + bz) * 6 + slot] = ahead


def cell_body(s_ref, *refs):
    inputs = refs[:10]
    send_ref, view_ref, ext_ref, end_ref, vel_ref = refs[10:]
    view_body(*inputs, view_ref, ext_ref, end_ref)

    def group(g, carry):
        first = pl.multiple_of(g * 8, 8)
        acc = [jnp.zeros((8, 128), F32) for _ in range(3)]
        total = jnp.zeros((8, 128), F32)
        for bx in range(2):
            for bz in range(2):
                wide = [view_ref[(bx * 2 + bz) * 6 + k, pl.ds(first, 16), :] for k in range(6)]
                for by in range(2):
                    o = bx * 4 + by * 2 + bz
                    ux, uy, uz, nx, ny, nz = [w[4 * by : 4 * by + 8] for w in wide]
                    sx, sy, sz, num = [s_ref[o * 4 + q, pl.ds(first, 8), :] for q in range(4)]
                    mx, my, mz = num * ux, num * uy, num * uz
                    wx, wy, wz = sx - mx, sy - my, sz - mz
                    along = (1.0 - ROT_COS) * (nx * wx + ny * wy + nz * wz)
                    acc[0] += mx + ROT_COS * wx + ROT_SIN * (ny * wz - nz * wy) + along * nx
                    acc[1] += my + ROT_COS * wy + ROT_SIN * (nz * wx - nx * wz) + along * ny
                    acc[2] += mz + ROT_COS * wz + ROT_SIN * (nx * wy - ny * wx) + along * nz
                    total += num
        inverse = 1.0 / jnp.maximum(total, 1.0)
        for c in range(3):
            vel_ref[c, pl.ds(first, 8), :] = acc[c] * inverse
        return carry

    lax.fori_loop(0, TILES // 8, group, 0)
    lane = iota((TILES, 128), 1)
    row = iota((TILES, 128), 0)
    for c in range(3):
        plane = vel_ref[c]
        for bit in range(4):
            size = 1 << bit
            row_bit = (row >> bit) & 1
            lane_bit = (lane >> bit) & 1
            down = sroll(lroll(plane, size), -size)
            up = sroll(lroll(plane, -size), size)
            plane = jnp.where(row_bit == lane_bit, plane, jnp.where(row_bit == 0, down, up))
        for part in range(8):
            send_ref[part, 64 * c : 64 * c + 64, :] = plane[64 * (part // 4) : 64 * (part // 4) + 64]


def collide_body(start, shift_ref, v_ref, p_ref, view_ref, *refs):
    out_ref, turn_ref = refs[-2:]
    step = pl.program_id(0) + start
    cells = iota((TILE, TILE), 0).astype(F32).astype(BF16)

    @pl.when(step == start)
    def _():
        turn_ref[...] = jnp.zeros(turn_ref.shape, F32)

    def group(g, carry):
        place = p_ref[pl.ds(pl.multiple_of(g * 40, 8), 40), :]
        member = (place >> 6).astype(F32)
        octant = octants(place, shift_ref)
        first = pl.multiple_of((step * PARTS + g) * 8, 8)
        for bx in range(2):
            for bz in range(2):
                for k in range(6):
                    wide = view_ref[(bx * 2 + bz) * 6 + k, pl.ds(first, 16), :]
                    for by in range(2):
                        o = bx * 4 + by * 2 + bz
                        turn_ref[pl.ds(8 * o + k, 8, stride=LROW), :] = wide[4 * by : 4 * by + 8]
        for t in range(8):
            high, low = split(turn_ref[LROW * t : LROW * t + 64, :])
            onehot = onehot_of(member, t, cells)
            picked = dot(
                jnp.concatenate([high, low], axis=1), jnp.concatenate([onehot, onehot], axis=0)
            )
            code = jnp.broadcast_to(tile_row(octant, t), (8, 640))
            chosen = picked[0:8]
            for o in range(1, 8):
                chosen = jnp.where(code == o, picked[8 * o : 8 * o + 8], chosen)
            speed = v_ref[:, pl.ds(pl.multiple_of(g * 5120 + t * 640, 128), 640)]
            ux, uy, uz, nx, ny, nz = [chosen[k : k + 1] for k in range(6)]
            wx, wy, wz = speed[0:1] - ux, speed[1:2] - uy, speed[2:3] - uz
            along = (1.0 - ROT_COS) * (nx * wx + ny * wy + nz * wz)
            new = [
                ux + ROT_COS * wx + ROT_SIN * (ny * wz - nz * wy) + along * nx,
                uy + ROT_COS * wy + ROT_SIN * (nz * wx - nx * wz) + along * ny,
                uz + ROT_COS * wz + ROT_SIN * (nx * wy - ny * wx) + along * nz,
            ]
            out_ref[:, pl.ds(pl.multiple_of(g * 5120 + t * 640, 128), 640)] = jnp.concatenate(
                new, axis=0
            )
        return carry

    lax.fori_loop(0, PARTS, group, 0)


def table_parts(table):
    table = np.asarray(table, np.float32)
    high = table.astype(BF16)
    low = (table - high.astype(np.float32)).astype(BF16)
    return high, low


def z_tables():
    pos = np.arange(NZ)[None, :]
    line = np.arange(16)[:, None]
    quarters = []
    for quarter in range(4):
        owner = line // 2 * 8 + line % 2 * 4 + quarter
        for q in range(4):
            phase = (2 * owner + q // 2) * pos % NZ * (2.0 * np.pi / NZ)
            quarters.append(-np.sin(phase) if q % 2 else np.cos(phase))
    return table_parts(np.concatenate(quarters, axis=0).reshape(4, 64, NZ))


def y_tables():
    phase = np.arange(NY)[:, None] * np.arange(NY)[None, :] % NY * (2.0 * np.pi / NY)
    return table_parts(np.concatenate([np.cos(phase), np.sin(phase)], axis=0))


def x_tables():
    k = np.arange(512)
    lane = k % 128
    x = k // 128 * 32 + (lane & 3) * 8 + lane // 16
    kz = (lane >> 3) & 1
    part = (lane >> 2) & 1
    n = np.arange(512)
    part_out, kz_out, kx = n // 256, n // 128 % 2, n % 128
    phase = x[:, None] * kx[None, :] % NX * (2.0 * np.pi / NX)
    same = kz[:, None] == kz_out[None, :]
    c, s = np.cos(phase), np.sin(phase)
    real = np.where(part[:, None] == 0, c, s)
    imag = np.where(part[:, None] == 0, -s, c)
    table = np.where(part_out[None, :] == 0, real, imag) * same / math.sqrt(NX * NY * NZ)
    return table_parts(table)


def shell_counts():
    def wave(n):
        k = np.arange(n)
        return np.where(k >= n // 2, k - n, k)

    square = wave(NZ)[:, None, None] ** 2 + wave(NY)[None, :, None] ** 2 + wave(NX)[None, None, :] ** 2
    edges = np.arange(NSHELL + 1) ** 2
    below = np.searchsorted(np.sort(square.reshape(-1)), edges, side="left")
    return np.diff(below).astype(np.float32)


def z_body(first_ref, in_ref, fh_ref, fl_ref, out_ref):
    lane = iota((16, 128), 1)
    fh, fl = fh_ref[first_ref[2]], fl_ref[first_ref[2]]
    for c in range(3):
        data = jnp.concatenate(
            [
                in_ref[:, 64 * c + 16 * r : 64 * c + 16 * r + 16, :].reshape(128, 128)
                for r in range(4)
            ],
            axis=1,
        )
        high, low = split(data)
        res = dot(fh, high) + dot(fh, low) + dot(fl, high)
        for r in range(4):
            g = [res[16 * q : 16 * q + 16, 128 * r : 128 * r + 128] for q in range(4)]
            for bit, size in ((2, 8), (1, 4)):
                clear = (lane & size) == 0
                new = list(g)
                for q in range(4):
                    if not q & bit:
                        a, b = g[q], g[q | bit]
                        new[q] = jnp.where(clear, a, lroll(b, size))
                        new[q | bit] = jnp.where(clear, lroll(a, -size), b)
                g = new
            for k in range(4):
                out_ref[pl.ds(16 * c + 4 * r + k, 16, stride=48), :] = g[k]


def y_body(in_ref, fh_ref, fl_ref, out_ref):
    both = in_ref[...].reshape(16, 48, 128)
    data = jnp.concatenate(
        [both[:, 16 * c : 16 * c + 16].reshape(256, 128) for c in range(3)], axis=1
    )
    high, low = split(data)
    fh, fl = fh_ref[...], fl_ref[...]
    res = dot(fh, high) + dot(fh, low) + dot(fl, high)
    is_real = (iota((256, 128), 1) & 4) == 0
    for c in range(3):
        even = res[0:256, 128 * c : 128 * c + 128]
        odd = res[256:512, 128 * c : 128 * c + 128]
        out = even + jnp.where(is_real, lroll(odd, -4), -lroll(odd, 4))
        for d in range(4):
            out_ref[d, 64 * c : 64 * c + 64, :] = out[64 * d : 64 * d + 64]
            out_ref[d, 192 + 64 * c : 256 + 64 * c, :] = out[0:64]


def x_lines(in_ref, fh_ref, fl_ref, first):
    data = jnp.concatenate([in_ref[s, first : first + 192, :] for s in range(4)], axis=1)
    high, low = split(data)
    fh, fl = fh_ref[...], fl_ref[...]
    return dot(high, fh) + dot(low, fh) + dot(high, fl)


def mode_body(in_ref, fh_ref, fl_ref, out_ref):
    res = x_lines(in_ref, fh_ref, fl_ref, 0)
    for part in range(2):
        for c in range(3):
            for kz in range(2):
                here = slice(256 * part + 128 * kz, 256 * part + 128 * kz + 128)
                out_ref[part, c, kz] = res[64 * c : 64 * c + 64, here]


def shell_body(first_ref, in_ref, fh_ref, fl_ref, shell_ref, sums_ref):
    res = x_lines(in_ref, fh_ref, fl_ref, 192)
    ky = iota((64, 128), 0)
    kx = iota((64, 128), 1)
    kx = jnp.where(kx >= NX // 2, kx - NX, kx)
    plane = ky * ky + kx * kx
    weight = jnp.where(ky == 0, 1.0, 2.0)
    energy, square = [], []
    for kz in range(2):
        total = jnp.zeros((64, 128), F32)
        for part in range(2):
            for c in range(3):
                here = slice(256 * part + 128 * kz, 256 * part + 128 * kz + 128)
                block = res[64 * c : 64 * c + 64, here]
                total += block * block
        wave = first_ref[0] + kz
        wave = jnp.where(wave >= NZ // 2, wave - NZ, wave)
        energy.append(total * weight)
        square.append(plane + wave * wave)
    energy = jnp.concatenate(energy, axis=0)
    square = jnp.concatenate(square, axis=0)
    for s in range(NSHELL):
        kept = jnp.where(square < (s + 1) * (s + 1), energy, 0.0)
        sums_ref[s : s + 1, :] = jnp.sum(kept, axis=0, keepdims=True)
    cumulative = sums_ref[...]
    before = jnp.where(iota((NSHELL, 128), 0) == 0, 0.0, sroll(cumulative, 1))
    own = jnp.concatenate([cumulative - before, jnp.zeros((64, 128), F32)], axis=0)
    shell_ref[...] = jnp.sum(own.T, axis=0, keepdims=True)


def struct(*shape):
    return jax.ShapeDtypeStruct(shape, F32)


SMEM = pl.BlockSpec(memory_space=pltpu.SMEM)


def ring(x, axis):
    count = lax.axis_size(axis)
    forward = [(i, (i + 1) % count) for i in range(count)]
    backward = [(target, source) for source, target in forward]
    low, high = x
    return lax.ppermute(high, axis, forward), lax.ppermute(low, axis, backward)


def gathered_sum(x, axes):
    count = lax.axis_size(axes)
    copies = jnp.broadcast_to(x[None], (count, *x.shape))
    return jnp.sum(lax.all_to_all(copies, axes, split_axis=0, concat_axis=0, tiled=True), axis=0)


def params(mib):
    return pltpu.CompilerParams(vmem_limit_bytes=mib * 1024 * 1024)


def whole(*shape):
    return pl.BlockSpec(shape, lambda i: (0,) * len(shape))


def collide(start, stop, grid_shift, velocity, place, views, earlier):
    span = TILES * TILE * PPC // STEPS
    speed_spec = pl.BlockSpec((3, span), lambda i: (0, i + start))
    place_spec = pl.BlockSpec((640 // STEPS, 128), lambda i: (i + start, 0))
    more = [] if earlier is None else [earlier]
    return pl.pallas_call(
        lambda *refs: collide_body(start, *refs),
        name="collide",
        grid=(stop - start,),
        in_specs=[SMEM, speed_spec, place_spec, whole(24, VROWS, 128)]
        + [pl.BlockSpec(memory_space=pl.ANY)] * len(more),
        out_specs=speed_spec,
        out_shape=struct(*velocity.shape),
        scratch_shapes=[pltpu.VMEM((8 * LROW, 128), F32)],
        input_output_aliases={4: 0} if more else {},
        compiler_params=params(12),
        cost_estimate=pl.CostEstimate(
            flops=800_000_000 * (stop - start), bytes_accessed=4_000_000, transcendentals=0
        ),
    )(grid_shift, velocity, place, views, *more)


def per_device(velocity, particle_place, grid_shift, rotation_axis):
    place = particle_place.reshape(640, 128)
    axis_index = rotation_axis.reshape(TILES, 128)
    span = TILES * TILE * PPC // BLOCKS
    speed_spec = pl.BlockSpec((3, span), lambda i: (0, i))
    place_spec = pl.BlockSpec((640 // BLOCKS, 128), lambda i: (i, 0))
    out_shapes = [(32, TILES, 128), (3, TILES, 128), (40, 128), (40, 128)]
    sums, normal, x_lo, x_hi = pl.pallas_call(
        scatter_body,
        name="scatter",
        grid=(BLOCKS,),
        in_specs=[SMEM, speed_spec, place_spec, whole(TILES, 128)],
        out_specs=[whole(*s) for s in out_shapes],
        out_shape=[struct(*s) for s in out_shapes],
        scratch_shapes=[pltpu.VMEM((8 * SROW, 128), F32)],
        compiler_params=params(12),
    )(grid_shift, velocity, place, axis_index)
    main, y_lo, y_hi, z_lo, z_hi = pl.pallas_call(
        plane_body,
        name="planes",
        out_shape=[struct(4, ROWS, 128)] + [struct(40, 128)] * 2 + [struct(ROWS, 128)] * 2,
        scratch_shapes=[pltpu.VMEM((5, ROWS, 128), F32), pltpu.VMEM((1, ROWS, 128), F32)],
        compiler_params=params(12),
        cost_estimate=pl.CostEstimate(flops=1_000_000_000, bytes_accessed=3_000_000, transcendentals=0),
    )(sums, normal)
    below, above = ring((x_lo, x_hi), "gx")
    x_lo, x_hi, y_lo, y_hi = pl.pallas_call(
        fold_x_body, name="fold_x", out_shape=[struct(40, 128)] * 4, compiler_params=params(2)
    )(x_lo, x_hi, below, above, y_lo, y_hi)
    below, above = ring((y_lo, y_hi), GY)
    y_lo, y_hi, z_lo, z_hi = pl.pallas_call(
        fold_y_body, name="fold_y", out_shape=[struct(40, 128)] * 2 + [struct(ROWS, 128)] * 2,
        compiler_params=params(3),
    )(y_lo, y_hi, below, above, x_lo, x_hi, z_lo, z_hi)
    below, above = ring((z_lo, z_hi), GZ)
    pieces = (main, normal, x_lo, x_hi, y_lo, y_hi, z_lo, z_hi, below, above)
    plane = pltpu.VMEM((7, ROWS, 128), F32)
    sent = pl.pallas_call(
        cell_body,
        name="cells",
        out_shape=struct(8, 192, 128),
        scratch_shapes=[
            pltpu.VMEM((24, VROWS, 128), F32),
            plane,
            plane,
            pltpu.VMEM((3, TILES, 128), F32),
        ],
        compiler_params=params(12),
    )(sums, *pieces)
    pieces, sent = lax.optimization_barrier((pieces, sent))
    views = pl.pallas_call(
        view_body,
        name="views",
        out_shape=struct(24, VROWS, 128),
        scratch_shapes=[plane, plane],
        compiler_params=params(12),
        cost_estimate=pl.CostEstimate(flops=1_000_000_000, bytes_accessed=3_000_000, transcendentals=0),
    )(*pieces)
    first = jnp.stack(
        [lax.axis_index(GY_GZ) * 2, lax.axis_index("gx") * 64, lax.axis_index("gz_1")]
    ).astype(jnp.int32)
    arrived = lax.all_to_all(sent, GZ, split_axis=0, concat_axis=0, tiled=True)
    updated = collide(0, EARLY, grid_shift, velocity, place, views, None)
    arrived, updated = lax.optimization_barrier((arrived, updated))
    vmem = pl.BlockSpec(memory_space=pltpu.VMEM)
    lines = pl.pallas_call(
        z_body,
        name="z_lines",
        in_specs=[SMEM, vmem, vmem, vmem],
        out_shape=struct(768, 128),
        compiler_params=params(6),
    )(first, arrived, *z_tables())
    pencil = lax.all_to_all(
        lines.reshape(16, 48, 128), ("gy_0", "gy_1", "gz_0"), split_axis=0, concat_axis=0, tiled=True
    )
    new_velocity = collide(EARLY, STEPS, grid_shift, velocity, place, views, updated)
    pencil, new_velocity = lax.optimization_barrier((pencil, new_velocity))
    rows = pl.pallas_call(y_body, name="y_lines", out_shape=struct(4, 384, 128), compiler_params=params(12))(
        pencil.reshape(768, 128), *y_tables()
    )
    columns = lax.all_to_all(rows, "gx", split_axis=0, concat_axis=0, tiled=True)
    tables = x_tables()
    shells = pl.pallas_call(
        shell_body,
        name="x_shells",
        in_specs=[SMEM, vmem, vmem, vmem],
        out_shape=struct(1, 128),
        scratch_shapes=[pltpu.VMEM((NSHELL, 128), F32)],
        compiler_params=params(12),
    )(first, columns, *tables)
    columns, shells = lax.optimization_barrier((columns, shells))
    modes = pl.pallas_call(
        mode_body,
        name="x_modes",
        out_shape=struct(2, 3, 2, 64, 128),
        compiler_params=params(12),
        cost_estimate=pl.CostEstimate(flops=2_000_000_000, bytes_accessed=3_000_000, transcendentals=0),
    )(columns, *tables)
    total = gathered_sum(shells, GY_GZ)
    spectrum = total[0, :NSHELL] / shell_counts()
    return new_velocity, modes, spectrum


def solution(mesh):
    torus = Mesh(
        mesh.devices.reshape(mesh.shape["gx"], 4, 2, 2, 4), ("gx", "gy_0", "gy_1", "gz_0", "gz_1")
    )
    in_specs = (P(None, GX_GY_GZ), P(GX_GY_GZ), P(), P(GY, "gx", GZ))
    out_specs = (P(None, GX_GY_GZ), P(None, None, GY_GZ, "gx", None), P())
    return jax.shard_map(
        per_device, mesh=torus, in_specs=in_specs, out_specs=out_specs, check_vma=False
    )
```

```python
import math

import jax
import jax.numpy as jnp
import numpy as np
from jax import lax
from jax.experimental import pallas as pl
from jax.experimental.pallas import tpu as pltpu
from jax.sharding import Mesh
from jax.sharding import PartitionSpec as P

PPC = 5
TILE = 128
SUB = 4
NAXES = 1024
NSHELL = 64
NX, NY, NZ = 128, 256, 128
GX_GY_GZ = ("gx", "gy_0", "gy_1", "gz_0", "gz_1")
GY = ("gy_0", "gy_1")
GZ = ("gz_0", "gz_1")
GY_GZ = ("gy_0", "gy_1", "gz_0", "gz_1")
ROT_COS = math.cos(130.0 * math.pi / 180.0)
ROT_SIN = math.sin(130.0 * math.pi / 180.0)
F32 = jnp.float32
BF16 = jnp.bfloat16
TILES = 128
ROWS = 160
SROW = 36
LROW = 68
BLOCKS = 1
GROUPS = TILES // 8 // BLOCKS
STEPS = 8
EARLY = 5
PARTS = TILES // 8 // STEPS


def axis_vectors(axis_index):
    level = 1.0 - (2.0 * axis_index.astype(F32) + 1.0) / NAXES
    radius = jnp.sqrt(1.0 - level * level)
    whole_turns = (axis_index * 1597).astype(F32) * (1.0 / 2584.0)
    turn = (axis_index * 1597 - 2584 * jnp.floor(whole_turns).astype(jnp.int32)).astype(F32)
    turn = turn * (2.0 * math.pi / 2584.0)
    return radius * jnp.cos(turn), radius * jnp.sin(turn), level


def iota(shape, dim):
    return lax.broadcasted_iota(jnp.int32, shape, dim)


def lroll(x, amount):
    amount %= 128
    return pltpu.roll(x, amount, 1) if amount else x


def sroll(x, amount):
    return pltpu.roll(x, amount % x.shape[0], 0)


def split(x):
    high = x.astype(BF16)
    return high, (x - high.astype(F32)).astype(BF16)


def dot(a, b):
    return jnp.dot(a, b, preferred_element_type=F32)


def octants(place, shift_ref):
    bit_x = (((place >> 4) & 3) + shift_ref[0] >= SUB).astype(jnp.int32)
    bit_y = (((place >> 2) & 3) + shift_ref[1] >= SUB).astype(jnp.int32)
    bit_z = ((place & 3) + shift_ref[2] >= SUB).astype(jnp.int32)
    return bit_x * 4 + bit_y * 2 + bit_z


def tile_row(rows, t):
    return jnp.concatenate([rows[PPC * t + r : PPC * t + r + 1, :] for r in range(PPC)], axis=1)


def onehot_of(member, t, cells):
    return jnp.concatenate(
        [
            jnp.where(
                cells
                == jnp.broadcast_to(
                    member[PPC * t + r : PPC * t + r + 1, :], cells.shape
                ).astype(BF16),
                jnp.ones(cells.shape, BF16),
                jnp.zeros(cells.shape, BF16),
            )
            for r in range(PPC)
        ],
        axis=1,
    )


def scatter_body(shift_ref, v_ref, p_ref, axis_ref, s_ref, n_ref, xlo_ref, xhi_ref, turn_ref):
    step = pl.program_id(0)
    cells = iota((TILE, TILE), 0).astype(F32).astype(BF16)
    upper = iota((8, TILE), 0) < 4

    def group(g, carry):
        place = p_ref[pl.ds(pl.multiple_of(g * 40, 8), 40), :]
        member = (place >> 6).astype(F32)
        octant = octants(place, shift_ref)
        speed = v_ref[:, pl.ds(pl.multiple_of(g * 5120, 128), 5120)]
        high = speed.astype(BF16).astype(F32)
        low = speed - high
        one = jnp.ones((1, 640), F32)
        zero = jnp.zeros((1, 640), F32)
        for t in range(8):
            here = slice(t * 640, (t + 1) * 640)
            onehot = onehot_of(member, t, cells)
            code = jnp.broadcast_to(tile_row(octant, t), (8, 640))
            values = jnp.concatenate([high[:, here], one, low[:, here], zero], axis=0)
            weighted = jnp.concatenate(
                [jnp.where(code == o, values, 0.0) for o in range(8)], axis=0
            ).astype(BF16)
            sums = lax.dot_general(
                onehot, weighted, (((1,), (1,)), ((), ())), preferred_element_type=F32
            ).T
            for pair in range(4):
                even = sums[16 * pair : 16 * pair + 8]
                odd = sums[16 * pair + 8 : 16 * pair + 16]
                both = jnp.where(upper, even + sroll(even, 4), odd + sroll(odd, 4))
                turn_ref[SROW * t + 8 * pair : SROW * t + 8 * pair + 8, :] = both
        first = pl.multiple_of((step * GROUPS + g) * 8, 8)
        for c, axis in enumerate(axis_vectors(axis_ref[pl.ds(first, 8), :])):
            n_ref[c, pl.ds(first, 8), :] = axis
        for r in range(32):
            s_ref[r, pl.ds(first, 8), :] = turn_ref[pl.ds(r, 8, stride=SROW), :]
        return carry

    lax.fori_loop(0, GROUPS, group, 0)

    @pl.when(step == BLOCKS - 1)
    def _():
        z = iota((32, 128), 1) & 15
        lane = iota((40, 128), 1)
        pad = jnp.zeros((8, 128), F32)
        low_face = jnp.zeros((40, 128), F32)
        high_face = jnp.zeros((40, 128), F32)
        for q in range(5):
            faces = []
            for bx in range(2):
                parts = []
                for by in range(2):
                    base = bx * 4 + by * 2
                    rows = pl.ds(3 * bx, 32, stride=4)
                    if q < 4:
                        above = s_ref[(base + 1) * 4 + q, rows, :]
                        part = s_ref[base * 4 + q, rows, :] + jnp.where(z > 0, lroll(above, 1), 0.0)
                    else:
                        part = jnp.zeros((32, 128), F32)
                        for k in range(4):
                            above = s_ref[(base + 1) * 4 + k, rows, :]
                            part = jnp.where(z == k, lroll(above, k - 15), part)
                    parts.append(jnp.concatenate([part, pad], axis=0))
                faces.append(parts[0] + sroll(parts[1], 1))
            inside = (lane >> 4) == q if q < 4 else (lane >> 2) == 16
            low_face = jnp.where(inside, lroll(faces[0], 16 * q), low_face)
            high_face = jnp.where(inside, lroll(faces[1], 16 * q - 112), high_face)
        for c in range(3):
            inside = ((lane >> 4) == 5 + c) & (iota((40, 128), 0) < 32)
            face = jnp.concatenate([n_ref[c, pl.ds(0, 32, stride=4), :], pad], axis=0)
            low_face = jnp.where(inside, lroll(face, 80 + 16 * c), low_face)
        xlo_ref[...] = low_face
        xhi_ref[...] = high_face


def plane_body(s_ref, n_ref, m_ref, ylo_ref, yhi_ref, zlo_ref, zhi_ref, edge_ref, zed_ref):
    lane = iota((TILES, 128), 1)
    row = iota((TILES, 128), 0)
    z = lane & 15
    x_in = lane >> 4
    x_out = row & 3
    last = (x_in == 7) & (x_out == 3)

    def x_shift(plane):
        rolled = lroll(plane, 16)
        return jnp.where(
            x_in > 0, rolled, jnp.where(x_out > 0, sroll(rolled, 1), 0.0)
        )

    for q in range(5):
        for by in range(2):
            parts = []
            for bx in range(2):
                base = bx * 4 + by * 2
                if q < 4:
                    above = s_ref[(base + 1) * 4 + q]
                    parts.append(
                        s_ref[base * 4 + q] + jnp.where(z > 0, lroll(above, 1), 0.0)
                    )
                else:
                    rim = jnp.zeros((TILES, 128), F32)
                    for k in range(4):
                        rim = jnp.where(z == k, lroll(s_ref[(base + 1) * 4 + k], k - 15), rim)
                    parts.append(rim)
            main = parts[0] + x_shift(parts[1])
            edge = jnp.where(last, parts[1], 0.0)
            dst = m_ref if q < 4 else zed_ref
            at = q if q < 4 else 0
            if by == 0:
                dst[at, 0:TILES, :] = main
                dst[at, TILES:ROWS, :] = jnp.zeros((ROWS - TILES, 128), F32)
                edge_ref[q, 0:TILES, :] = edge
                edge_ref[q, TILES:ROWS, :] = jnp.zeros((ROWS - TILES, 128), F32)
            else:
                dst[at, 4:132, :] = dst[at, 4:132, :] + main
                edge_ref[q, 4:132, :] = edge_ref[q, 4:132, :] + edge
    ylo_ref[...] = jnp.zeros((40, 128), F32)
    yhi_ref[...] = jnp.zeros((40, 128), F32)
    for q in range(5):
        src = m_ref if q < 4 else zed_ref
        at = q if q < 4 else 0
        ylo_ref[4 * q : 4 * q + 4, :] = src[at, 0:4, :]
        yhi_ref[4 * q : 4 * q + 4, :] = src[at, 128:132, :]
    for c in range(3):
        ylo_ref[20 + 4 * c : 24 + 4 * c, :] = n_ref[c, 0:4, :]
    big = iota((ROWS, 128), 1)
    slot = big & 15
    low_z = jnp.zeros((ROWS, 128), F32)
    for q in range(4):
        low_z = jnp.where(slot == q, lroll(m_ref[q], q), low_z)
    for c in range(3):
        face = jnp.concatenate([n_ref[c], jnp.zeros((ROWS - TILES, 128), F32)], axis=0)
        low_z = jnp.where(slot == 4 + c, lroll(face, 4 + c), low_z)
    zlo_ref[...] = low_z
    zhi_ref[...] = zed_ref[0]


def fold_x_body(xlo_ref, xhi_ref, from_low, from_high, ylo_ref, yhi_ref,
                xlo_out, xhi_out, ylo_out, yhi_out):
    low = xlo_ref[...] + from_low[...]
    high = xhi_ref[...] + from_high[...]
    xlo_out[...] = low
    xhi_out[...] = high
    lane = iota((1, 128), 1)
    for src, dst, y in ((ylo_ref, ylo_out, 0), (yhi_ref, yhi_out, 32)):
        dst[...] = src[...]
        for q in range(4):
            dst[4 * q : 4 * q + 1, :] = jnp.where(
                lane < 16, lroll(low[y : y + 1], -16 * q), src[4 * q : 4 * q + 1, :]
            )
        dst[16:17, :] = jnp.where(lane < 4, lroll(low[y : y + 1], -64), src[16:17, :])
        dst[32:33, :] = high[y : y + 1]


def fold_y_body(ylo_ref, yhi_ref, from_low, from_high, xlo_ref, xhi_ref, zlo_ref, zhi_ref,
                ylo_out, yhi_out, zlo_out, zhi_out):
    low = ylo_ref[...] + from_low[...]
    high = yhi_ref[...] + from_high[...]
    ylo_out[...] = low
    yhi_out[...] = high
    zlo_out[...] = zlo_ref[...]
    zhi_out[...] = zhi_ref[...]
    x_low = xlo_ref[...]
    x_high = xhi_ref[...]
    lane = iota((40, 128), 1)
    lo0 = zlo_out[pl.ds(0, 40, stride=4), :]
    hi0 = zhi_out[pl.ds(0, 40, stride=4), :]
    lo3 = zlo_out[pl.ds(3, 40, stride=4), :]
    hi3 = zhi_out[pl.ds(3, 40, stride=4), :]
    for q in range(4):
        lo0 = jnp.where(lane == q, lroll(x_low, q - 16 * q), lo0)
        lo3 = jnp.where(lane == 120 + q, lroll(x_high, 120 + q - 16 * q), lo3)
    for c in range(3):
        lo3 = jnp.where(lane == 124 + c, lroll(x_high, 124 + c - 80 - 16 * c), lo3)
    hi0 = jnp.where(lane < 4, lroll(x_low, -64), hi0)
    hi3 = jnp.where((lane >= 120) & (lane < 124), lroll(x_high, 120 - 64), hi3)
    zlo_out[pl.ds(0, 40, stride=4), :] = lo0
    zhi_out[pl.ds(0, 40, stride=4), :] = hi0
    zlo_out[pl.ds(3, 40, stride=4), :] = lo3
    zhi_out[pl.ds(3, 40, stride=4), :] = hi3
    lane4 = iota((4, 128), 1)
    slot = lane4 & 15
    corner = (iota((4, 128), 0) == 3) & (lane4 >= 120)
    for face, first in ((low, 0), (high, 128)):
        lo = jnp.zeros((4, 128), F32)
        for q in range(4):
            lo = jnp.where(slot == q, lroll(face[4 * q : 4 * q + 4], q), lo)
        for c in range(3):
            lo = jnp.where(slot == 4 + c, lroll(face[20 + 4 * c : 24 + 4 * c], 4 + c), lo)
        end = face[32:33]
        tail = jnp.zeros((1, 128), F32)
        lane1 = iota((1, 128), 1)
        for q in range(4):
            tail = jnp.where(lane1 == 120 + q, lroll(end, 120 + q - 16 * q), tail)
        for c in range(3):
            tail = jnp.where(lane1 == 124 + c, lroll(end, 124 + c - 80 - 16 * c), tail)
        zlo_out[first : first + 4, :] = jnp.where(corner, tail, lo)
        hi = jnp.where(slot < 4, face[16:20], 0.0)
        zhi_out[first : first + 4, :] = jnp.where(
            corner, jnp.where(lane1 < 124, lroll(end, 120 - 64), 0.0), hi
        )


VROWS = 136


def view_body(m_ref, n_ref, xlo_ref, xhi_ref, ylo_ref, yhi_ref, zlo_ref, zhi_ref,
              from_low, from_high, view_ref, ext_ref, end_ref):
    z_low = zlo_ref[0:VROWS, :] + from_low[0:VROWS, :]
    z_high = zhi_ref[0:VROWS, :] + from_high[0:VROWS, :]
    x_low = xlo_ref[...]
    x_high = xhi_ref[...]
    y_low = ylo_ref[...]
    y_high = yhi_ref[...]
    lane40 = iota((40, 128), 1)
    lane = iota((VROWS, 128), 1)
    row = iota((VROWS, 128), 0)
    z = lane & 15
    x_in = lane >> 4
    x_out = row & 3
    for k in range(7):
        if k < 4:
            ext_ref[k] = m_ref[k]
            held = ext_ref[k, pl.ds(0, 40, stride=4), :]
            ext_ref[k, pl.ds(0, 40, stride=4), :] = jnp.where(
                lane40 < 16, lroll(x_low, -16 * k), held
            )
            ext_ref[k, 0:4, :] = y_low[4 * k : 4 * k + 4]
            ext_ref[k, 128:132, :] = y_high[4 * k : 4 * k + 4]
            amount = 112 - 16 * k
        else:
            c = k - 4
            ext_ref[k, 0:TILES, :] = n_ref[c]
            ext_ref[k, 128:132, :] = y_high[20 + 4 * c : 24 + 4 * c]
            amount = 32 - 16 * c
        end_ref[k, pl.ds(3, 40, stride=4), :] = lroll(x_high, amount)
        end_ref[k, 131:132, :] = lroll(y_high[32:33], amount)
        if k < 4:
            end_ref[k, 3:4, :] = lroll(y_low[32:33], amount)

    def pair(k):
        main = ext_ref[k, 0:VROWS, :]
        end = end_ref[k, 0:VROWS, :]
        if k < 4:
            main = jnp.where(z == 0, lroll(z_low, -k), main)
            end = jnp.where(z == 0, lroll(z_low, -8 - k), end)
        main1 = jnp.where(z < 15, lroll(main, -1), lroll(z_high, 15 - k))
        end1 = jnp.where(z < 15, lroll(end, -1), lroll(z_high, 7 - k))
        return (main, main1), (end, end1)

    count_main, count_end = pair(3)
    inv_main = [1.0 / jnp.maximum(a, 1.0) for a in count_main]
    inv_end = [1.0 / jnp.maximum(a, 1.0) for a in count_end]
    for slot, k in enumerate((0, 1, 2, 4, 5, 6)):
        mains, ends = pair(k)
        for bz in range(2):
            main, end = mains[bz], ends[bz]
            if k < 3:
                main = main * inv_main[bz]
                end = end * inv_end[bz]
            rolled = lroll(main, -16)
            ahead = jnp.where(x_in < 7, rolled, jnp.where(x_out == 3, end, sroll(rolled, -1)))
            view_ref[bz * 6 + slot] = main
            view_ref[(2 + bz) * 6 + slot] = ahead


def cell_body(s_ref, *refs):
    inputs = refs[:10]
    send_ref, view_ref, ext_ref, end_ref, vel_ref = refs[10:]
    view_body(*inputs, view_ref, ext_ref, end_ref)

    def group(g, carry):
        first = pl.multiple_of(g * 8, 8)
        acc = [jnp.zeros((8, 128), F32) for _ in range(3)]
        total = jnp.zeros((8, 128), F32)
        for bx in range(2):
            for bz in range(2):
                wide = [view_ref[(bx * 2 + bz) * 6 + k, pl.ds(first, 16), :] for k in range(6)]
                for by in range(2):
                    o = bx * 4 + by * 2 + bz
                    ux, uy, uz, nx, ny, nz = [w[4 * by : 4 * by + 8] for w in wide]
                    sx, sy, sz, num = [s_ref[o * 4 + q, pl.ds(first, 8), :] for q in range(4)]
                    mx, my, mz = num * ux, num * uy, num * uz
                    wx, wy, wz = sx - mx, sy - my, sz - mz
                    along = (1.0 - ROT_COS) * (nx * wx + ny * wy + nz * wz)
                    acc[0] += mx + ROT_COS * wx + ROT_SIN * (ny * wz - nz * wy) + along * nx
                    acc[1] += my + ROT_COS * wy + ROT_SIN * (nz * wx - nx * wz) + along * ny
                    acc[2] += mz + ROT_COS * wz + ROT_SIN * (nx * wy - ny * wx) + along * nz
                    total += num
        inverse = 1.0 / jnp.maximum(total, 1.0)
        for c in range(3):
            vel_ref[c, pl.ds(first, 8), :] = acc[c] * inverse
        return carry

    lax.fori_loop(0, TILES // 8, group, 0)
    lane = iota((TILES, 128), 1)
    row = iota((TILES, 128), 0)
    for c in range(3):
        plane = vel_ref[c]
        for bit in range(4):
            size = 1 << bit
            row_bit = (row >> bit) & 1
            lane_bit = (lane >> bit) & 1
            down = sroll(lroll(plane, size), -size)
            up = sroll(lroll(plane, -size), size)
            plane = jnp.where(row_bit == lane_bit, plane, jnp.where(row_bit == 0, down, up))
        for part in range(8):
            send_ref[part, 64 * c : 64 * c + 64, :] = plane[64 * (part // 4) : 64 * (part // 4) + 64]


def collide_body(start, shift_ref, v_ref, p_ref, view_ref, *refs):
    out_ref, turn_ref = refs[-2:]
    step = pl.program_id(0) + start
    cells = iota((TILE, TILE), 0).astype(F32).astype(BF16)

    @pl.when(step == start)
    def _():
        turn_ref[...] = jnp.zeros(turn_ref.shape, F32)

    def group(g, carry):
        place = p_ref[pl.ds(pl.multiple_of(g * 40, 8), 40), :]
        member = (place >> 6).astype(F32)
        octant = octants(place, shift_ref)
        first = pl.multiple_of((step * PARTS + g) * 8, 8)
        for bx in range(2):
            for bz in range(2):
                for k in range(6):
                    wide = view_ref[(bx * 2 + bz) * 6 + k, pl.ds(first, 16), :]
                    for by in range(2):
                        o = bx * 4 + by * 2 + bz
                        turn_ref[pl.ds(8 * o + k, 8, stride=LROW), :] = wide[4 * by : 4 * by + 8]
        for t in range(8):
            high, low = split(turn_ref[LROW * t : LROW * t + 64, :])
            onehot = onehot_of(member, t, cells)
            picked = dot(
                jnp.concatenate([high, low], axis=1), jnp.concatenate([onehot, onehot], axis=0)
            )
            code = jnp.broadcast_to(tile_row(octant, t), (8, 640))
            chosen = picked[0:8]
            for o in range(1, 8):
                chosen = jnp.where(code == o, picked[8 * o : 8 * o + 8], chosen)
            speed = v_ref[:, pl.ds(pl.multiple_of(g * 5120 + t * 640, 128), 640)]
            ux, uy, uz, nx, ny, nz = [chosen[k : k + 1] for k in range(6)]
            wx, wy, wz = speed[0:1] - ux, speed[1:2] - uy, speed[2:3] - uz
            along = (1.0 - ROT_COS) * (nx * wx + ny * wy + nz * wz)
            new = [
                ux + ROT_COS * wx + ROT_SIN * (ny * wz - nz * wy) + along * nx,
                uy + ROT_COS * wy + ROT_SIN * (nz * wx - nx * wz) + along * ny,
                uz + ROT_COS * wz + ROT_SIN * (nx * wy - ny * wx) + along * nz,
            ]
            out_ref[:, pl.ds(pl.multiple_of(g * 5120 + t * 640, 128), 640)] = jnp.concatenate(
                new, axis=0
            )
        return carry

    lax.fori_loop(0, PARTS, group, 0)


def table_parts(table):
    table = np.asarray(table, np.float32)
    high = table.astype(BF16)
    low = (table - high.astype(np.float32)).astype(BF16)
    return high, low


def z_tables():
    pos = np.arange(NZ)[None, :]
    line = np.arange(16)[:, None]
    quarters = []
    for quarter in range(4):
        owner = line // 2 * 8 + line % 2 * 4 + quarter
        for q in range(4):
            phase = (2 * owner + q // 2) * pos % NZ * (2.0 * np.pi / NZ)
            quarters.append(-np.sin(phase) if q % 2 else np.cos(phase))
    return table_parts(np.concatenate(quarters, axis=0).reshape(4, 64, NZ))


def y_tables():
    phase = np.arange(NY)[:, None] * np.arange(NY)[None, :] % NY * (2.0 * np.pi / NY)
    return table_parts(np.concatenate([np.cos(phase), np.sin(phase)], axis=0))


def x_tables():
    k = np.arange(512)
    lane = k % 128
    x = k // 128 * 32 + (lane & 3) * 8 + lane // 16
    kz = (lane >> 3) & 1
    part = (lane >> 2) & 1
    n = np.arange(512)
    part_out, kz_out, kx = n // 256, n // 128 % 2, n % 128
    phase = x[:, None] * kx[None, :] % NX * (2.0 * np.pi / NX)
    same = kz[:, None] == kz_out[None, :]
    c, s = np.cos(phase), np.sin(phase)
    real = np.where(part[:, None] == 0, c, s)
    imag = np.where(part[:, None] == 0, -s, c)
    table = np.where(part_out[None, :] == 0, real, imag) * same / math.sqrt(NX * NY * NZ)
    return table_parts(table)


def shell_counts():
    def wave(n):
        k = np.arange(n)
        return np.where(k >= n // 2, k - n, k)

    square = wave(NZ)[:, None, None] ** 2 + wave(NY)[None, :, None] ** 2 + wave(NX)[None, None, :] ** 2
    edges = np.arange(NSHELL + 1) ** 2
    below = np.searchsorted(np.sort(square.reshape(-1)), edges, side="left")
    return np.diff(below).astype(np.float32)


def z_body(first_ref, in_ref, fh_ref, fl_ref, out_ref):
    lane = iota((16, 128), 1)
    fh, fl = fh_ref[first_ref[2]], fl_ref[first_ref[2]]
    for c in range(3):
        data = jnp.concatenate(
            [
                in_ref[:, 64 * c + 16 * r : 64 * c + 16 * r + 16, :].reshape(128, 128)
                for r in range(4)
            ],
            axis=1,
        )
        high, low = split(data)
        res = dot(fh, high) + dot(fh, low) + dot(fl, high)
        for r in range(4):
            g = [res[16 * q : 16 * q + 16, 128 * r : 128 * r + 128] for q in range(4)]
            for bit, size in ((2, 8), (1, 4)):
                clear = (lane & size) == 0
                new = list(g)
                for q in range(4):
                    if not q & bit:
                        a, b = g[q], g[q | bit]
                        new[q] = jnp.where(clear, a, lroll(b, size))
                        new[q | bit] = jnp.where(clear, lroll(a, -size), b)
                g = new
            for k in range(4):
                out_ref[pl.ds(16 * c + 4 * r + k, 16, stride=48), :] = g[k]


def y_body(first_ref, in_ref, fh_ref, fl_ref, extra_ref, *refs):
    own_ref = refs[-1]
    both = in_ref[...].reshape(16, 48, 128)
    data = jnp.concatenate(
        [both[:, 16 * c : 16 * c + 16].reshape(256, 128) for c in range(3)], axis=1
    )
    high, low = split(data)
    fh, fl = fh_ref[...], fl_ref[...]
    res = dot(fh, high) + dot(fh, low) + dot(fl, high)
    is_real = (iota((256, 128), 1) & 4) == 0
    for c in range(3):
        even = res[0:256, 128 * c : 128 * c + 128]
        odd = res[256:512, 128 * c : 128 * c + 128]
        out = even + jnp.where(is_real, lroll(odd, -4), -lroll(odd, 4))
        for d in range(4):
            own_ref[d, 64 * c : 64 * c + 64, :] = out[64 * d : 64 * d + 64]
            extra_ref[d, 64 * c : 64 * c + 64, :] = out[0:64]
    for k in range(4):
        refs[k][...] = own_ref[(first_ref[3] + k) & 3]


def x_lines(in_ref, fh_ref, fl_ref):
    data = jnp.concatenate([in_ref[s] for s in range(4)], axis=1)
    high, low = split(data)
    fh, fl = fh_ref[...], fl_ref[...]
    return dot(high, fh) + dot(low, fh) + dot(high, fl)


def mode_body(first_ref, a_ref, b_ref, c_ref, d_ref, fh_ref, fl_ref, out_ref, all_ref):
    for k, part in enumerate((a_ref, b_ref, c_ref, d_ref)):
        all_ref[(first_ref[3] - k) & 3] = part[...]
    res = x_lines(all_ref, fh_ref, fl_ref)
    for part in range(2):
        for c in range(3):
            for kz in range(2):
                here = slice(256 * part + 128 * kz, 256 * part + 128 * kz + 128)
                out_ref[part, c, kz] = res[64 * c : 64 * c + 64, here]


def shell_body(first_ref, in_ref, fh_ref, fl_ref, shell_ref, sums_ref):
    res = x_lines(in_ref, fh_ref, fl_ref)
    ky = iota((64, 128), 0)
    kx = iota((64, 128), 1)
    kx = jnp.where(kx >= NX // 2, kx - NX, kx)
    plane = ky * ky + kx * kx
    weight = jnp.where(ky == 0, 1.0, 2.0)
    energy, square = [], []
    for kz in range(2):
        total = jnp.zeros((64, 128), F32)
        for part in range(2):
            for c in range(3):
                here = slice(256 * part + 128 * kz, 256 * part + 128 * kz + 128)
                block = res[64 * c : 64 * c + 64, here]
                total += block * block
        wave = first_ref[0] + kz
        wave = jnp.where(wave >= NZ // 2, wave - NZ, wave)
        energy.append(total * weight)
        square.append(plane + wave * wave)
    energy = jnp.concatenate(energy, axis=0)
    square = jnp.concatenate(square, axis=0)
    for s in range(NSHELL):
        kept = jnp.where(square < (s + 1) * (s + 1), energy, 0.0)
        sums_ref[s : s + 1, :] = jnp.sum(kept, axis=0, keepdims=True)
    cumulative = sums_ref[...]
    before = jnp.where(iota((NSHELL, 128), 0) == 0, 0.0, sroll(cumulative, 1))
    own = jnp.concatenate([cumulative - before, jnp.zeros((64, 128), F32)], axis=0)
    shell_ref[...] = jnp.broadcast_to(jnp.sum(own.T, axis=0, keepdims=True), (64, 128))


def struct(*shape):
    return jax.ShapeDtypeStruct(shape, F32)


SMEM = pl.BlockSpec(memory_space=pltpu.SMEM)


def ring(x, axis):
    count = lax.axis_size(axis)
    forward = [(i, (i + 1) % count) for i in range(count)]
    backward = [(target, source) for source, target in forward]
    low, high = x
    return lax.ppermute(high, axis, forward), lax.ppermute(low, axis, backward)


def params(mib):
    return pltpu.CompilerParams(vmem_limit_bytes=mib * 1024 * 1024)


def whole(*shape):
    return pl.BlockSpec(shape, lambda i: (0,) * len(shape))


def collide(start, stop, grid_shift, velocity, place, views, earlier):
    span = TILES * TILE * PPC // STEPS
    speed_spec = pl.BlockSpec((3, span), lambda i: (0, i + start))
    place_spec = pl.BlockSpec((640 // STEPS, 128), lambda i: (i + start, 0))
    more = [] if earlier is None else [earlier]
    return pl.pallas_call(
        lambda *refs: collide_body(start, *refs),
        name="collide",
        grid=(stop - start,),
        in_specs=[SMEM, speed_spec, place_spec, whole(24, VROWS, 128)]
        + [pl.BlockSpec(memory_space=pl.ANY)] * len(more),
        out_specs=speed_spec,
        out_shape=struct(*velocity.shape),
        scratch_shapes=[pltpu.VMEM((8 * LROW, 128), F32)],
        input_output_aliases={4: 0} if more else {},
        compiler_params=params(12),
        cost_estimate=pl.CostEstimate(
            flops=800_000_000 * (stop - start), bytes_accessed=4_000_000, transcendentals=0
        ),
    )(grid_shift, velocity, place, views, *more)


def per_device(velocity, particle_place, grid_shift, rotation_axis):
    place = particle_place.reshape(640, 128)
    axis_index = rotation_axis.reshape(TILES, 128)
    span = TILES * TILE * PPC // BLOCKS
    speed_spec = pl.BlockSpec((3, span), lambda i: (0, i))
    place_spec = pl.BlockSpec((640 // BLOCKS, 128), lambda i: (i, 0))
    out_shapes = [(32, TILES, 128), (3, TILES, 128), (40, 128), (40, 128)]
    sums, normal, x_lo, x_hi = pl.pallas_call(
        scatter_body,
        name="scatter",
        grid=(BLOCKS,),
        in_specs=[SMEM, speed_spec, place_spec, whole(TILES, 128)],
        out_specs=[whole(*s) for s in out_shapes],
        out_shape=[struct(*s) for s in out_shapes],
        scratch_shapes=[pltpu.VMEM((8 * SROW, 128), F32)],
        compiler_params=params(12),
    )(grid_shift, velocity, place, axis_index)
    main, y_lo, y_hi, z_lo, z_hi = pl.pallas_call(
        plane_body,
        name="planes",
        out_shape=[struct(4, ROWS, 128)] + [struct(40, 128)] * 2 + [struct(ROWS, 128)] * 2,
        scratch_shapes=[pltpu.VMEM((5, ROWS, 128), F32), pltpu.VMEM((1, ROWS, 128), F32)],
        compiler_params=params(12),
        cost_estimate=pl.CostEstimate(flops=1_000_000_000, bytes_accessed=3_000_000, transcendentals=0),
    )(sums, normal)
    below, above = ring((x_lo, x_hi), "gx")
    x_lo, x_hi, y_lo, y_hi = pl.pallas_call(
        fold_x_body, name="fold_x", out_shape=[struct(40, 128)] * 4, compiler_params=params(2)
    )(x_lo, x_hi, below, above, y_lo, y_hi)
    below, above = ring((y_lo, y_hi), GY)
    y_lo, y_hi, z_lo, z_hi = pl.pallas_call(
        fold_y_body, name="fold_y", out_shape=[struct(40, 128)] * 2 + [struct(ROWS, 128)] * 2,
        compiler_params=params(3),
    )(y_lo, y_hi, below, above, x_lo, x_hi, z_lo, z_hi)
    below, above = ring((z_lo, z_hi), GZ)
    pieces = (main, normal, x_lo, x_hi, y_lo, y_hi, z_lo, z_hi, below, above)
    plane = pltpu.VMEM((7, ROWS, 128), F32)
    sent = pl.pallas_call(
        cell_body,
        name="cells",
        out_shape=struct(8, 192, 128),
        scratch_shapes=[
            pltpu.VMEM((24, VROWS, 128), F32),
            plane,
            plane,
            pltpu.VMEM((3, TILES, 128), F32),
        ],
        compiler_params=params(12),
    )(sums, *pieces)
    pieces, sent = lax.optimization_barrier((pieces, sent))
    views = pl.pallas_call(
        view_body,
        name="views",
        out_shape=struct(24, VROWS, 128),
        scratch_shapes=[plane, plane],
        compiler_params=params(12),
        cost_estimate=pl.CostEstimate(flops=1_000_000_000, bytes_accessed=3_000_000, transcendentals=0),
    )(*pieces)
    first = jnp.stack(
        [lax.axis_index(GY_GZ) * 2, lax.axis_index("gx") * 64, lax.axis_index("gz_1"),
         lax.axis_index("gx")]
    ).astype(jnp.int32)
    arrived = lax.all_to_all(sent, GZ, split_axis=0, concat_axis=0, tiled=True)
    updated = collide(0, EARLY, grid_shift, velocity, place, views, None)
    arrived, updated = lax.optimization_barrier((arrived, updated))
    vmem = pl.BlockSpec(memory_space=pltpu.VMEM)
    lines = pl.pallas_call(
        z_body,
        name="z_lines",
        in_specs=[SMEM, vmem, vmem, vmem],
        out_shape=struct(768, 128),
        compiler_params=params(6),
    )(first, arrived, *z_tables())
    pencil = lax.all_to_all(
        lines.reshape(16, 48, 128), ("gy_0", "gy_1", "gz_0"), split_axis=0, concat_axis=0, tiled=True
    )
    new_velocity = collide(EARLY, STEPS, grid_shift, velocity, place, views, updated)
    pencil, new_velocity = lax.optimization_barrier((pencil, new_velocity))
    extra, *own = pl.pallas_call(
        y_body,
        name="y_lines",
        in_specs=[SMEM, vmem, vmem, vmem],
        out_shape=[struct(4, 192, 128)] + [struct(192, 128)] * 4,
        scratch_shapes=[pltpu.VMEM((4, 192, 128), F32)],
        compiler_params=params(12),
    )(first, pencil.reshape(768, 128), *y_tables())
    columns = lax.all_to_all(extra, "gx", split_axis=0, concat_axis=0, tiled=True)
    tables = x_tables()
    shells = pl.pallas_call(
        shell_body,
        name="x_shells",
        in_specs=[SMEM, vmem, vmem, vmem],
        out_shape=struct(64, 128),
        scratch_shapes=[pltpu.VMEM((NSHELL, 128), F32)],
        compiler_params=params(12),
    )(first, columns, *tables)
    own, shells = lax.optimization_barrier((own, shells))
    gathered = lax.all_to_all(shells.reshape(64, 1, 128), GY_GZ, split_axis=0, concat_axis=0, tiled=True)
    received = [own[0]] + [
        lax.ppermute(own[k], "gx", [(i, (i + k) % 4) for i in range(4)]) for k in range(1, 4)
    ]
    modes = pl.pallas_call(
        mode_body,
        name="x_modes",
        in_specs=[SMEM] + [vmem] * 6,
        out_shape=struct(2, 3, 2, 64, 128),
        scratch_shapes=[pltpu.VMEM((4, 192, 128), F32)],
        compiler_params=params(12),
        cost_estimate=pl.CostEstimate(flops=2_000_000_000, bytes_accessed=3_000_000, transcendentals=0),
    )(first, *received, *tables)
    total = jnp.sum(gathered, axis=0)
    spectrum = total[0, :NSHELL] / shell_counts()
    return new_velocity, modes, spectrum


def solution(mesh):
    torus = Mesh(
        mesh.devices.reshape(mesh.shape["gx"], 4, 2, 2, 4), ("gx", "gy_0", "gy_1", "gz_0", "gz_1")
    )
    in_specs = (P(None, GX_GY_GZ), P(GX_GY_GZ), P(), P(GY, "gx", GZ))
    out_specs = (P(None, GX_GY_GZ), P(None, None, GY_GZ, "gx", None), P())
    return jax.shard_map(
        per_device, mesh=torus, in_specs=in_specs, out_specs=out_specs, check_vma=False
    )
```
